8 devices in a mesh: dp: 1 (over z), tp: 2 (over y), ep: 4 (over x, core).
Axes of the slice: x: 2, y: 2, z: 1, core: 2. Of those that a mesh axis runs over, the one named last changes fastest.
Arguments:
- hidden_in: bfloat16 [32, 256, 1024], P(('dp', 'ep'), 'tp')
- ln_attn: float32 [2, 1024], replicated
- ln_ffn: float32 [2, 1024], replicated
- w_query: bfloat16 [2, 1024, 1024], P(None, None, 'tp')
- w_key: bfloat16 [2, 1024, 1024], P(None, None, 'tp')
- w_value: bfloat16 [2, 1024, 1024], P(None, None, 'tp')
- w_out: bfloat16 [2, 1024, 1024], P(None, 'tp')
- bias_table: float32 [2, 16, 32], P(None, 'tp')
- w_gate: bfloat16 [1024, 512], P(None, 'tp')
- w_up: bfloat16 [1024, 512], P(None, 'tp')
- w_down: bfloat16 [512, 1024], P('tp')
- w_router: float32 [1024, 32], replicated
- expert_in: bfloat16 [32, 1024, 512], P(('tp', 'ep'))
- expert_out: bfloat16 [32, 512, 1024], P(('tp', 'ep'))
- expert_ids: int32 [32, 256, 2], P(('dp', 'ep'), 'tp')
Outputs:
- output 1: bfloat16 [32, 256, 1024], P(('dp', 'ep'), 'tp')
- output 2: bfloat16 [2, 32, 16, 256, 64], P(None, ('dp', 'ep'), 'tp')
- output 3: bfloat16 [2, 32, 16, 256, 64], P(None, ('dp', 'ep'), 'tp')
All inputs are finite; a program needn't handle non-finite values.
Results may differ from the reference program's by a relative error of at most 0.0146873.
Values are sent between devices in bfloat16 or wider.
A program may use at most 1 GiB of HBM per device.

```python
import jax
import jax.numpy as jnp
from jax import lax

D_MODEL = 1024
NUM_HEADS = 16
HEAD_DIM = 64
FF_DIM = 512
NUM_EXPERTS = 32
EP_SIZE = 4
TP_SIZE = 2
BATCH = 32
SEQ_LEN = 256
NUM_BUCKETS = 32
EXACT_BUCKETS = 16

THRESHOLDS = (18, 20, 23, 26, 30, 34, 39, 45, 51, 58, 66, 76, 86, 98, 112)
EPSILON = 1e-6
INNER = NUM_HEADS * HEAD_DIM
LOCAL_BATCH = BATCH // EP_SIZE
LOCAL_SEQ = SEQ_LEN // TP_SIZE
LOCAL_TOKENS = LOCAL_BATCH * LOCAL_SEQ
NUM_GROUPS = EP_SIZE * TP_SIZE
CAPACITY = 4 * LOCAL_TOKENS // NUM_EXPERTS


def draw_ids(id_key):
    coin_key, hot_key, start_key, uniform_key, second_key = jax.random.split(id_key, 5)
    id_shape = (BATCH, SEQ_LEN)
    hot_width = max(NUM_EXPERTS // 8, 1)
    hot_start = jax.random.randint(start_key, (), 0, NUM_EXPERTS)
    hot_pick = (hot_start + jax.random.randint(hot_key, id_shape, 0, hot_width)) % NUM_EXPERTS
    uniform_pick = jax.random.randint(uniform_key, id_shape, 0, NUM_EXPERTS)
    coin_flip = jax.random.randint(coin_key, id_shape, 0, 4)
    first_pick = jnp.where(coin_flip == 0, hot_pick, uniform_pick)
    flat_pos = jnp.arange(BATCH * SEQ_LEN).reshape(id_shape)
    first_pick = jnp.where(flat_pos < NUM_EXPERTS, flat_pos, first_pick)
    second_pick = (first_pick + 1 + jax.random.randint(second_key, id_shape, 0, NUM_EXPERTS - 1)) % NUM_EXPERTS
    return jnp.stack([first_pick, second_pick], axis=-1).astype(jnp.int32)


def setup_inputs(seed: int = 0, part: int = 0) -> dict:
    keys_all = jax.random.split(jax.random.key(seed), 16)
    part_key = jax.random.fold_in(keys_all[0], part)
    act_key, id_key = jax.random.split(part_key)

    def normal(sub_key, dim_tuple, scale_by):
        return jax.random.normal(sub_key, dim_tuple, jnp.float32) * scale_by

    return {
        'hidden_in': normal(act_key, (BATCH, SEQ_LEN, D_MODEL), 1.0).astype(jnp.bfloat16),
        'ln_attn': jax.random.uniform(keys_all[1], (2, D_MODEL), jnp.float32, 0.5, 1.5),
        'ln_ffn': jax.random.uniform(keys_all[2], (2, D_MODEL), jnp.float32, 0.5, 1.5),
        'w_query': normal(keys_all[3], (2, D_MODEL, INNER), D_MODEL ** -0.5).astype(jnp.bfloat16),
        'w_key': normal(keys_all[4], (2, D_MODEL, INNER), D_MODEL ** -0.5).astype(jnp.bfloat16),
        'w_value': normal(keys_all[5], (2, D_MODEL, INNER), D_MODEL ** -0.5).astype(jnp.bfloat16),
        'w_out': normal(keys_all[6], (2, INNER, D_MODEL), INNER ** -0.5).astype(jnp.bfloat16),
        'bias_table': normal(keys_all[7], (2, NUM_HEADS, NUM_BUCKETS), 1.5),
        'w_gate': normal(keys_all[8], (D_MODEL, FF_DIM), D_MODEL ** -0.5).astype(jnp.bfloat16),
        'w_up': normal(keys_all[9], (D_MODEL, FF_DIM), D_MODEL ** -0.5).astype(jnp.bfloat16),
        'w_down': normal(keys_all[10], (FF_DIM, D_MODEL), FF_DIM ** -0.5).astype(jnp.bfloat16),
        'w_router': normal(keys_all[11], (D_MODEL, NUM_EXPERTS), D_MODEL ** -0.5),
        'expert_in': normal(keys_all[12], (NUM_EXPERTS, D_MODEL, FF_DIM), D_MODEL ** -0.5).astype(jnp.bfloat16),
        'expert_out': normal(keys_all[13], (NUM_EXPERTS, FF_DIM, D_MODEL), FF_DIM ** -0.5).astype(jnp.bfloat16),
        'expert_ids': draw_ids(id_key),
    }


def bucket_of(rel_pos):
    bucket_idx = jnp.minimum(rel_pos, EXACT_BUCKETS)
    for threshold in THRESHOLDS:
        bucket_idx = bucket_idx + (rel_pos >= threshold).astype(jnp.int32)
    return bucket_idx


def rms_norm(rows_in, ln_scale):
    wide_rows = rows_in.astype(jnp.float32)
    inv_rms = lax.rsqrt(jnp.mean(wide_rows * wide_rows, axis=-1, keepdims=True) + EPSILON)
    return (wide_rows * inv_rms * ln_scale).astype(jnp.bfloat16)


def causal_bias(bias_rows):
    positions = jnp.arange(SEQ_LEN)
    rel_pos = positions[:, None] - positions[None, :]
    bias_full = jnp.take(bias_rows, bucket_of(jnp.maximum(rel_pos, 0)), axis=1)
    return jnp.where(rel_pos[None] >= 0, bias_full, -jnp.inf)


def attention(hidden, ln_scale, w_query, w_key, w_value, w_out, bias_rows):
    normed = rms_norm(hidden, ln_scale).reshape(BATCH * SEQ_LEN, D_MODEL)

    def project(weight):
        projected = jnp.dot(normed, weight, preferred_element_type=jnp.float32)
        return projected.astype(jnp.bfloat16).reshape(BATCH, SEQ_LEN, NUM_HEADS, HEAD_DIM)

    queries = project(w_query)
    keys_full = project(w_key)
    values_full = project(w_value)
    bias_full = causal_bias(bias_rows)

    def one_sequence(operands):
        query_seq, key_seq, value_seq = operands
        scores = jnp.einsum('qhd,khd->hqk', query_seq.astype(jnp.float32), key_seq.astype(jnp.float32))
        scores = scores * (HEAD_DIM ** -0.5) + bias_full
        attn_probs = jax.nn.softmax(scores, axis=-1).astype(jnp.bfloat16)
        context = jnp.einsum('hqk,khd->qhd', attn_probs.astype(jnp.float32), value_seq.astype(jnp.float32))
        return context.astype(jnp.bfloat16)

    context = lax.map(one_sequence, (queries, keys_full, values_full)).reshape(BATCH * SEQ_LEN, INNER)
    attn_out = jnp.dot(context, w_out, preferred_element_type=jnp.float32).reshape(BATCH, SEQ_LEN, D_MODEL)
    new_hidden = (hidden.astype(jnp.float32) + attn_out).astype(jnp.bfloat16)
    return new_hidden, jnp.swapaxes(keys_full, 1, 2), jnp.swapaxes(values_full, 1, 2)


def dense_ffn(hidden, ln_scale, w_gate, w_up, w_down):
    normed = rms_norm(hidden, ln_scale).reshape(BATCH * SEQ_LEN, D_MODEL)
    gate_pre = jnp.dot(normed, w_gate, preferred_element_type=jnp.float32)
    up_pre = jnp.dot(normed, w_up, preferred_element_type=jnp.float32)
    ffn_hidden = (jax.nn.gelu(gate_pre) * up_pre).astype(jnp.bfloat16)
    ffn_out = jnp.dot(ffn_hidden, w_down, preferred_element_type=jnp.float32).reshape(BATCH, SEQ_LEN, D_MODEL)
    return (hidden.astype(jnp.float32) + ffn_out).astype(jnp.bfloat16)


def to_groups(array_in):
    tail_dims = array_in.shape[2:]
    split_view = array_in.reshape((EP_SIZE, LOCAL_BATCH, TP_SIZE, LOCAL_SEQ) + tail_dims)
    return jnp.swapaxes(split_view, 1, 2).reshape((NUM_GROUPS, LOCAL_TOKENS) + tail_dims)


def from_groups(array_in):
    tail_dims = array_in.shape[2:]
    split_view = array_in.reshape((EP_SIZE, TP_SIZE, LOCAL_BATCH, LOCAL_SEQ) + tail_dims)
    return jnp.swapaxes(split_view, 1, 2).reshape((BATCH, SEQ_LEN) + tail_dims)


def slot_table(choices):
    experts = jnp.arange(NUM_EXPERTS, dtype=jnp.int32)
    first_hot = (choices[..., 0:1] == experts).astype(jnp.int32)
    second_hot = (choices[..., 1:2] == experts).astype(jnp.int32)
    first_pos = jnp.sum((jnp.cumsum(first_hot, axis=-2) - 1) * first_hot, axis=-1)
    second_base = jnp.cumsum(second_hot, axis=-2) - 1 + jnp.sum(first_hot, axis=-2, keepdims=True)
    second_pos = jnp.sum(second_base * second_hot, axis=-1)
    position = jnp.stack([first_pos, second_pos], axis=-1)
    return jnp.where(position < CAPACITY, choices * CAPACITY + position, NUM_EXPERTS * CAPACITY)


def dispatch(group_rows, slot_ids):
    buffer_rows = jnp.zeros((NUM_EXPERTS * CAPACITY + 1, D_MODEL), jnp.bfloat16)
    buffer_rows = buffer_rows.at[slot_ids[:, 0]].set(group_rows).at[slot_ids[:, 1]].set(group_rows)
    return buffer_rows[:-1]


def run_expert(operands):
    rows_in, weight_in, weight_out = operands
    expert_hidden = jax.nn.gelu(jnp.dot(rows_in, weight_in, preferred_element_type=jnp.float32)).astype(jnp.bfloat16)
    return jnp.dot(expert_hidden, weight_out, preferred_element_type=jnp.float32).astype(jnp.bfloat16)


def gather_rows(table_rows, slot_ids):
    return jnp.take(table_rows, slot_ids, axis=0)


def moe_layer(hidden, ln_scale, w_router, expert_in, expert_out, expert_ids):
    tok_rows = to_groups(rms_norm(hidden, ln_scale))
    choices = to_groups(expert_ids)
    logits = jnp.einsum('gnd,de->gne', tok_rows.astype(jnp.float32), w_router)
    router_probs = jax.nn.softmax(logits, axis=-1)
    picked = jnp.take_along_axis(router_probs, choices, axis=-1)
    gate_weights = picked / jnp.sum(picked, axis=-1, keepdims=True)
    slot_ids = slot_table(choices)
    buffers = jax.vmap(dispatch)(tok_rows, slot_ids)
    per_expert = jnp.swapaxes(buffers.reshape(NUM_GROUPS, NUM_EXPERTS, CAPACITY, D_MODEL), 0, 1)
    per_expert = per_expert.reshape(NUM_EXPERTS, NUM_GROUPS * CAPACITY, D_MODEL)
    expert_result = lax.map(run_expert, (per_expert, expert_in, expert_out))
    returned = jnp.swapaxes(expert_result.reshape(NUM_EXPERTS, NUM_GROUPS, CAPACITY, D_MODEL), 0, 1)
    returned = returned.reshape(NUM_GROUPS, NUM_EXPERTS * CAPACITY, D_MODEL)
    padded = jnp.concatenate([returned, jnp.zeros((NUM_GROUPS, 1, D_MODEL), jnp.bfloat16)], axis=1)
    gathered_out = jax.vmap(gather_rows)(padded, slot_ids)
    moe_sum = jnp.sum(gate_weights[..., None] * gathered_out.astype(jnp.float32), axis=2)
    return (hidden.astype(jnp.float32) + from_groups(moe_sum)).astype(jnp.bfloat16)


def reference(hidden_in, ln_attn, ln_ffn, w_query, w_key, w_value, w_out, bias_table, w_gate, w_up, w_down, w_router, expert_in, expert_out, expert_ids):
    hidden, keys_zero, values_zero = attention(hidden_in, ln_attn[0], w_query[0], w_key[0], w_value[0], w_out[0], bias_table[0])
    hidden = dense_ffn(hidden, ln_ffn[0], w_gate, w_up, w_down)
    hidden, keys_one, values_one = attention(hidden, ln_attn[1], w_query[1], w_key[1], w_value[1], w_out[1], bias_table[1])
    hidden = moe_layer(hidden, ln_ffn[1], w_router, expert_in, expert_out, expert_ids)
    return hidden, jnp.stack([keys_zero, keys_one]), jnp.stack([values_zero, values_one])
```

```python
import functools

import jax
import jax.numpy as jnp
from jax import lax
from jax.experimental import pallas as pl
from jax.experimental.pallas import tpu as pltpu
from jax.sharding import PartitionSpec as P

EXACT_BUCKETS = 16
THRESHOLDS = (18, 20, 23, 26, 30, 34, 39, 45, 51, 58, 66, 76, 86, 98, 112)
EPSILON = 1e-6
F32 = jnp.float32
BF16 = jnp.bfloat16
TP_SWAP = ((0, 1), (1, 0))
VMEM_LIMIT = 60 * 1024 * 1024


def rms_rows(rows, ln_scale):
    wide = rows.astype(F32)
    inv_rms = lax.rsqrt(jnp.mean(wide * wide, axis=-1, keepdims=True) + EPSILON)
    return (wide * inv_rms * ln_scale).astype(BF16)


def mm(a, b):
    return lax.dot_general(a, b, (((1,), (0,)), ((), ())), preferred_element_type=F32)


def mm_t(a, b):
    return lax.dot_general(a, b, (((1,), (1,)), ((), ())), preferred_element_type=F32)


def fixed(shape, index):
    return pl.BlockSpec(shape, lambda *_: index, pipeline_mode=pl.Buffered(1))


def bias_map(table, seq_len):
    pos = jnp.arange(seq_len, dtype=jnp.int32)
    rel = pos[:, None] - pos[None, :]
    bucket = jnp.minimum(jnp.maximum(rel, 0), EXACT_BUCKETS)
    for threshold in THRESHOLDS:
        bucket = bucket + (rel >= threshold).astype(jnp.int32)
    out = jnp.broadcast_to(table[:, 0][:, None, None], (table.shape[0], seq_len, seq_len))
    for k in range(1, table.shape[1]):
        out = jnp.where(bucket[None] == k, table[:, k][:, None, None], out)
    return jnp.where(rel[None] >= 0, out, -jnp.inf)


def softmax_bf16(scores):
    top = jnp.max(scores, axis=-1, keepdims=True)
    grown = jnp.exp(scores - top)
    return (grown / jnp.sum(grown, axis=-1, keepdims=True)).astype(BF16)


def attention_body(x_ref, ln_ref, wq_ref, wk_ref, wv_ref, w_other_ref, wo_ref, wo_other_ref, bias_ref, out_ref, ctx_ref):
    x = x_ref[0]
    seq_len = x.shape[0]
    half = seq_len // 2
    a = rms_rows(x, ln_ref[0])
    inner = wq_ref.shape[2]
    lanes = lax.broadcasted_iota(jnp.int32, (1, 128), 1)
    first = lanes < 64
    for side in range(2):
        if side == 0:
            q, k, v = (mm(a, ref[0]).astype(BF16) for ref in (wq_ref, wk_ref, wv_ref))
        else:
            q, k, v = (mm(a, w_other_ref[:, i * inner:(i + 1) * inner]).astype(BF16) for i in range(3))
        for pair in range(inner // 128):
            cols = slice(pair * 128, (pair + 1) * 128)
            qp, kp, vp = q[:, cols], k[:, cols], v[:, cols]
            low, high = [], []
            for sub in range(2):
                head = side * (inner // 64) + pair * 2 + sub
                keep = first if sub == 0 else jnp.logical_not(first)
                qh = jnp.where(keep, qp, jnp.zeros_like(qp))
                s_low = mm_t(qh[:half], kp[:half]) * 0.125 + bias_ref[head, :half, :half]
                s_high = mm_t(qh[half:], kp) * 0.125 + bias_ref[head, half:, :]
                low.append(mm(softmax_bf16(s_low), vp[:half]))
                high.append(mm(softmax_bf16(s_high), vp))
            at = side * inner + pair * 128
            ctx_ref[:half, at:at + 128] = jnp.where(first, low[0], low[1]).astype(BF16)
            ctx_ref[half:, at:at + 128] = jnp.where(first, high[0], high[1]).astype(BF16)
    total = mm(ctx_ref[:, :inner], wo_ref[0]) + mm(ctx_ref[:, inner:], wo_other_ref[...])
    out_ref[0] = (x.astype(F32) + total).astype(BF16)


def attention_layer(layer, x, ln, w_query, w_key, w_value, w_other, w_out, wo_other, bias):
    seqs, seq_len, d_model = x.shape
    inner = w_query.shape[2]
    own = fixed((1, d_model, inner), (layer, 0, 0))
    flops = 2 * seqs * seq_len * d_model * (4 * 2 * inner) + 4 * seqs * seq_len * seq_len * 2 * inner
    return pl.pallas_call(
        attention_body,
        grid=(seqs,),
        in_specs=[
            pl.BlockSpec((1, seq_len, d_model), lambda s: (s, 0, 0)),
            fixed((1, d_model), (0, 0)),
            own, own, own,
            fixed(w_other.shape, (0, 0)),
            fixed((1, inner, d_model), (layer, 0, 0)),
            fixed(wo_other.shape, (0, 0)),
            fixed(bias.shape, (0, 0, 0)),
        ],
        out_specs=pl.BlockSpec((1, seq_len, d_model), lambda s: (s, 0, 0)),
        out_shape=jax.ShapeDtypeStruct(x.shape, BF16),
        scratch_shapes=[pltpu.VMEM((seq_len, 2 * inner), BF16)],
        compiler_params=pltpu.CompilerParams(vmem_limit_bytes=VMEM_LIMIT),
        cost_estimate=pl.CostEstimate(flops=flops, bytes_accessed=18 << 20, transcendentals=0),
        name=f"attention{layer}",
    )(x, ln, w_query, w_key, w_value, w_other, w_out, wo_other, bias)


def ffn_body(h_ref, ln_ref, wg_ref, wu_ref, wd_ref, gu_other_ref, wd_other_ref, out_ref):
    h = h_ref[...]
    b = rms_rows(h, ln_ref[0])
    width = wg_ref.shape[1]
    own = (jax.nn.gelu(mm(b, wg_ref[...])) * mm(b, wu_ref[...])).astype(BF16)
    other = (jax.nn.gelu(mm(b, gu_other_ref[:, :width])) * mm(b, gu_other_ref[:, width:])).astype(BF16)
    total = mm(own, wd_ref[...]) + mm(other, wd_other_ref[...])
    out_ref[...] = (h.astype(F32) + total).astype(BF16)


def ffn_layer(rows, ln, w_gate, w_up, w_down, gu_other, wd_other, block=256):
    n, d_model = rows.shape
    flops = 2 * n * d_model * 6 * w_gate.shape[1]
    row_spec = pl.BlockSpec((block, d_model), lambda i: (i, 0))
    weights = [w_gate, w_up, w_down, gu_other, wd_other]
    return pl.pallas_call(
        ffn_body,
        grid=(n // block,),
        in_specs=[row_spec, fixed((1, d_model), (0, 0))] + [fixed(w.shape, (0, 0)) for w in weights],
        out_specs=row_spec,
        out_shape=jax.ShapeDtypeStruct(rows.shape, BF16),
        compiler_params=pltpu.CompilerParams(vmem_limit_bytes=VMEM_LIMIT),
        cost_estimate=pl.CostEstimate(flops=flops, bytes_accessed=7 << 20, transcendentals=0),
        name="ffn",
    )(rows, ln, *weights)


def cache_body(tp_ref, mine_ref, theirs_ref, ln_ref, wk_ref, wv_ref, *rest):
    k_ref, v_ref = rest[-2:]
    step = pl.program_id(0)
    x = jnp.where(step < pl.num_programs(0) // 2, mine_ref[0], theirs_ref[0])
    a = rms_rows(x, ln_ref[0])
    for w_ref, out_ref in ((wk_ref, k_ref), (wv_ref, v_ref)):
        full = mm(a, w_ref[0]).astype(BF16)
        for head in range(out_ref.shape[2]):
            out_ref[0, 0, head] = full[:, head * 64:(head + 1) * 64]


def cache_layer(layer, tp, mine, theirs, ln, w_key, w_value, caches=None):
    half, seq_len, d_model = mine.shape
    inner = w_key.shape[2]
    heads = inner // 64
    shape = jax.ShapeDtypeStruct((2, 2 * half, heads, seq_len, 64), BF16)

    def out_index(t, tp_ref):
        owner = jnp.where(t < half, tp_ref[0], 1 - tp_ref[0])
        return layer, owner * half + lax.rem(t, half), 0, 0, 0

    out_spec = pl.BlockSpec((1, 1, heads, seq_len, 64), out_index)
    own = fixed((1, d_model, inner), (layer, 0, 0))
    in_specs = [
        pl.BlockSpec((1, seq_len, d_model), lambda t, tp_ref: (jnp.minimum(t, half - 1), 0, 0)),
        pl.BlockSpec((1, seq_len, d_model), lambda t, tp_ref: (jnp.maximum(t - half, 0), 0, 0)),
        fixed((1, d_model), (0, 0)), own, own,
    ]
    args = [tp, mine, theirs, ln, w_key, w_value]
    aliases = {}
    if caches is not None:
        in_specs += [pl.BlockSpec(memory_space=pl.ANY)] * 2
        args += list(caches)
        aliases = {6: 0, 7: 1}
    return pl.pallas_call(
        cache_body,
        grid_spec=pltpu.PrefetchScalarGridSpec(
            num_scalar_prefetch=1, grid=(2 * half,), in_specs=in_specs, out_specs=[out_spec, out_spec]),
        out_shape=[shape, shape],
        input_output_aliases=aliases,
        compiler_params=pltpu.CompilerParams(vmem_limit_bytes=VMEM_LIMIT),
        cost_estimate=pl.CostEstimate(flops=8 * half * seq_len * d_model * inner, bytes_accessed=14 << 20, transcendentals=0),
        name=f"cache{layer}",
    )(*args)


def experts_body(dev_ref, h_ref, slot_ref, ln_ref, w_in_ref, w_out_ref, out_ref):
    h = h_ref[...].reshape(-1, h_ref.shape[-1])
    tokens = h.shape[0]
    experts = w_in_ref.shape[0]
    rows = out_ref.shape[1]
    capacity = rows // experts
    want = dev_ref[0] * rows + lax.broadcasted_iota(jnp.int32, (rows, tokens), 0)
    slots = slot_ref[0]
    pick = jnp.logical_or(slots[0:1] == want, slots[1:2] == want)
    chosen = mm(jnp.where(pick, 1.0, 0.0).astype(BF16), h)
    b = rms_rows(chosen, ln_ref[0])
    for e in range(experts):
        at = slice(e * capacity, (e + 1) * capacity)
        hid = jax.nn.gelu(mm(b[at], w_in_ref[e])).astype(BF16)
        out_ref[0, at] = mm(hid, w_out_ref[e]).astype(BF16)


def experts_layer(dev, h_all, slots, ln, expert_in, expert_out):
    tp_n, ep_n, seqs, _, positions, d_model = h_all.shape
    experts = expert_in.shape[0]
    tokens = tp_n * seqs * positions
    groups = tp_n * ep_n
    rows = experts * (4 * tokens // (experts * groups))
    flops = groups * 2 * rows * d_model * (tokens + 2 * expert_in.shape[2])
    return pl.pallas_call(
        experts_body,
        grid_spec=pltpu.PrefetchScalarGridSpec(
            num_scalar_prefetch=1,
            grid=(groups,),
            in_specs=[
                pl.BlockSpec((tp_n, 1, seqs, 1, positions, d_model), lambda g, d: (0, g % ep_n, 0, g // ep_n, 0, 0)),
                pl.BlockSpec((1, 2, tokens), lambda g, d: (g, 0, 0)),
                fixed((1, d_model), (0, 0)),
                fixed(expert_in.shape, (0, 0, 0)),
                fixed(expert_out.shape, (0, 0, 0)),
            ],
            out_specs=pl.BlockSpec((1, rows, d_model), lambda g, d: (g, 0, 0)),
        ),
        out_shape=jax.ShapeDtypeStruct((groups, rows, d_model), BF16),
        compiler_params=pltpu.CompilerParams(vmem_limit_bytes=VMEM_LIMIT),
        cost_estimate=pl.CostEstimate(flops=flops, bytes_accessed=32 << 20, transcendentals=0),
        name="experts",
    )(dev, h_all, slots, ln, expert_in, expert_out)


def combine_body(h_ref, slot_ref, gate_ref, rows_ref, out_ref):
    block = h_ref.shape[0]
    total = rows_ref.shape[0]
    columns = lax.broadcasted_iota(jnp.int32, (block, total), 1)
    out = h_ref[...].astype(F32)
    parts = []
    for c in range(2):
        pick = jnp.where(slot_ref[:, c:c + 1] == columns, 1.0, 0.0).astype(BF16)
        parts.append(gate_ref[:, c:c + 1] * mm(pick, rows_ref[...]))
    out_ref[...] = (out + (parts[0] + parts[1])).astype(BF16)


def combine_layer(h, slots, gates, rows, block=128):
    n, d_model = h.shape
    total = rows.shape[0]
    return pl.pallas_call(
        combine_body,
        grid=(n // block,),
        in_specs=[
            pl.BlockSpec((block, d_model), lambda i: (i, 0)),
            pl.BlockSpec((block, 2), lambda i: (i, 0)),
            pl.BlockSpec((block, 2), lambda i: (i, 0)),
            fixed(rows.shape, (0, 0)),
        ],
        out_specs=pl.BlockSpec((block, d_model), lambda i: (i, 0)),
        out_shape=jax.ShapeDtypeStruct(h.shape, BF16),
        compiler_params=pltpu.CompilerParams(vmem_limit_bytes=VMEM_LIMIT),
        cost_estimate=pl.CostEstimate(flops=4 * n * total * d_model, bytes_accessed=13 << 20, transcendentals=0),
        name="combine",
    )(h, slots, gates, rows)


def slot_table(choices, num_experts, capacity):
    tokens = choices.shape[0]
    experts = jnp.arange(num_experts, dtype=jnp.int32)
    hot = (choices[:, :, None] == experts).astype(BF16).reshape(tokens, 2 * num_experts)
    rows = jnp.arange(tokens, dtype=jnp.int32)
    tri = (rows[:, None] >= rows[None, :]).astype(BF16)
    upto = mm(tri, hot)
    wide = hot.astype(F32)
    first_hot, second_hot = wide[:, :num_experts], wide[:, num_experts:]
    first_pos = jnp.sum((upto[:, :num_experts] - 1.0) * first_hot, axis=-1)
    base = upto[-1:, :num_experts] - 1.0
    second_pos = jnp.sum((upto[:, num_experts:] + base) * second_hot, axis=-1)
    position = jnp.stack([first_pos, second_pos], axis=-1).astype(jnp.int32)
    return jnp.where(position < capacity, choices * capacity + position, -1)


def solution(mesh):
    act_spec = P(('dp', 'ep'), 'tp', None)
    col_spec = P(None, None, 'tp')
    row_spec = P(None, 'tp', None)
    expert_spec = P(('tp', 'ep'), None, None)
    cache_spec = P(None, ('dp', 'ep'), 'tp', None, None)
    in_specs = (act_spec, P(), P(), col_spec, col_spec, col_spec, row_spec, row_spec,
                P(None, 'tp'), P(None, 'tp'), P('tp', None), P(), expert_spec, expert_spec, act_spec)
    tp_n, ep_n = mesh.shape['tp'], mesh.shape['ep']

    def device_fn(hidden_in, ln_attn, ln_ffn, w_query, w_key, w_value, w_out, bias_table, w_gate, w_up, w_down, w_router, expert_in, expert_out, expert_ids):
        batch, positions, d_model = hidden_in.shape
        half = batch // 2
        tp, ep = lax.axis_index('tp'), lax.axis_index('ep')
        swap = lambda value: lax.ppermute(value, 'tp', TP_SWAP)
        spread = lambda value: lax.all_gather(value, 'ep', axis=0, tiled=False)

        def quarter(weight):
            rows = weight.shape[0] // ep_n
            return lax.dynamic_slice_in_dim(weight, ep * rows, rows, 0)

        def whole_seq(own, other):
            return jnp.where(tp == 0, jnp.concatenate([own, other], axis=1), jnp.concatenate([other, own], axis=1))

        def qkv_other(layer):
            part = jnp.concatenate([quarter(w[layer]) for w in (w_query, w_key, w_value)], axis=1)
            return spread(swap(part)).reshape(d_model, -1)

        kept = lax.dynamic_slice_in_dim(hidden_in, tp * half, half, 0)
        given = lax.dynamic_slice_in_dim(hidden_in, (1 - tp) * half, half, 0)

        wqkv0 = qkv_other(0)
        x0 = whole_seq(kept, swap(given))
        out_part0 = quarter(w_out[0])
        down_part = quarter(w_down)
        gu_part = jnp.concatenate([quarter(w_gate), quarter(w_up)], axis=1)
        tail0 = jnp.concatenate([out_part0, down_part, gu_part.reshape(-1, d_model)], axis=0)
        tail0 = spread(swap(tail0))
        n_out, n_down = out_part0.shape[0], down_part.shape[0]
        wo0 = tail0[:, :n_out].reshape(-1, d_model)
        wd_other = tail0[:, n_out:n_out + n_down].reshape(-1, d_model)
        gu_other = tail0[:, n_out + n_down:].reshape(d_model, -1)
        wqkv1 = qkv_other(1)
        wo1 = spread(swap(quarter(w_out[1]))).reshape(-1, d_model)
        bias_all = jnp.concatenate([bias_table, swap(bias_table)], axis=1)

        num_experts = w_router.shape[1]
        tokens = batch * positions
        capacity = 4 * tokens // num_experts
        choices = expert_ids.reshape(tokens, 2)
        slots = slot_table(choices, num_experts, capacity)
        slots_all = lax.all_gather(slots.T, ('tp', 'ep'), axis=0, tiled=False)

        h = attention_layer(0, x0, ln_attn[0:1], w_query, w_key, w_value, wqkv0, w_out, wo0, bias_map(bias_all[0], tp_n * positions))
        h1 = ffn_layer(h.reshape(tokens, d_model), ln_ffn[0:1], w_gate, w_up, w_down, gu_other, wd_other).reshape(h.shape)
        h2 = attention_layer(1, h1, ln_attn[1:2], w_query, w_key, w_value, wqkv1, w_out, wo1, bias_map(bias_all[1], tp_n * positions))

        tp_arr = tp.reshape(1).astype(jnp.int32)
        x0_theirs = whole_seq(given, swap(kept))
        caches = cache_layer(0, tp_arr, x0, x0_theirs, ln_attn[0:1], w_key, w_value)
        k_cache, v_cache = cache_layer(1, tp_arr, h1, swap(h1), ln_attn[1:2], w_key, w_value, caches)

        h_all = lax.all_gather(h2, ('tp', 'ep'), axis=0, tiled=False)
        h_all = h_all.reshape(tp_n, ep_n, half, tp_n, positions, d_model)
        dev = (tp * ep_n + ep).reshape(1).astype(jnp.int32)
        results = experts_layer(dev, h_all, slots_all, ln_ffn[1:2], expert_in, expert_out)
        returned = lax.all_to_all(results, ('tp', 'ep'), 0, 0, tiled=True).reshape(num_experts * capacity, d_model)

        h_own = lax.dynamic_slice(h_all, (0, ep, 0, tp, 0, 0), (tp_n, 1, half, 1, positions, d_model)).reshape(tokens, d_model)
        b = rms_rows(h_own, ln_ffn[1])
        logits = jnp.dot(b.astype(F32), w_router, precision=lax.Precision.HIGHEST)
        probs = jax.nn.softmax(logits, axis=-1)
        hot = choices[:, :, None] == jnp.arange(num_experts, dtype=jnp.int32)
        picked = jnp.sum(jnp.where(hot, probs[:, None, :], 0.0), axis=-1)
        gates = picked / jnp.sum(picked, axis=-1, keepdims=True)
        hidden = combine_layer(h_own, slots, gates, returned).reshape(hidden_in.shape)
        return hidden, k_cache, v_cache

    return jax.shard_map(device_fn, mesh=mesh, in_specs=in_specs, out_specs=(act_spec, cache_spec, cache_spec), check_vma=False)
```

```python
import functools

import jax
import jax.numpy as jnp
from jax import lax
from jax.experimental import pallas as pl
from jax.experimental.pallas import tpu as pltpu
from jax.sharding import PartitionSpec as P

EXACT_BUCKETS = 16
THRESHOLDS = (18, 20, 23, 26, 30, 34, 39, 45, 51, 58, 66, 76, 86, 98, 112)
EPSILON = 1e-6
F32 = jnp.float32
BF16 = jnp.bfloat16
TP_SWAP = ((0, 1), (1, 0))
VMEM_LIMIT = 60 * 1024 * 1024


def rms_rows(rows, ln_scale):
    wide = rows.astype(F32)
    inv_rms = lax.rsqrt(jnp.mean(wide * wide, axis=-1, keepdims=True) + EPSILON)
    return (wide * inv_rms * ln_scale).astype(BF16)


def mm(a, b):
    return lax.dot_general(a, b, (((1,), (0,)), ((), ())), preferred_element_type=F32)


def mm_t(a, b):
    return lax.dot_general(a, b, (((1,), (1,)), ((), ())), preferred_element_type=F32)


def fixed(shape, index):
    return pl.BlockSpec(shape, lambda *_: index, pipeline_mode=pl.Buffered(1))


def bias_map(table, seq_len):
    pos = jnp.arange(seq_len, dtype=jnp.int32)
    rel = pos[:, None] - pos[None, :]
    bucket = jnp.minimum(jnp.maximum(rel, 0), EXACT_BUCKETS)
    for threshold in THRESHOLDS:
        bucket = bucket + (rel >= threshold).astype(jnp.int32)
    out = jnp.broadcast_to(table[:, 0][:, None, None], (table.shape[0], seq_len, seq_len))
    for k in range(1, table.shape[1]):
        out = jnp.where(bucket[None] == k, table[:, k][:, None, None], out)
    return jnp.where(rel[None] >= 0, out, -jnp.inf)


def softmax_bf16(scores):
    top = jnp.max(scores, axis=-1, keepdims=True)
    grown = jnp.exp(scores - top)
    return (grown / jnp.sum(grown, axis=-1, keepdims=True)).astype(BF16)


def attention_body(x_ref, ln_ref, wq_ref, wk_ref, wv_ref, w_other_ref, wo_ref, wo_other_ref, bias_ref, out_ref, ctx_ref):
    x = x_ref[0]
    seq_len = x.shape[0]
    half = seq_len // 2
    a = rms_rows(x, ln_ref[0])
    inner = wq_ref.shape[2]
    lanes = lax.broadcasted_iota(jnp.int32, (1, 128), 1)
    first = lanes < 64
    for side in range(2):
        if side == 0:
            q, k, v = (mm(a, ref[0]).astype(BF16) for ref in (wq_ref, wk_ref, wv_ref))
        else:
            q, k, v = (mm(a, w_other_ref[:, i * inner:(i + 1) * inner]).astype(BF16) for i in range(3))
        for pair in range(inner // 128):
            cols = slice(pair * 128, (pair + 1) * 128)
            qp, kp, vp = q[:, cols], k[:, cols], v[:, cols]
            low, high = [], []
            for sub in range(2):
                head = side * (inner // 64) + pair * 2 + sub
                keep = first if sub == 0 else jnp.logical_not(first)
                qh = jnp.where(keep, qp, jnp.zeros_like(qp))
                s_low = mm_t(qh[:half], kp[:half]) * 0.125 + bias_ref[head, :half, :half]
                s_high = mm_t(qh[half:], kp) * 0.125 + bias_ref[head, half:, :]
                low.append(mm(softmax_bf16(s_low), vp[:half]))
                high.append(mm(softmax_bf16(s_high), vp))
            at = side * inner + pair * 128
            ctx_ref[:half, at:at + 128] = jnp.where(first, low[0], low[1]).astype(BF16)
            ctx_ref[half:, at:at + 128] = jnp.where(first, high[0], high[1]).astype(BF16)
    total = mm(ctx_ref[:, :inner], wo_ref[0]) + mm(ctx_ref[:, inner:], wo_other_ref[...])
    out_ref[0] = (x.astype(F32) + total).astype(BF16)


def attention_layer(layer, x, ln, w_query, w_key, w_value, w_other, w_out, wo_other, bias):
    seqs, seq_len, d_model = x.shape
    inner = w_query.shape[2]
    own = fixed((1, d_model, inner), (layer, 0, 0))
    flops = 2 * seqs * seq_len * d_model * (4 * 2 * inner) + 4 * seqs * seq_len * seq_len * 2 * inner
    return pl.pallas_call(
        attention_body,
        grid=(seqs,),
        in_specs=[
            pl.BlockSpec((1, seq_len, d_model), lambda s: (s, 0, 0)),
            fixed((1, d_model), (0, 0)),
            own, own, own,
            fixed(w_other.shape, (0, 0)),
            fixed((1, inner, d_model), (layer, 0, 0)),
            fixed(wo_other.shape, (0, 0)),
            fixed(bias.shape, (0, 0, 0)),
        ],
        out_specs=pl.BlockSpec((1, seq_len, d_model), lambda s: (s, 0, 0)),
        out_shape=jax.ShapeDtypeStruct(x.shape, BF16),
        scratch_shapes=[pltpu.VMEM((seq_len, 2 * inner), BF16)],
        compiler_params=pltpu.CompilerParams(vmem_limit_bytes=VMEM_LIMIT),
        cost_estimate=pl.CostEstimate(flops=flops, bytes_accessed=18 << 20, transcendentals=0),
        name=f"attention{layer}",
    )(x, ln, w_query, w_key, w_value, w_other, w_out, wo_other, bias)


def ffn_body(h_ref, ln_ref, wg_ref, wu_ref, wd_ref, gu_other_ref, wd_other_ref, out_ref):
    h = h_ref[...]
    b = rms_rows(h, ln_ref[0])
    width = wg_ref.shape[1]
    own = (jax.nn.gelu(mm(b, wg_ref[...])) * mm(b, wu_ref[...])).astype(BF16)
    other = (jax.nn.gelu(mm(b, gu_other_ref[:, :width])) * mm(b, gu_other_ref[:, width:])).astype(BF16)
    total = mm(own, wd_ref[...]) + mm(other, wd_other_ref[...])
    out_ref[...] = (h.astype(F32) + total).astype(BF16)


def ffn_layer(rows, ln, w_gate, w_up, w_down, gu_other, wd_other, block=256):
    n, d_model = rows.shape
    flops = 2 * n * d_model * 6 * w_gate.shape[1]
    row_spec = pl.BlockSpec((block, d_model), lambda i: (i, 0))
    weights = [w_gate, w_up, w_down, gu_other, wd_other]
    return pl.pallas_call(
        ffn_body,
        grid=(n // block,),
        in_specs=[row_spec, fixed((1, d_model), (0, 0))] + [fixed(w.shape, (0, 0)) for w in weights],
        out_specs=row_spec,
        out_shape=jax.ShapeDtypeStruct(rows.shape, BF16),
        compiler_params=pltpu.CompilerParams(vmem_limit_bytes=VMEM_LIMIT),
        cost_estimate=pl.CostEstimate(flops=flops, bytes_accessed=7 << 20, transcendentals=0),
        name="ffn",
    )(rows, ln, *weights)


def axis_neighbours(tp, ep):
    core = lax.rem(ep, 2)
    beside = ep + 1 - 2 * core
    return beside, lax.rem(ep + 2, 4), lax.rem(beside + 2, 4)


def remote(src, dst, send, recv, tp, ep):
    return pltpu.make_async_remote_copy(
        src_ref=src, dst_ref=dst, send_sem=send, recv_sem=recv,
        device_id=(lax.axis_index('dp'), tp, ep), device_id_type=pl.DeviceIdType.MESH)


def moe_body(h2_ref, h1_ref, x0_ref, x0t_ref, slot_row_ref, slot_col_ref, ids_ref, ln_ref, ln_attn_ref, router_ref,
             w_in_hbm, w_out_hbm, wk_hbm, wv_hbm,
             out_ref, k_ref, v_ref, h1t_ref,
             hall, res, ret, w_in, w_out, wkv, acc, slots_all, gates, xbuf, kvbuf,
             in_sem, cache_sem, store_sem, slot_send, slot_recv, hs_send, hs_recv, ret_send, ret_recv, h1_send, h1_recv):
    tp, ep = lax.axis_index('tp'), lax.axis_index('ep')
    other = 1 - tp
    ep1, ep2, ep3 = axis_neighbours(tp, ep)
    me = tp * 4 + ep
    seqs, seq_len, d_model = h2_ref.shape
    tokens = acc.shape[0]
    rows = res.shape[1]
    half_pos = seq_len // 2
    experts = w_in.shape[0]
    capacity = rows // experts

    loads = [pltpu.make_async_copy(a, b, in_sem.at[n]) for n, (a, b) in enumerate((
        (x0_ref, xbuf), (wk_hbm, wkv.at[0]), (wv_hbm, wkv.at[1]), (h2_ref, hall.at[me]),
        (w_in_hbm, w_in), (w_out_hbm, w_out)))]
    for load in loads:
        load.start()
    slots_all[me] = slot_row_ref[...]

    barrier = pltpu.get_barrier_semaphore()
    peers = [(other, ep), (tp, ep2), (tp, ep1), (other, ep1), (other, ep2), (tp, ep3), (other, ep3)]
    for peer_tp, peer_ep in peers:
        pl.semaphore_signal(barrier, inc=1, device_id=(lax.axis_index('dp'), peer_tp, peer_ep), device_id_type=pl.DeviceIdType.MESH)
    pl.semaphore_wait(barrier, len(peers))

    def block(owner):
        return hall.at[owner]

    send_y = remote(h2_ref, block(me), hs_send.at[0], hs_recv.at[me], other, ep)
    send_x = remote(h2_ref, block(me), hs_send.at[1], hs_recv.at[me], tp, ep2)
    send_c = remote(h2_ref, block(me), hs_send.at[2], hs_recv.at[me], tp, ep1)
    for copy in (send_y, send_x, send_c):
        copy.start()
    slot_copies = [remote(slot_row_ref, slots_all.at[me], slot_send.at[n], slot_recv.at[me], *peer) for n, peer in enumerate(peers)]
    for copy in slot_copies:
        copy.start()
    send_h1 = remote(h1_ref, h1t_ref, h1_send, h1_recv, other, ep)
    send_h1.start()

    def arrived(ref, sem):
        remote(ref, ref, hs_send.at[0], sem, tp, ep).wait_recv()

    def block_arrived(owner):
        arrived(hall.at[owner], hs_recv.at[owner])

    def cache_part(source, layer, owner, load=None):
        if load is None:
            load = pltpu.make_async_copy(source, xbuf, cache_sem)
            load.start()
        load.wait()

        @pl.loop(0, seqs)
        def _(s):
            a = rms_rows(xbuf[s], ln_attn_ref[layer])
            for n, ref in enumerate((k_ref, v_ref)):
                full = mm(a, wkv[n, layer])
                kvbuf[s, n] = full.T.astype(BF16).reshape(kvbuf.shape[2:])
                pltpu.make_async_copy(kvbuf.at[s, n], ref.at[layer, owner * seqs + s], store_sem.at[s, n]).start()

        @pl.loop(0, seqs)
        def _(s):
            for n, ref in enumerate((k_ref, v_ref)):
                pltpu.make_async_copy(kvbuf.at[s, n], ref.at[layer, owner * seqs + s], store_sem.at[s, n]).wait()

    loads[1].wait()
    loads[2].wait()
    cache_part(x0_ref, 0, tp, loads[0])
    cache_part(x0t_ref, 0, other)
    cache_part(h1_ref, 1, tp)

    y_owner, x_owner, c_owner = other * 4 + ep, tp * 4 + ep2, tp * 4 + ep1
    yx_owner, yc_owner, xc_owner, yxc_owner = other * 4 + ep2, other * 4 + ep1, tp * 4 + ep3, other * 4 + ep3
    block_arrived(y_owner)
    fwd_yx = remote(block(y_owner), block(y_owner), hs_send.at[3], hs_recv.at[y_owner], tp, ep2)
    fwd_yc = remote(block(y_owner), block(y_owner), hs_send.at[4], hs_recv.at[y_owner], tp, ep1)
    fwd_yx.start()
    fwd_yc.start()
    loads[3].wait()

    def own_tokens(owner):
        return hall[owner, :, pl.ds(pl.multiple_of(tp * half_pos, half_pos), half_pos), :].reshape(tokens // 2, d_model)

    for part in range(2):
        at = slice(part * (tokens // 2), (part + 1) * (tokens // 2))
        h_own = own_tokens(part * 4 + ep)
        acc[at] = h_own.astype(F32)
        b = rms_rows(h_own, ln_ref[0])
        logits = jnp.dot(b.astype(F32), router_ref[...], precision=lax.Precision.HIGHEST, preferred_element_type=F32)
        grown = jnp.exp(logits - jnp.max(logits, axis=-1, keepdims=True))
        probs = grown / jnp.sum(grown, axis=-1, keepdims=True)
        lanes = lax.broadcasted_iota(jnp.int32, probs.shape, 1)
        picked = [jnp.sum(jnp.where(ids_ref[at, c:c + 1] == lanes, probs, 0.0), axis=-1, keepdims=True) for c in range(2)]
        both = picked[0] + picked[1]
        gates[at, 0:1] = picked[0] / both
        gates[at, 1:2] = picked[1] / both

    block_arrived(x_owner)
    fwd_xc = remote(block(x_owner), block(x_owner), hs_send.at[5], hs_recv.at[x_owner], tp, ep1)
    fwd_xc.start()
    for peer_tp, peer_ep in peers:
        arrived(slots_all.at[peer_tp * 4 + peer_ep], slot_recv.at[peer_tp * 4 + peer_ep])
    loads[4].wait()
    loads[5].wait()

    def run_group(i, k):
        dest = k * 4 + i
        slots = slots_all[dest]
        want = me * rows + lax.broadcasted_iota(jnp.int32, (rows, tokens // 2), 0)
        chosen = None
        for part in range(2):
            h = hall[part * 4 + i, :, pl.ds(pl.multiple_of(k * half_pos, half_pos), half_pos), :].reshape(tokens // 2, d_model)
            at = slice(part * (tokens // 2), (part + 1) * (tokens // 2))
            pick = jnp.logical_or(slots[0:1, at] == want, slots[1:2, at] == want)
            term = mm(jnp.where(pick, 1.0, 0.0).astype(BF16), h)
            chosen = term if chosen is None else chosen + term
        b = rms_rows(chosen, ln_ref[0])
        for e in range(experts):
            at = slice(e * capacity, (e + 1) * capacity)
            hid = jax.nn.gelu(mm(b[at], w_in[e])).astype(BF16)
            res[dest, at] = mm(hid, w_out[e]).astype(BF16)
        return dest

    def give_back(i, k):
        dest = k * 4 + i
        return remote(res.at[dest], ret.at[me], ret_send.at[dest], ret_recv.at[me], k, i)

    def add_rows(source_ref, owner):
        step = 256

        @pl.loop(0, tokens // step)
        def _(r):
            at = pl.ds(pl.multiple_of(r * step, step), step)
            columns = owner * rows + lax.broadcasted_iota(jnp.int32, (step, rows), 1)
            total = acc[at, :]
            for c in range(2):
                pick = jnp.where(slot_col_ref[at, c:c + 1] == columns, 1.0, 0.0).astype(BF16)
                total = total + gates[at, c:c + 1] * mm(pick, source_ref[...])
            acc[at, :] = total

    block_arrived(c_owner)
    block_arrived(yc_owner)

    @pl.loop(0, 4)
    def _(t):
        late = t // 2
        beside = lax.rem((t + 1) // 2, 2)
        i = ep + beside * (ep1 - ep)
        k = late * tp + (1 - late) * other
        run_group(i, k)

        @pl.when(t < 3)
        def _():
            give_back(i, k).start()

    add_rows(res.at[me], me)

    block_arrived(yx_owner)
    fwd_yxc = remote(block(yx_owner), block(yx_owner), hs_send.at[6], hs_recv.at[yx_owner], tp, ep1)
    fwd_yxc.start()

    def far_groups(i):
        @pl.loop(0, 2)
        def _(t):
            k = t * tp + (1 - t) * other
            run_group(i, k)
            give_back(i, k).start()

    far_groups(ep2)
    block_arrived(xc_owner)
    block_arrived(yxc_owner)
    far_groups(ep3)

    arrived(h1t_ref, h1_recv)
    cache_part(h1t_ref, 1, other)

    for peer_tp, peer_ep in ((tp, ep1), (other, ep), (other, ep1), (other, ep2), (tp, ep2), (other, ep3), (tp, ep3)):
        owner = peer_tp * 4 + peer_ep
        arrived(ret.at[owner], ret_recv.at[owner])
        add_rows(ret.at[owner], owner)
    out_ref[...] = acc[...].astype(BF16)

    for copy in (send_y, send_x, send_c, fwd_yx, fwd_yc, fwd_xc, fwd_yxc, send_h1):
        copy.wait_send()
    for copy in slot_copies:
        copy.wait_send()
    for peer_tp, peer_ep in peers:
        give_back(peer_ep, peer_tp).wait_send()


def moe_layer(h2, h1, x0, x0t, slots, choices, ln, ln_attn, w_router, expert_in, expert_out, w_key, w_value):
    seqs, seq_len, d_model = h2.shape
    tokens = seqs * seq_len
    experts, _, d_ff = expert_in.shape
    groups = 8
    rows = experts * 4 * tokens // (experts * groups)
    inner = w_key.shape[2]
    heads = inner // 64
    any_spec = pl.BlockSpec(memory_space=pl.ANY)
    vmem_spec = pl.BlockSpec(memory_space=pltpu.VMEM)
    cache_shape = jax.ShapeDtypeStruct((2, 2 * seqs, heads, 64, seq_len), BF16)
    dma = pltpu.SemaphoreType.DMA
    return pl.pallas_call(
        moe_body,
        in_specs=[any_spec] * 4 + [vmem_spec] * 6 + [any_spec] * 4,
        out_specs=[vmem_spec, any_spec, any_spec, any_spec],
        out_shape=[jax.ShapeDtypeStruct((tokens, d_model), BF16), cache_shape, cache_shape, jax.ShapeDtypeStruct(h1.shape, BF16)],
        scratch_shapes=[
            pltpu.VMEM((groups,) + h2.shape, BF16),
            pltpu.VMEM((groups, rows, d_model), BF16),
            pltpu.VMEM((groups, rows, d_model), BF16),
            pltpu.VMEM(expert_in.shape, BF16),
            pltpu.VMEM(expert_out.shape, BF16),
            pltpu.VMEM((2, 2, d_model, inner), BF16),
            pltpu.VMEM((tokens, d_model), F32),
            pltpu.VMEM((groups, 2, tokens), jnp.int32),
            pltpu.VMEM((tokens, 2), F32),
            pltpu.VMEM(h1.shape, BF16),
            pltpu.VMEM((seqs, 2, heads, 64, seq_len), BF16),
            dma((6,)), dma, dma((seqs, 2)), dma((7,)), dma((groups,)), dma((7,)), dma((groups,)),
            dma((groups,)), dma((groups,)), dma, dma,
        ],
        compiler_params=pltpu.CompilerParams(vmem_limit_bytes=67043328, collective_id=2, has_side_effects=True),
        cost_estimate=pl.CostEstimate(flops=40_000_000_000, bytes_accessed=64 << 20, transcendentals=0),
        name="moe",
    )(h2, h1, x0, x0t, slots.T, slots, choices, ln, ln_attn, w_router, expert_in, expert_out, w_key, w_value)


def slot_table(choices, num_experts, capacity):
    tokens = choices.shape[0]
    experts = jnp.arange(num_experts, dtype=jnp.int32)
    hot = (choices[:, :, None] == experts).astype(BF16).reshape(tokens, 2 * num_experts)
    rows = jnp.arange(tokens, dtype=jnp.int32)
    tri = (rows[:, None] >= rows[None, :]).astype(BF16)
    upto = mm(tri, hot)
    wide = hot.astype(F32)
    first_hot, second_hot = wide[:, :num_experts], wide[:, num_experts:]
    first_pos = jnp.sum((upto[:, :num_experts] - 1.0) * first_hot, axis=-1)
    base = upto[-1:, :num_experts] - 1.0
    second_pos = jnp.sum((upto[:, num_experts:] + base) * second_hot, axis=-1)
    position = jnp.stack([first_pos, second_pos], axis=-1).astype(jnp.int32)
    return jnp.where(position < capacity, choices * capacity + position, -1)


def solution(mesh):
    act_spec = P(('dp', 'ep'), 'tp', None)
    col_spec = P(None, None, 'tp')
    row_spec = P(None, 'tp', None)
    expert_spec = P(('tp', 'ep'), None, None)
    cache_spec = P(None, ('dp', 'ep'), 'tp', None, None)
    in_specs = (act_spec, P(), P(), col_spec, col_spec, col_spec, row_spec, row_spec,
                P(None, 'tp'), P(None, 'tp'), P('tp', None), P(), expert_spec, expert_spec, act_spec)
    tp_n, ep_n = mesh.shape['tp'], mesh.shape['ep']

    def device_fn(hidden_in, ln_attn, ln_ffn, w_query, w_key, w_value, w_out, bias_table, w_gate, w_up, w_down, w_router, expert_in, expert_out, expert_ids):
        batch, positions, d_model = hidden_in.shape
        half = batch // 2
        tp, ep = lax.axis_index('tp'), lax.axis_index('ep')
        swap = lambda value: lax.ppermute(value, 'tp', TP_SWAP)
        spread = lambda value: lax.all_gather(value, 'ep', axis=0, tiled=False)

        def quarter(weight):
            rows = weight.shape[0] // ep_n
            return lax.dynamic_slice_in_dim(weight, ep * rows, rows, 0)

        def whole_seq(own, other):
            return jnp.where(tp == 0, jnp.concatenate([own, other], axis=1), jnp.concatenate([other, own], axis=1))

        def qkv_other(layer):
            part = jnp.concatenate([quarter(w[layer]) for w in (w_query, w_key, w_value)], axis=1)
            return spread(swap(part)).reshape(d_model, -1)

        kept = lax.dynamic_slice_in_dim(hidden_in, tp * half, half, 0)
        given = lax.dynamic_slice_in_dim(hidden_in, (1 - tp) * half, half, 0)

        wqkv0 = qkv_other(0)
        x0 = whole_seq(kept, swap(given))
        out_part0 = quarter(w_out[0])
        down_part = quarter(w_down)
        gu_part = jnp.concatenate([quarter(w_gate), quarter(w_up)], axis=1)
        tail0 = jnp.concatenate([out_part0, down_part, gu_part.reshape(-1, d_model)], axis=0)
        tail0 = spread(swap(tail0))
        n_out, n_down = out_part0.shape[0], down_part.shape[0]
        wo0 = tail0[:, :n_out].reshape(-1, d_model)
        wd_other = tail0[:, n_out:n_out + n_down].reshape(-1, d_model)
        gu_other = tail0[:, n_out + n_down:].reshape(d_model, -1)
        wqkv1 = qkv_other(1)
        wo1 = spread(swap(quarter(w_out[1]))).reshape(-1, d_model)
        bias_all = jnp.concatenate([bias_table, swap(bias_table)], axis=1)

        num_experts = w_router.shape[1]
        tokens = batch * positions
        capacity = 4 * tokens // num_experts
        choices = expert_ids.reshape(tokens, 2)
        slots = slot_table(choices, num_experts, capacity)

        h = attention_layer(0, x0, ln_attn[0:1], w_query, w_key, w_value, wqkv0, w_out, wo0, bias_map(bias_all[0], tp_n * positions))
        h1 = ffn_layer(h.reshape(tokens, d_model), ln_ffn[0:1], w_gate, w_up, w_down, gu_other, wd_other).reshape(h.shape)
        h2 = attention_layer(1, h1, ln_attn[1:2], w_query, w_key, w_value, wqkv1, w_out, wo1, bias_map(bias_all[1], tp_n * positions))

        x0_theirs = whole_seq(given, swap(kept))
        hidden, k_cache, v_cache, _ = moe_layer(
            h2, h1, x0, x0_theirs, slots, choices, ln_ffn[1:2], ln_attn, w_router, expert_in, expert_out, w_key, w_value)
        return hidden.reshape(hidden_in.shape), jnp.swapaxes(k_cache, 3, 4), jnp.swapaxes(v_cache, 3, 4)

    return jax.shard_map(device_fn, mesh=mesh, in_specs=in_specs, out_specs=(act_spec, cache_spec, cache_spec), check_vma=False)
```

```python
import jax
import jax.numpy as jnp
from jax import lax
from jax.experimental import pallas as pl
from jax.experimental.pallas import tpu as pltpu
from jax.sharding import PartitionSpec as P

EXACT_BUCKETS = 16
THRESHOLDS = (18, 20, 23, 26, 30, 34, 39, 45, 51, 58, 66, 76, 86, 98, 112)
EPSILON = 1e-6
F32 = jnp.float32
BF16 = jnp.bfloat16
VMEM_LIMIT = 60 * 1024 * 1024


def rms_rows(rows, ln_scale):
    wide = rows.astype(F32)
    inv_rms = lax.rsqrt(jnp.mean(wide * wide, axis=-1, keepdims=True) + EPSILON)
    return (wide * inv_rms * ln_scale).astype(BF16)


def mm(a, b):
    return lax.dot_general(a, b, (((1,), (0,)), ((), ())), preferred_element_type=F32)


def mm_t(a, b):
    return lax.dot_general(a, b, (((1,), (1,)), ((), ())), preferred_element_type=F32)


def bias_rows(table, seq_len):
    at = jnp.arange(2 * seq_len, dtype=jnp.int32)
    rel = jnp.where(at == 0, 0, 2 * seq_len - at)
    bucket = jnp.minimum(rel, EXACT_BUCKETS)
    for threshold in THRESHOLDS:
        bucket = bucket + (rel >= threshold).astype(jnp.int32)
    out = jnp.broadcast_to(table[..., 0:1], table.shape[:-1] + (2 * seq_len,))
    for k in range(1, table.shape[-1]):
        out = jnp.where(bucket == k, table[..., k:k + 1], out)
    return jnp.where(rel < seq_len, out, -jnp.inf)


def softmax_bf16(scores):
    top = jnp.max(scores, axis=-1, keepdims=True)
    grown = jnp.exp(scores - top)
    return (grown * (1.0 / jnp.sum(grown, axis=-1, keepdims=True))).astype(BF16)


def axis_neighbours(tp, ep):
    core = lax.rem(ep, 2)
    beside = ep + 1 - 2 * core
    return beside, lax.rem(ep + 2, 4), lax.rem(beside + 2, 4)


def remote(src, dst, send, recv, tp, ep):
    return pltpu.make_async_remote_copy(
        src_ref=src, dst_ref=dst, send_sem=send, recv_sem=recv,
        device_id=(lax.axis_index('dp'), tp, ep), device_id_type=pl.DeviceIdType.MESH)


def layers_body(hid_ref, ln_attn_ref, ln_ffn_ref, wq_hbm, wk_hbm, wv_hbm, wo_hbm, u_ref, wg_hbm, wu_hbm, wd_hbm,
                h1_ref, h2_ref, x0_ref, x0t_ref,
                x, a_ref, acc, w, wo, gu, wd, u_other, bias_low, bias_high, qkv, ctx, stage,
                in_sem, own_sem, out_sem, misc_send, misc_recv, y_send, y_recv, x_send, x_recv, c_send, c_recv, d_send, d_recv):
    tp, ep = lax.axis_index('tp'), lax.axis_index('ep')
    other = 1 - tp
    ep1, ep2, ep3 = axis_neighbours(tp, ep)
    seqs, seq_len, d_model = x.shape
    half = seq_len // 2
    tokens = seqs * seq_len
    quad = qkv.shape[2]

    def part(count, quarter):
        return pl.ds(pl.multiple_of(quarter * count, count), count)

    my_pos = part(half, tp)
    mine = hid_ref.at[pl.ds(tp * seqs, seqs)]
    theirs = hid_ref.at[pl.ds(other * seqs, seqs)]

    sources, places = [], []
    for layer in range(2):
        for kind, hbm in enumerate((wq_hbm, wk_hbm, wv_hbm)):
            sources.append(hbm.at[layer, :, part(128, ep)])
            places.append(lambda q, layer=layer, kind=kind: w.at[layer, 1, kind, :, part(128, q)])
        sources.append(wo_hbm.at[layer, part(128, ep), :])
        places.append(lambda q, layer=layer: wo.at[layer, 1, part(128, q), :])
        if layer == 0:
            for kind, hbm in enumerate((wg_hbm, wu_hbm)):
                sources.append(hbm.at[part(256, ep), :])
                places.append(lambda q, kind=kind: gu.at[1, kind, part(256, q), :])
            sources.append(wd_hbm.at[part(64, ep), :])
            places.append(lambda q: wd.at[1, part(64, q), :])

    own_x = pltpu.make_async_copy(mine, x.at[:, my_pos, :], in_sem.at[0])
    own_stage = pltpu.make_async_copy(theirs, stage, in_sem.at[1])
    own_x.start()
    own_loads = []
    for layer in range(2):
        for kind, hbm in enumerate((wq_hbm, wk_hbm, wv_hbm)):
            own_loads.append((hbm.at[layer], w.at[layer, 0, kind]))
        own_loads.append((wo_hbm.at[layer], wo.at[layer, 0]))
        if layer == 0:
            own_loads += [(wg_hbm, gu.at[0, 0]), (wu_hbm, gu.at[0, 1]), (wd_hbm, wd.at[0])]
    own_loads = [pltpu.make_async_copy(s, d, own_sem.at[n]) for n, (s, d) in enumerate(own_loads)]
    for load in own_loads:
        load.start()
    own_stage.start()

    barrier = pltpu.get_barrier_semaphore()
    for peer_tp, peer_ep in ((other, ep), (tp, ep2), (tp, ep1)):
        pl.semaphore_signal(barrier, inc=1, device_id=(lax.axis_index('dp'), peer_tp, peer_ep), device_id_type=pl.DeviceIdType.MESH)
    pl.semaphore_wait(barrier, 3)

    def arrived(ref, sem):
        remote(ref, ref, misc_send.at[0], sem, tp, ep).wait_recv()

    pieces = range(len(sources))
    send_entry = remote(theirs, x.at[:, my_pos, :], misc_send.at[0], misc_recv.at[0], other, ep)
    send_u = remote(u_ref, u_other, misc_send.at[1], misc_recv.at[1], other, ep)
    send_rest = remote(mine, x0t_ref.at[:, my_pos, :], misc_send.at[2], misc_recv.at[2], other, ep)
    y_copies = [remote(sources[n], places[n](ep), y_send.at[n], y_recv.at[n], other, ep) for n in pieces]
    x_copies = [remote(places[n](ep), places[n](ep), x_send.at[n], x_recv.at[n], tp, ep2) for n in pieces]
    c_copies = [remote(places[n](ep), places[n](ep), c_send.at[n], c_recv.at[n], tp, ep1) for n in pieces]
    d_copies = [remote(places[n](ep2), places[n](ep2), d_send.at[n], d_recv.at[n], tp, ep1) for n in pieces]
    send_u.start()
    send_entry.start()
    for copy in y_copies:
        copy.start()
    send_rest.start()

    def pass_on(n):
        arrived(places[n](ep), y_recv.at[n])
        x_copies[n].start()
        c_copies[n].start()

    def pass_across(n):
        arrived(places[n](ep2), x_recv.at[n])
        d_copies[n].start()

    def complete(n):
        arrived(places[n](ep1), c_recv.at[n])
        arrived(places[n](ep3), d_recv.at[n])

    def build_bias(rows_ref, side):
        @pl.loop(0, 8)
        def _(n):
            layer, pair = n // 4, lax.rem(n, 4)
            for sub in range(2):
                row = rows_ref[layer, pair * 2 + sub]
                wide = pltpu.roll(jnp.broadcast_to(row, (seq_len, 2 * seq_len)), 0, 1, stride=1, stride_axis=0)
                at = slice(sub * half, (sub + 1) * half)
                place = layer * 8 + side * 4 + pair
                bias_low[place, at, :] = wide[:half, :half]
                bias_high[place, at, :] = wide[half:, :seq_len]

    def begin_layer(layer):
        @pl.loop(0, seqs)
        def _(s):
            rows = part(seq_len, s)
            a_ref[rows, :] = rms_rows(x[s], ln_attn_ref[layer])
            acc[rows, :] = x[s].astype(F32)

    def end_layer():
        @pl.loop(0, seqs)
        def _(s):
            x[s] = acc[part(seq_len, s), :].astype(BF16)

    first = lax.broadcasted_iota(jnp.int32, (1, 128), 1) < 64

    def heads(layer, side, block):
        cols = slice(block * quad, (block + 1) * quad)
        for kind in range(3):
            qkv[kind] = mm(a_ref[...], w[layer, side, kind, :, cols]).astype(BF16)

        @pl.loop(0, seqs)
        def _(s):
            rows = part(seq_len, s)
            for pair in range(quad // 128):
                lanes = slice(pair * 128, (pair + 1) * 128)
                place = layer * 8 + side * 4 + block * (quad // 128) + pair
                q, k, v = (qkv[kind, rows, lanes] for kind in range(3))
                none = jnp.zeros_like(q[:half])
                outs = []
                for upper in range(2):
                    qs = q[half:] if upper else q[:half]
                    ks, vs = (k, v) if upper else (k[:half], v[:half])
                    both = jnp.concatenate([jnp.where(first, qs, none), jnp.where(first, none, qs)], axis=0)
                    bias = bias_high[place] if upper else bias_low[place]
                    got = mm(softmax_bf16(mm_t(both, ks) * 0.125 + bias), vs)
                    outs.append(jnp.where(first, got[:half], got[half:]))
                ctx[rows, lanes] = jnp.concatenate(outs, axis=0).astype(BF16)

        @pl.loop(0, seqs)
        def _(s):
            rows = part(seq_len, s)
            acc[rows, :] += mm(ctx[rows, :], wo[layer, side, cols, :])

    def dense(s):
        h = x[s]
        b = rms_rows(h, ln_ffn_ref[0])
        total = h.astype(F32)
        for side in range(2):
            hid = (jax.nn.gelu(mm(b, gu[side, 0])) * mm(b, gu[side, 1])).astype(BF16)
            total = total + mm(hid, wd[side])
        x[s] = total.astype(BF16)

    build_bias(u_ref, 0)
    arrived(u_other, misc_recv.at[1])
    build_bias(u_other, 1)
    own_stage.wait()
    own_x0t = pltpu.make_async_copy(stage, x0t_ref.at[:, my_pos, :], out_sem.at[0])
    own_x0t.start()

    own_x.wait()
    arrived(x.at[:, part(half, other), :], misc_recv.at[0])
    out_x0 = pltpu.make_async_copy(x, x0_ref, out_sem.at[1])
    out_x0.start()
    begin_layer(0)
    for n in range(4):
        own_loads[n].wait()
    heads(0, 0, 0)
    heads(0, 0, 1)
    for n in range(4):
        pass_on(n)
    for n in range(4):
        pass_across(n)
    for n in range(4, 7):
        pass_on(n)
    for n in range(4):
        complete(n)
    heads(0, 1, 0)
    pass_on(7)
    heads(0, 1, 1)
    for n in range(4, 7):
        pass_across(n)
    out_x0.wait()
    end_layer()
    for n in range(4, 7):
        own_loads[n].wait()
        complete(n)
    pass_on(8)

    @pl.loop(0, seqs // 2)
    def _(s):
        dense(s)

    pass_on(9)

    @pl.loop(seqs // 2, seqs)
    def _(s):
        dense(s)

    out_h1 = pltpu.make_async_copy(x, h1_ref, out_sem.at[2])
    out_h1.start()
    begin_layer(1)
    for n in range(7, 11):
        own_loads[n].wait()
    heads(1, 0, 0)
    pass_on(10)
    heads(1, 0, 1)
    for n in range(7, 11):
        pass_across(n)
    for n in range(7, 11):
        complete(n)
    heads(1, 1, 0)
    heads(1, 1, 1)
    out_h1.wait()
    end_layer()
    out_h2 = pltpu.make_async_copy(x, h2_ref, out_sem.at[3])
    out_h2.start()

    arrived(x0t_ref.at[:, part(half, other), :], misc_recv.at[2])
    own_x0t.wait()
    for copy in [send_entry, send_u, send_rest] + y_copies + x_copies + c_copies + d_copies:
        copy.wait_send()
    out_h2.wait()


def dense_layers(hidden_in, ln_attn, ln_ffn, w_query, w_key, w_value, w_out, bias_u, w_gate, w_up, w_down):
    batch, positions, d_model = hidden_in.shape
    seqs, seq_len = batch // 2, 2 * positions
    inner = w_query.shape[2]
    any_spec = pl.BlockSpec(memory_space=pl.ANY)
    vmem_spec = pl.BlockSpec(memory_space=pltpu.VMEM)
    dma = pltpu.SemaphoreType.DMA
    shape = jax.ShapeDtypeStruct((seqs, seq_len, d_model), BF16)
    return pl.pallas_call(
        layers_body,
        in_specs=[any_spec, vmem_spec, vmem_spec] + [any_spec] * 4 + [vmem_spec] + [any_spec] * 3,
        out_specs=[any_spec] * 4,
        out_shape=[shape] * 4,
        scratch_shapes=[
            pltpu.VMEM(shape.shape, BF16),
            pltpu.VMEM((seqs * seq_len, d_model), BF16),
            pltpu.VMEM((seqs * seq_len, d_model), F32),
            pltpu.VMEM((2, 2, 3, d_model, inner), BF16),
            pltpu.VMEM((2, 2, inner, d_model), BF16),
            pltpu.VMEM((2, 2) + w_gate.shape, BF16),
            pltpu.VMEM((2,) + w_down.shape, BF16),
            pltpu.VMEM(bias_u.shape, F32),
            pltpu.VMEM((16, seq_len, seq_len // 2), F32),
            pltpu.VMEM((16, seq_len, seq_len), F32),
            pltpu.VMEM((3, seqs * seq_len, 256), BF16),
            pltpu.VMEM((seqs * seq_len, 256), BF16),
            pltpu.VMEM((seqs, positions, d_model), BF16),
            dma((2,)), dma((11,)), dma((4,)), dma((3,)), dma((3,)),
        ] + [dma((11,))] * 8,
        compiler_params=pltpu.CompilerParams(vmem_limit_bytes=VMEM_LIMIT, collective_id=1, has_side_effects=True),
        cost_estimate=pl.CostEstimate(flops=32_000_000_000, bytes_accessed=40 << 20, transcendentals=0),
        name="dense_layers",
    )(hidden_in, ln_attn, ln_ffn, w_query, w_key, w_value, w_out, bias_u, w_gate, w_up, w_down)


def moe_body(h2_ref, h1_ref, x0_ref, x0t_ref, slot_row_ref, slot_col_ref, ids_ref, ln_ref, ln_attn_ref, router_ref,
             w_in_hbm, w_out_hbm, wk_hbm, wv_hbm,
             out_ref, k_ref, v_ref, h1t_ref,
             hall, res, ret, w_in, w_out, wkv, acc, slots_all, gates, xbuf, kvbuf,
             in_sem, cache_sem, store_sem, slot_send, slot_recv, hs_send, hs_recv, ret_send, ret_recv, h1_send, h1_recv):
    tp, ep = lax.axis_index('tp'), lax.axis_index('ep')
    other = 1 - tp
    ep1, ep2, ep3 = axis_neighbours(tp, ep)
    me = tp * 4 + ep
    seqs, seq_len, d_model = h2_ref.shape
    tokens = acc.shape[0]
    rows = res.shape[1]
    half_pos = seq_len // 2
    experts = w_in.shape[0]
    capacity = rows // experts

    loads = [pltpu.make_async_copy(a, b, in_sem.at[n]) for n, (a, b) in enumerate((
        (x0_ref, xbuf), (wk_hbm, wkv.at[0]), (wv_hbm, wkv.at[1]), (h2_ref, hall.at[me]),
        (w_in_hbm, w_in), (w_out_hbm, w_out)))]
    for load in loads:
        load.start()
    slots_all[me] = slot_row_ref[...]

    barrier = pltpu.get_barrier_semaphore()
    peers = [(other, ep), (tp, ep2), (tp, ep1), (other, ep1), (other, ep2), (tp, ep3), (other, ep3)]
    for peer_tp, peer_ep in peers:
        pl.semaphore_signal(barrier, inc=1, device_id=(lax.axis_index('dp'), peer_tp, peer_ep), device_id_type=pl.DeviceIdType.MESH)
    pl.semaphore_wait(barrier, len(peers))

    def block(owner):
        return hall.at[owner]

    send_y = remote(h2_ref, block(me), hs_send.at[0], hs_recv.at[me], other, ep)
    send_x = remote(h2_ref, block(me), hs_send.at[1], hs_recv.at[me], tp, ep2)
    send_c = remote(h2_ref, block(me), hs_send.at[2], hs_recv.at[me], tp, ep1)
    for copy in (send_y, send_x, send_c):
        copy.start()
    slot_copies = [remote(slot_row_ref, slots_all.at[me], slot_send.at[n], slot_recv.at[me], *peer) for n, peer in enumerate(peers)]
    for copy in slot_copies:
        copy.start()
    send_h1 = remote(h1_ref, h1t_ref, h1_send, h1_recv, other, ep)
    send_h1.start()

    def arrived(ref, sem):
        remote(ref, ref, hs_send.at[0], sem, tp, ep).wait_recv()

    def block_arrived(owner):
        arrived(hall.at[owner], hs_recv.at[owner])

    def cache_part(source, layer, owner, load=None):
        if load is None:
            load = pltpu.make_async_copy(source, xbuf, cache_sem)
            load.start()
        load.wait()

        @pl.loop(0, seqs)
        def _(s):
            a = rms_rows(xbuf[s], ln_attn_ref[layer])
            for n, ref in enumerate((k_ref, v_ref)):
                full = mm(a, wkv[n, layer])
                kvbuf[s, n] = full.T.astype(BF16).reshape(kvbuf.shape[2:])
                pltpu.make_async_copy(kvbuf.at[s, n], ref.at[layer, owner * seqs + s], store_sem.at[s, n]).start()

        @pl.loop(0, seqs)
        def _(s):
            for n, ref in enumerate((k_ref, v_ref)):
                pltpu.make_async_copy(kvbuf.at[s, n], ref.at[layer, owner * seqs + s], store_sem.at[s, n]).wait()

    loads[1].wait()
    loads[2].wait()
    cache_part(x0_ref, 0, tp, loads[0])
    cache_part(x0t_ref, 0, other)
    cache_part(h1_ref, 1, tp)

    y_owner, x_owner, c_owner = other * 4 + ep, tp * 4 + ep2, tp * 4 + ep1
    yx_owner, yc_owner, xc_owner, yxc_owner = other * 4 + ep2, other * 4 + ep1, tp * 4 + ep3, other * 4 + ep3
    block_arrived(y_owner)
    fwd_yx = remote(block(y_owner), block(y_owner), hs_send.at[3], hs_recv.at[y_owner], tp, ep2)
    fwd_yc = remote(block(y_owner), block(y_owner), hs_send.at[4], hs_recv.at[y_owner], tp, ep1)
    fwd_yx.start()
    fwd_yc.start()
    loads[3].wait()

    def own_tokens(owner):
        return hall[owner, :, pl.ds(pl.multiple_of(tp * half_pos, half_pos), half_pos), :].reshape(tokens // 2, d_model)

    for part in range(2):
        at = slice(part * (tokens // 2), (part + 1) * (tokens // 2))
        h_own = own_tokens(part * 4 + ep)
        acc[at] = h_own.astype(F32)
        b = rms_rows(h_own, ln_ref[0])
        logits = jnp.dot(b.astype(F32), router_ref[...], precision=lax.Precision.HIGHEST, preferred_element_type=F32)
        grown = jnp.exp(logits - jnp.max(logits, axis=-1, keepdims=True))
        probs = grown / jnp.sum(grown, axis=-1, keepdims=True)
        lanes = lax.broadcasted_iota(jnp.int32, probs.shape, 1)
        picked = [jnp.sum(jnp.where(ids_ref[at, c:c + 1] == lanes, probs, 0.0), axis=-1, keepdims=True) for c in range(2)]
        both = picked[0] + picked[1]
        gates[at, 0:1] = picked[0] / both
        gates[at, 1:2] = picked[1] / both

    block_arrived(x_owner)
    fwd_xc = remote(block(x_owner), block(x_owner), hs_send.at[5], hs_recv.at[x_owner], tp, ep1)
    fwd_xc.start()
    for peer_tp, peer_ep in peers:
        arrived(slots_all.at[peer_tp * 4 + peer_ep], slot_recv.at[peer_tp * 4 + peer_ep])
    loads[4].wait()
    loads[5].wait()

    def run_group(i, k):
        dest = k * 4 + i
        slots = slots_all[dest]
        want = me * rows + lax.broadcasted_iota(jnp.int32, (rows, tokens // 2), 0)
        chosen = None
        for part in range(2):
            h = hall[part * 4 + i, :, pl.ds(pl.multiple_of(k * half_pos, half_pos), half_pos), :].reshape(tokens // 2, d_model)
            at = slice(part * (tokens // 2), (part + 1) * (tokens // 2))
            pick = jnp.logical_or(slots[0:1, at] == want, slots[1:2, at] == want)
            term = mm(jnp.where(pick, 1.0, 0.0).astype(BF16), h)
            chosen = term if chosen is None else chosen + term
        b = rms_rows(chosen, ln_ref[0])
        for e in range(experts):
            at = slice(e * capacity, (e + 1) * capacity)
            hid = jax.nn.gelu(mm(b[at], w_in[e])).astype(BF16)
            res[dest, at] = mm(hid, w_out[e]).astype(BF16)
        return dest

    def give_back(i, k):
        dest = k * 4 + i
        return remote(res.at[dest], ret.at[me], ret_send.at[dest], ret_recv.at[me], k, i)

    def add_rows(source_ref, owner):
        step = 256

        @pl.loop(0, tokens // step)
        def _(r):
            at = pl.ds(pl.multiple_of(r * step, step), step)
            columns = owner * rows + lax.broadcasted_iota(jnp.int32, (step, rows), 1)
            total = acc[at, :]
            for c in range(2):
                pick = jnp.where(slot_col_ref[at, c:c + 1] == columns, 1.0, 0.0).astype(BF16)
                total = total + gates[at, c:c + 1] * mm(pick, source_ref[...])
            acc[at, :] = total

    block_arrived(c_owner)
    block_arrived(yc_owner)

    @pl.loop(0, 4)
    def _(t):
        late = t // 2
        beside = lax.rem((t + 1) // 2, 2)
        i = ep + beside * (ep1 - ep)
        k = late * tp + (1 - late) * other
        run_group(i, k)

        @pl.when(t < 3)
        def _():
            give_back(i, k).start()

    add_rows(res.at[me], me)

    block_arrived(yx_owner)
    fwd_yxc = remote(block(yx_owner), block(yx_owner), hs_send.at[6], hs_recv.at[yx_owner], tp, ep1)
    fwd_yxc.start()

    def far_groups(i):
        @pl.loop(0, 2)
        def _(t):
            k = t * tp + (1 - t) * other
            run_group(i, k)
            give_back(i, k).start()

    far_groups(ep2)
    block_arrived(xc_owner)
    block_arrived(yxc_owner)
    far_groups(ep3)

    arrived(h1t_ref, h1_recv)
    cache_part(h1t_ref, 1, other)

    for peer_tp, peer_ep in ((tp, ep1), (other, ep), (other, ep1), (other, ep2), (tp, ep2), (other, ep3), (tp, ep3)):
        owner = peer_tp * 4 + peer_ep
        arrived(ret.at[owner], ret_recv.at[owner])
        add_rows(ret.at[owner], owner)
    out_ref[...] = acc[...].astype(BF16)

    for copy in (send_y, send_x, send_c, fwd_yx, fwd_yc, fwd_xc, fwd_yxc, send_h1):
        copy.wait_send()
    for copy in slot_copies:
        copy.wait_send()
    for peer_tp, peer_ep in peers:
        give_back(peer_ep, peer_tp).wait_send()


def moe_layer(h2, h1, x0, x0t, slots, choices, ln, ln_attn, w_router, expert_in, expert_out, w_key, w_value):
    seqs, seq_len, d_model = h2.shape
    tokens = seqs * seq_len
    experts, _, d_ff = expert_in.shape
    groups = 8
    rows = experts * 4 * tokens // (experts * groups)
    inner = w_key.shape[2]
    heads = inner // 64
    any_spec = pl.BlockSpec(memory_space=pl.ANY)
    vmem_spec = pl.BlockSpec(memory_space=pltpu.VMEM)
    cache_shape = jax.ShapeDtypeStruct((2, 2 * seqs, heads, 64, seq_len), BF16)
    dma = pltpu.SemaphoreType.DMA
    return pl.pallas_call(
        moe_body,
        in_specs=[any_spec] * 4 + [vmem_spec] * 6 + [any_spec] * 4,
        out_specs=[vmem_spec, any_spec, any_spec, any_spec],
        out_shape=[jax.ShapeDtypeStruct((tokens, d_model), BF16), cache_shape, cache_shape, jax.ShapeDtypeStruct(h1.shape, BF16)],
        scratch_shapes=[
            pltpu.VMEM((groups,) + h2.shape, BF16),
            pltpu.VMEM((groups, rows, d_model), BF16),
            pltpu.VMEM((groups, rows, d_model), BF16),
            pltpu.VMEM(expert_in.shape, BF16),
            pltpu.VMEM(expert_out.shape, BF16),
            pltpu.VMEM((2, 2, d_model, inner), BF16),
            pltpu.VMEM((tokens, d_model), F32),
            pltpu.VMEM((groups, 2, tokens), jnp.int32),
            pltpu.VMEM((tokens, 2), F32),
            pltpu.VMEM(h1.shape, BF16),
            pltpu.VMEM((seqs, 2, heads, 64, seq_len), BF16),
            dma((6,)), dma, dma((seqs, 2)), dma((7,)), dma((groups,)), dma((7,)), dma((groups,)),
            dma((groups,)), dma((groups,)), dma, dma,
        ],
        compiler_params=pltpu.CompilerParams(vmem_limit_bytes=67043328, collective_id=2, has_side_effects=True),
        cost_estimate=pl.CostEstimate(flops=40_000_000_000, bytes_accessed=64 << 20, transcendentals=0),
        name="moe",
    )(h2, h1, x0, x0t, slots.T, slots, choices, ln, ln_attn, w_router, expert_in, expert_out, w_key, w_value)


def slot_table(choices, num_experts, capacity):
    tokens = choices.shape[0]
    experts = jnp.arange(num_experts, dtype=jnp.int32)
    hot = (choices[:, :, None] == experts).astype(BF16).reshape(tokens, 2 * num_experts)
    rows = jnp.arange(tokens, dtype=jnp.int32)
    tri = (rows[:, None] >= rows[None, :]).astype(BF16)
    upto = mm(tri, hot)
    wide = hot.astype(F32)
    first_hot, second_hot = wide[:, :num_experts], wide[:, num_experts:]
    first_pos = jnp.sum((upto[:, :num_experts] - 1.0) * first_hot, axis=-1)
    base = upto[-1:, :num_experts] - 1.0
    second_pos = jnp.sum((upto[:, num_experts:] + base) * second_hot, axis=-1)
    position = jnp.stack([first_pos, second_pos], axis=-1).astype(jnp.int32)
    return jnp.where(position < capacity, choices * capacity + position, -1)


def solution(mesh):
    act_spec = P(('dp', 'ep'), 'tp', None)
    col_spec = P(None, None, 'tp')
    row_spec = P(None, 'tp', None)
    expert_spec = P(('tp', 'ep'), None, None)
    cache_spec = P(None, ('dp', 'ep'), 'tp', None, None)
    in_specs = (act_spec, P(), P(), col_spec, col_spec, col_spec, row_spec, row_spec,
                P(None, 'tp'), P(None, 'tp'), P('tp', None), P(), expert_spec, expert_spec, act_spec)

    def device_fn(hidden_in, ln_attn, ln_ffn, w_query, w_key, w_value, w_out, bias_table, w_gate, w_up, w_down, w_router, expert_in, expert_out, expert_ids):
        batch, positions, d_model = hidden_in.shape
        num_experts = w_router.shape[1]
        tokens = batch * positions
        capacity = 4 * tokens // num_experts
        choices = expert_ids.reshape(tokens, 2)
        slots = slot_table(choices, num_experts, capacity)
        bias_u = bias_rows(bias_table, 2 * positions)[:, :, None, :]
        h1, h2, x0, x0t = dense_layers(hidden_in, ln_attn, ln_ffn, w_query, w_key, w_value, w_out, bias_u, w_gate, w_up, w_down)
        hidden, k_cache, v_cache, _ = moe_layer(
            h2, h1, x0, x0t, slots, choices, ln_ffn[1:2], ln_attn, w_router, expert_in, expert_out, w_key, w_value)
        return hidden.reshape(hidden_in.shape), jnp.swapaxes(k_cache, 3, 4), jnp.swapaxes(v_cache, 3, 4)

    return jax.shard_map(device_fn, mesh=mesh, in_specs=in_specs, out_specs=(act_spec, cache_spec, cache_spec), check_vma=False)
```

```python
import contextlib

import jax
import jax.numpy as jnp
from jax import lax
from jax.experimental import pallas as pl
from jax.experimental.pallas import tpu as pltpu
from jax.sharding import PartitionSpec as P

EXACT_BUCKETS = 16
THRESHOLDS = (18, 20, 23, 26, 30, 34, 39, 45, 51, 58, 66, 76, 86, 98, 112)
EPSILON = 1e-6
F32 = jnp.float32
BF16 = jnp.bfloat16
VMEM_LIMIT = 60 * 1024 * 1024
MESH = pl.DeviceIdType.MESH


def scope(name):
    return contextlib.nullcontext()


def rms_rows(rows, ln_scale):
    wide = rows.astype(F32)
    inv_rms = lax.rsqrt(jnp.mean(wide * wide, axis=-1, keepdims=True) + EPSILON)
    return (wide * inv_rms * ln_scale).astype(BF16)


def mm(a, b):
    return lax.dot_general(a, b, (((1,), (0,)), ((), ())), preferred_element_type=F32)


def mm_t(a, b):
    return lax.dot_general(a, b, (((1,), (1,)), ((), ())), preferred_element_type=F32)


def bias_rows(table, seq_len):
    at = lax.broadcasted_iota(jnp.int32, (table.shape[1], 2 * seq_len), 1)
    rel = jnp.where(at == 0, 0, 2 * seq_len - at)
    bucket = jnp.minimum(rel, EXACT_BUCKETS)
    for threshold in THRESHOLDS:
        bucket = bucket + jnp.where(rel >= threshold, 1, 0)
    hot = jnp.where(bucket == lax.broadcasted_iota(jnp.int32, bucket.shape, 0), 1.0, 0.0)
    rows = jnp.dot(table, hot, precision=lax.Precision.HIGHEST, preferred_element_type=F32)
    return jnp.where(rel[:1] < seq_len, rows, -jnp.inf)


def softmax_bf16(scores):
    top = jnp.max(scores, axis=-1, keepdims=True)
    grown = jnp.exp(scores - top)
    return (grown * (1.0 / jnp.sum(grown, axis=-1, keepdims=True))).astype(BF16)


def axis_neighbours(tp, ep):
    core = lax.rem(ep, 2)
    beside = ep + 1 - 2 * core
    return beside, lax.rem(ep + 2, 4), lax.rem(beside + 2, 4)


def remote(src, dst, send, recv, tp, ep):
    return pltpu.make_async_remote_copy(
        src_ref=src, dst_ref=dst, send_sem=send, recv_sem=recv,
        device_id=(lax.axis_index('dp'), tp, ep), device_id_type=MESH)


def layers_body(hid_ref, ln_attn_ref, ln_ffn_ref, wq_hbm, wk_hbm, wv_hbm, wo_hbm, table_ref, wg_hbm, wu_hbm, wd_hbm,
                h1_ref, h2_ref, x0_ref, x0t_ref,
                x, a_ref, acc, w, wo, gu, wd, table_other, u_rows, bias_low, bias_high, qkv, ctx, stage,
                in_sem, own_sem, out_sem, misc_send, misc_recv, y_send, y_recv, x_send, x_recv, c_send, c_recv, d_send, d_recv):
    tp, ep = lax.axis_index('tp'), lax.axis_index('ep')
    other = 1 - tp
    ep1, ep2, ep3 = axis_neighbours(tp, ep)
    seqs, seq_len, d_model = x.shape
    half = seq_len // 2
    tokens = seqs * seq_len
    quad = qkv.shape[2]

    def part(count, quarter):
        return pl.ds(pl.multiple_of(quarter * count, count), count)

    my_pos = part(half, tp)
    mine = hid_ref.at[pl.ds(tp * seqs, seqs)]
    theirs = hid_ref.at[pl.ds(other * seqs, seqs)]

    sources, places = [], []
    for layer in range(2):
        for kind, hbm in enumerate((wq_hbm, wk_hbm, wv_hbm)):
            sources.append(hbm.at[layer, :, part(128, ep)])
            places.append(lambda q, layer=layer, kind=kind: w.at[layer, 1, kind, :, part(128, q)])
        sources.append(wo_hbm.at[layer, part(128, ep), :])
        places.append(lambda q, layer=layer: wo.at[layer, 1, part(128, q), :])
        if layer == 0:
            for kind, hbm in enumerate((wg_hbm, wu_hbm)):
                sources.append(hbm.at[part(256, ep), :])
                places.append(lambda q, kind=kind: gu.at[1, kind, part(256, q), :])
            sources.append(wd_hbm.at[part(64, ep), :])
            places.append(lambda q: wd.at[1, part(64, q), :])

    own_x = pltpu.make_async_copy(mine, x.at[:, my_pos, :], in_sem.at[0])
    own_stage = pltpu.make_async_copy(theirs, stage, in_sem.at[1])
    own_x.start()
    own_loads = []
    for layer in range(2):
        for kind, hbm in enumerate((wq_hbm, wk_hbm, wv_hbm)):
            own_loads.append((hbm.at[layer], w.at[layer, 0, kind]))
        own_loads.append((wo_hbm.at[layer], wo.at[layer, 0]))
        if layer == 0:
            own_loads += [(wg_hbm, gu.at[0, 0]), (wu_hbm, gu.at[0, 1]), (wd_hbm, wd.at[0])]
    own_loads = [pltpu.make_async_copy(s, d, own_sem.at[n]) for n, (s, d) in enumerate(own_loads)]
    for load in own_loads:
        load.start()
    own_stage.start()

    barrier = pltpu.get_barrier_semaphore()
    for peer_tp, peer_ep in ((other, ep), (tp, ep2), (tp, ep1)):
        pl.semaphore_signal(barrier, inc=1, device_id=(lax.axis_index('dp'), peer_tp, peer_ep), device_id_type=MESH)
    pl.semaphore_wait(barrier, 3)

    def arrived(ref, sem):
        remote(ref, ref, misc_send.at[0], sem, tp, ep).wait_recv()

    pieces = range(len(sources))
    send_entry = remote(theirs, x.at[:, my_pos, :], misc_send.at[0], misc_recv.at[0], other, ep)
    send_u = remote(table_ref, table_other, misc_send.at[1], misc_recv.at[1], other, ep)
    send_rest = remote(mine, x0t_ref.at[:, my_pos, :], misc_send.at[2], misc_recv.at[2], other, ep)
    y_copies = [remote(sources[n], places[n](ep), y_send.at[n], y_recv.at[n], other, ep) for n in pieces]
    x_copies = [remote(places[n](ep), places[n](ep), x_send.at[n], x_recv.at[n], tp, ep2) for n in pieces]
    c_copies = [remote(places[n](ep), places[n](ep), c_send.at[n], c_recv.at[n], tp, ep1) for n in pieces]
    d_copies = [remote(places[n](ep2), places[n](ep2), d_send.at[n], d_recv.at[n], tp, ep1) for n in pieces]
    send_u.start()
    send_entry.start()
    for copy in y_copies:
        copy.start()
    send_rest.start()

    def pass_on(n):
        arrived(places[n](ep), y_recv.at[n])
        x_copies[n].start()
        c_copies[n].start()

    def pass_across(n):
        arrived(places[n](ep2), x_recv.at[n])
        d_copies[n].start()

    def complete(n):
        arrived(places[n](ep1), c_recv.at[n])
        arrived(places[n](ep3), d_recv.at[n])

    def build_bias(rows_ref, side):
        u_rows[...] = bias_rows(rows_ref[...].reshape(u_rows.shape[0], rows_ref.shape[2]), seq_len)

        @pl.loop(0, 8)
        def _(n):
            layer, pair = n // 4, lax.rem(n, 4)
            for sub in range(2):
                row = u_rows[pl.ds(n * 2 + sub, 1), :]
                wide = pltpu.roll(jnp.broadcast_to(row, (seq_len, 2 * seq_len)), 0, 1, stride=1, stride_axis=0)
                at = slice(sub * half, (sub + 1) * half)
                place = layer * 8 + side * 4 + pair
                bias_low[place, at, :] = wide[:half, :half]
                bias_high[place, at, :] = wide[half:, :seq_len]

    def begin_layer(layer):
        @pl.loop(0, seqs)
        def _(s):
            rows = part(seq_len, s)
            a_ref[rows, :] = rms_rows(x[s], ln_attn_ref[layer])
            acc[rows, :] = x[s].astype(F32)

    def end_layer():
        @pl.loop(0, seqs)
        def _(s):
            x[s] = acc[part(seq_len, s), :].astype(BF16)

    first = lax.broadcasted_iota(jnp.int32, (1, 128), 1) < 64

    def attend(layer, side, block):
        cols = slice(block * quad, (block + 1) * quad)
        for kind in range(3):
            qkv[kind] = mm(a_ref[...], w[layer, side, kind, :, cols]).astype(BF16)

        @pl.loop(0, seqs)
        def _(s):
            rows = part(seq_len, s)
            for pair in range(quad // 128):
                lanes = slice(pair * 128, (pair + 1) * 128)
                place = layer * 8 + side * 4 + block * (quad // 128) + pair
                q, k, v = (qkv[kind, rows, lanes] for kind in range(3))
                none = jnp.zeros_like(q[:half])
                outs = []
                for upper in range(2):
                    qs = q[half:] if upper else q[:half]
                    ks, vs = (k, v) if upper else (k[:half], v[:half])
                    both = jnp.concatenate([jnp.where(first, qs, none), jnp.where(first, none, qs)], axis=0)
                    bias = bias_high[place] if upper else bias_low[place]
                    got = mm(softmax_bf16(mm_t(both, ks) * 0.125 + bias), vs)
                    outs.append(jnp.where(first, got[:half], got[half:]))
                ctx[rows, lanes] = jnp.concatenate(outs, axis=0).astype(BF16)

    def project(layer, side, block):
        cols = slice(block * quad, (block + 1) * quad)

        @pl.loop(0, seqs)
        def _(s):
            rows = part(seq_len, s)
            acc[rows, :] += mm(ctx[rows, :], wo[layer, side, cols, :])

    def dense(s):
        h = x[s]
        b = rms_rows(h, ln_ffn_ref[0])
        total = h.astype(F32)
        for side in range(2):
            hid = (jax.nn.gelu(mm(b, gu[side, 0])) * mm(b, gu[side, 1])).astype(BF16)
            total = total + mm(hid, wd[side])
        x[s] = total.astype(BF16)

    def heads(layer, side, block):
        attend(layer, side, block)
        project(layer, side, block)

    build_bias(table_ref, 0)
    arrived(table_other, misc_recv.at[1])
    build_bias(table_other, 1)
    own_stage.wait()
    own_x0t = pltpu.make_async_copy(stage, x0t_ref.at[:, my_pos, :], out_sem.at[0])
    own_x0t.start()

    with scope("w_entry"):
        own_x.wait()
        arrived(x.at[:, part(half, other), :], misc_recv.at[0])
    out_x0 = pltpu.make_async_copy(x, x0_ref, out_sem.at[1])
    out_x0.start()
    begin_layer(0)
    for n in range(4):
        own_loads[n].wait()
    heads(0, 0, 0)
    heads(0, 0, 1)
    with scope("w_l0_y"):
        for n in range(4):
            pass_on(n)
    with scope("w_l0_x"):
        for n in range(3):
            pass_across(n)
    with scope("w_l0_all"):
        for n in range(3):
            complete(n)
    attend(0, 1, 0)
    with scope("w_l0_o"):
        pass_across(3)
        pass_on(4)
        complete(3)
        pass_on(5)
    project(0, 1, 0)
    with scope("w_ffn_y"):
        pass_on(6)
    heads(0, 1, 1)
    with scope("w_ffn_x"):
        pass_on(7)
        for n in range(4, 7):
            pass_across(n)
    out_x0.wait()
    end_layer()
    with scope("w_ffn_all"):
        for n in range(4, 7):
            own_loads[n].wait()
            complete(n)

    @pl.loop(0, seqs // 2)
    def _(s):
        dense(s)

    with scope("w_l1_k"):
        pass_on(8)

    @pl.loop(seqs // 2, seqs)
    def _(s):
        dense(s)

    out_h1 = pltpu.make_async_copy(x, h1_ref, out_sem.at[2])
    out_h1.start()
    begin_layer(1)
    for n in range(7, 11):
        own_loads[n].wait()
    attend(1, 0, 0)
    with scope("w_l1_v"):
        pass_on(9)
    project(1, 0, 0)
    heads(1, 0, 1)
    with scope("w_l1_o"):
        pass_on(10)
    with scope("w_l1_x"):
        for n in range(7, 10):
            pass_across(n)
    with scope("w_l1_all"):
        for n in range(7, 10):
            complete(n)
    attend(1, 1, 0)
    with scope("w_l1_o_all"):
        pass_across(10)
        complete(10)
    project(1, 1, 0)
    heads(1, 1, 1)
    out_h1.wait()
    end_layer()
    out_h2 = pltpu.make_async_copy(x, h2_ref, out_sem.at[3])
    out_h2.start()

    with scope("w_rest"):
        arrived(x0t_ref.at[:, part(half, other), :], misc_recv.at[2])
    own_x0t.wait()
    for copy in [send_entry, send_u, send_rest] + y_copies + x_copies + c_copies + d_copies:
        copy.wait_send()
    out_h2.wait()


def dense_layers(hidden_in, ln_attn, ln_ffn, w_query, w_key, w_value, w_out, bias_table, w_gate, w_up, w_down):
    batch, positions, d_model = hidden_in.shape
    seqs, seq_len = batch // 2, 2 * positions
    inner = w_query.shape[2]
    any_spec = pl.BlockSpec(memory_space=pl.ANY)
    vmem_spec = pl.BlockSpec(memory_space=pltpu.VMEM)
    dma = pltpu.SemaphoreType.DMA
    shape = jax.ShapeDtypeStruct((seqs, seq_len, d_model), BF16)
    return pl.pallas_call(
        layers_body,
        in_specs=[any_spec, vmem_spec, vmem_spec] + [any_spec] * 4 + [vmem_spec] + [any_spec] * 3,
        out_specs=[any_spec] * 4,
        out_shape=[shape] * 4,
        scratch_shapes=[
            pltpu.VMEM(shape.shape, BF16),
            pltpu.VMEM((seqs * seq_len, d_model), BF16),
            pltpu.VMEM((seqs * seq_len, d_model), F32),
            pltpu.VMEM((2, 2, 3, d_model, inner), BF16),
            pltpu.VMEM((2, 2, inner, d_model), BF16),
            pltpu.VMEM((2, 2) + w_gate.shape, BF16),
            pltpu.VMEM((2,) + w_down.shape, BF16),
            pltpu.VMEM(bias_table.shape, F32),
            pltpu.VMEM((bias_table.shape[0] * bias_table.shape[1], 2 * seq_len), F32),
            pltpu.VMEM((16, seq_len, seq_len // 2), F32),
            pltpu.VMEM((16, seq_len, seq_len), F32),
            pltpu.VMEM((3, seqs * seq_len, 256), BF16),
            pltpu.VMEM((seqs * seq_len, 256), BF16),
            pltpu.VMEM((seqs, positions, d_model), BF16),
            dma((2,)), dma((11,)), dma((4,)), dma((3,)), dma((3,)),
        ] + [dma((11,))] * 8,
        compiler_params=pltpu.CompilerParams(vmem_limit_bytes=VMEM_LIMIT, collective_id=1, has_side_effects=True),
        cost_estimate=pl.CostEstimate(flops=32_000_000_000, bytes_accessed=40 << 20, transcendentals=0),
        name="dense_layers",
    )(hidden_in, ln_attn, ln_ffn, w_query, w_key, w_value, w_out, bias_table, w_gate, w_up, w_down)


def moe_body(h2_ref, h1_ref, x0_ref, x0t_ref, ids_ref, ln_ffn_ref, ln_attn_ref, router_ref,
             w_in_hbm, w_out_hbm, wk_hbm, wv_hbm,
             out_ref, k_ref, v_ref, h1t_ref,
             hall, res, ret, w_in, w_out, wkv, acc, slot_row_ref, slots_all, columns_ref, gates, xbuf, kvbuf,
             in_sem, cache_sem, store_sem, slot_send, slot_recv, hs_send, hs_recv, ret_send, ret_recv, h1_send, h1_recv):
    tp, ep = lax.axis_index('tp'), lax.axis_index('ep')
    other = 1 - tp
    ep1, ep2, ep3 = axis_neighbours(tp, ep)
    me = tp * 4 + ep
    seqs, seq_len, d_model = h2_ref.shape
    tokens = acc.shape[0]
    rows = res.shape[1]
    half_pos = seq_len // 2
    experts = w_in.shape[0]
    capacity = rows // experts

    loads = [pltpu.make_async_copy(a, b, in_sem.at[n]) for n, (a, b) in enumerate((
        (x0_ref, xbuf), (wk_hbm, wkv.at[0]), (wv_hbm, wkv.at[1]), (h2_ref, hall.at[me]),
        (w_in_hbm, w_in), (w_out_hbm, w_out)))]
    for load in loads:
        load.start()

    barrier = pltpu.get_barrier_semaphore()
    peers = [(other, ep), (tp, ep2), (tp, ep1), (other, ep1), (other, ep2), (tp, ep3), (other, ep3)]
    for peer_tp, peer_ep in peers:
        pl.semaphore_signal(barrier, inc=1, device_id=(lax.axis_index('dp'), peer_tp, peer_ep), device_id_type=MESH)
    pl.semaphore_wait(barrier, len(peers))

    def half_at(k):
        return pl.ds(pl.multiple_of(k * half_pos, half_pos), half_pos)

    def block(owner, k):
        return hall.at[owner, :, half_at(k), :]

    sends = []
    for n, peer in enumerate(((other, ep), (tp, ep2), (tp, ep1))):
        for k in range(2):
            sends.append(remote(h2_ref.at[:, half_at(k), :], block(me, k), hs_send.at[n, k], hs_recv.at[me, k], *peer))
    for copy in sends:
        copy.start()
    send_h1 = remote(h1_ref, h1t_ref, h1_send, h1_recv, other, ep)
    send_h1.start()

    def arrived(ref, sem):
        remote(ref, ref, hs_send.at[0], sem, tp, ep).wait_recv()

    def block_arrived(owner, k):
        arrived(block(owner, k), hs_recv.at[owner, k])

    def forward(n, owner, k, *peer):
        copy = remote(block(owner, k), block(owner, k), hs_send.at[n, k], hs_recv.at[owner, k], *peer)
        copy.start()
        sends.append(copy)

    num_experts = router_ref.shape[0]
    ids_row = jnp.concatenate([ids_ref[s] for s in range(ids_ref.shape[0])], axis=1)
    expert = lax.broadcasted_iota(jnp.int32, (num_experts, tokens), 0)
    hot = [jnp.where(ids_row[c:c + 1] == expert, 1.0, 0.0) for c in range(2)]
    earlier = lax.broadcasted_iota(jnp.int32, (tokens, tokens), 0) <= lax.broadcasted_iota(jnp.int32, (tokens, tokens), 1)
    upto = mm(jnp.concatenate(hot, axis=0).astype(BF16), jnp.where(earlier, 1.0, 0.0).astype(BF16))
    base = (0.0, upto[:num_experts, tokens - 1:])
    wide_ids = ids_row.astype(F32)
    slot_rows = []
    for c in range(2):
        place = jnp.sum((upto[c * num_experts:(c + 1) * num_experts] - 1.0 + base[c]) * hot[c], axis=0, keepdims=True)
        slot_rows.append(jnp.where(place < capacity, wide_ids[c:c + 1] * capacity + place, -1.0))
    packed = jnp.concatenate(slot_rows + [wide_ids, jnp.zeros((4, tokens), F32)], axis=0)
    slot_row_ref[...] = packed[:2].astype(jnp.int32)
    slots_all[me] = packed[:2].astype(jnp.int32)
    columns_ref[...] = packed.T.astype(jnp.int32)

    def cache_part(source, layer, owner, load=None):
        if load is None:
            load = pltpu.make_async_copy(source, xbuf, cache_sem)
            load.start()
        load.wait()

        @pl.loop(0, seqs)
        def _(s):
            a = rms_rows(xbuf[s], ln_attn_ref[layer])
            for n, ref in enumerate((k_ref, v_ref)):
                full = mm(a, wkv[n, layer])
                kvbuf[s, n] = full.T.astype(BF16).reshape(kvbuf.shape[2:])
                pltpu.make_async_copy(kvbuf.at[s, n], ref.at[layer, owner * seqs + s], store_sem.at[s, n]).start()

        @pl.loop(0, seqs)
        def _(s):
            for n, ref in enumerate((k_ref, v_ref)):
                pltpu.make_async_copy(kvbuf.at[s, n], ref.at[layer, owner * seqs + s], store_sem.at[s, n]).wait()

    loads[1].wait()
    loads[2].wait()
    cache_part(x0_ref, 0, tp, loads[0])
    cache_part(x0t_ref, 0, other)
    cache_part(h1_ref, 1, tp)

    slot_copies = [remote(slot_row_ref, slots_all.at[me], slot_send.at[n], slot_recv.at[me], *peer) for n, peer in enumerate(peers)]
    for copy in slot_copies:
        copy.start()

    y_owner, x_owner, c_owner = other * 4 + ep, tp * 4 + ep2, tp * 4 + ep1
    yx_owner, yc_owner, xc_owner, yxc_owner = other * 4 + ep2, other * 4 + ep1, tp * 4 + ep3, other * 4 + ep3
    for k in range(2):
        with scope(f"w_y{k}"):
            block_arrived(y_owner, k)
        forward(3, y_owner, k, tp, ep2)
        forward(4, y_owner, k, tp, ep1)
    loads[3].wait()

    def own_tokens(owner):
        return hall[owner, :, half_at(tp), :].reshape(tokens // 2, d_model)

    for part in range(2):
        at = slice(part * (tokens // 2), (part + 1) * (tokens // 2))
        h_own = own_tokens(part * 4 + ep)
        acc[at] = h_own.astype(F32)
        b = rms_rows(h_own, ln_ffn_ref[1])
        logits = lax.dot_general(b.astype(F32), router_ref[...], (((1,), (1,)), ((), ())),
                                 precision=lax.Precision.HIGHEST, preferred_element_type=F32)
        grown = jnp.exp(logits - jnp.max(logits, axis=-1, keepdims=True))
        probs = grown / jnp.sum(grown, axis=-1, keepdims=True)
        lanes = lax.broadcasted_iota(jnp.int32, probs.shape, 1)
        picked = [jnp.sum(jnp.where(columns_ref[at, 2 + c:3 + c] == lanes, probs, 0.0), axis=-1, keepdims=True) for c in range(2)]
        both = picked[0] + picked[1]
        gates[at, 0:1] = picked[0] / both
        gates[at, 1:2] = picked[1] / both

    with scope("w_x"):
        for k in range(2):
            block_arrived(x_owner, k)
            forward(5, x_owner, k, tp, ep1)
    for peer_tp, peer_ep in peers:
        arrived(slots_all.at[peer_tp * 4 + peer_ep], slot_recv.at[peer_tp * 4 + peer_ep])
    loads[4].wait()
    loads[5].wait()

    def run_group(i, k):
        dest = k * 4 + i
        slots = slots_all[dest]
        want = me * rows + lax.broadcasted_iota(jnp.int32, (rows, tokens // 2), 0)
        chosen = None
        for part in range(2):
            h = hall[part * 4 + i, :, half_at(k), :].reshape(tokens // 2, d_model)
            at = slice(part * (tokens // 2), (part + 1) * (tokens // 2))
            pick = jnp.logical_or(slots[0:1, at] == want, slots[1:2, at] == want)
            term = mm(jnp.where(pick, 1.0, 0.0).astype(BF16), h)
            chosen = term if chosen is None else chosen + term
        b = rms_rows(chosen, ln_ffn_ref[1])
        for e in range(experts):
            at = slice(e * capacity, (e + 1) * capacity)
            hid = jax.nn.gelu(mm(b[at], w_in[e])).astype(BF16)
            res[dest, at] = mm(hid, w_out[e]).astype(BF16)
        return dest

    def give_back(i, k):
        dest = k * 4 + i
        return remote(res.at[dest], ret.at[me], ret_send.at[dest], ret_recv.at[me], k, i)

    def add_rows(source_ref, owner):
        step = 256

        @pl.loop(0, tokens // step)
        def _(r):
            at = pl.ds(pl.multiple_of(r * step, step), step)
            columns = owner * rows + lax.broadcasted_iota(jnp.int32, (step, rows), 1)
            total = acc[at, :]
            for c in range(2):
                pick = jnp.where(columns_ref[at, c:c + 1] == columns, 1.0, 0.0).astype(BF16)
                total = total + gates[at, c:c + 1] * mm(pick, source_ref[...])
            acc[at, :] = total

    with scope("w_yc"):
        for k in range(2):
            block_arrived(c_owner, k)
            block_arrived(yc_owner, k)

    @pl.loop(0, 4)
    def _(t):
        late = t // 2
        beside = lax.rem((t + 1) // 2, 2)
        i = ep + beside * (ep1 - ep)
        k = late * tp + (1 - late) * other
        run_group(i, k)

        @pl.when(t < 3)
        def _():
            give_back(i, k).start()

    add_rows(res.at[me], me)

    for k in range(2):
        with scope(f"w_yx{k}"):
            block_arrived(yx_owner, k)
        forward(6, yx_owner, k, tp, ep1)
        with scope(f"w_far{k}"):
            block_arrived(xc_owner, k)
            block_arrived(yxc_owner, k)

        @pl.loop(0, 2)
        def _(t):
            i = (1 - t) * ep2 + t * ep3
            run_group(i, k)
            give_back(i, k).start()

        if k == 0:
            with scope("w_h1"):
                arrived(h1t_ref, h1_recv)
            cache_part(h1t_ref, 1, other)

    for peer_tp, peer_ep in ((tp, ep1), (other, ep), (other, ep1), (other, ep2), (other, ep3), (tp, ep2), (tp, ep3)):
        owner = peer_tp * 4 + peer_ep
        with scope("w_ret"):
            arrived(ret.at[owner], ret_recv.at[owner])
        add_rows(ret.at[owner], owner)
    out_ref[...] = acc[...].astype(BF16)

    for copy in sends + slot_copies + [send_h1]:
        copy.wait_send()
    for peer_tp, peer_ep in peers:
        give_back(peer_ep, peer_tp).wait_send()


def moe_layer(h2, h1, x0, x0t, expert_ids, ln_ffn, ln_attn, w_router, expert_in, expert_out, w_key, w_value):
    seqs, seq_len, d_model = h2.shape
    tokens = seqs * seq_len
    experts, _, d_ff = expert_in.shape
    groups = 8
    rows = experts * 4 * tokens // (experts * groups)
    inner = w_key.shape[2]
    heads = inner // 64
    any_spec = pl.BlockSpec(memory_space=pl.ANY)
    vmem_spec = pl.BlockSpec(memory_space=pltpu.VMEM)
    cache_shape = jax.ShapeDtypeStruct((2, 2 * seqs, heads, 64, seq_len), BF16)
    dma = pltpu.SemaphoreType.DMA
    return pl.pallas_call(
        moe_body,
        in_specs=[any_spec] * 4 + [vmem_spec] * 4 + [any_spec] * 4,
        out_specs=[vmem_spec, any_spec, any_spec, any_spec],
        out_shape=[jax.ShapeDtypeStruct((tokens, d_model), BF16), cache_shape, cache_shape, jax.ShapeDtypeStruct(h1.shape, BF16)],
        scratch_shapes=[
            pltpu.VMEM((groups,) + h2.shape, BF16),
            pltpu.VMEM((groups, rows, d_model), BF16),
            pltpu.VMEM((groups, rows, d_model), BF16),
            pltpu.VMEM(expert_in.shape, BF16),
            pltpu.VMEM(expert_out.shape, BF16),
            pltpu.VMEM((2, 2, d_model, inner), BF16),
            pltpu.VMEM((tokens, d_model), F32),
            pltpu.VMEM((2, tokens), jnp.int32),
            pltpu.VMEM((groups, 2, tokens), jnp.int32),
            pltpu.VMEM((tokens, 8), jnp.int32),
            pltpu.VMEM((tokens, 2), F32),
            pltpu.VMEM(h1.shape, BF16),
            pltpu.VMEM((seqs, 2, heads, 64, seq_len), BF16),
            dma((6,)), dma, dma((seqs, 2)), dma((7,)), dma((groups,)), dma((7, 2)), dma((groups, 2)),
            dma((groups,)), dma((groups,)), dma, dma,
        ],
        compiler_params=pltpu.CompilerParams(vmem_limit_bytes=67043328, collective_id=2, has_side_effects=True),
        cost_estimate=pl.CostEstimate(flops=40_000_000_000, bytes_accessed=64 << 20, transcendentals=0),
        name="moe",
    )(h2, h1, x0, x0t, jnp.swapaxes(expert_ids, 1, 2), ln_ffn, ln_attn, w_router.T, expert_in, expert_out, w_key, w_value)


def solution(mesh):
    act_spec = P(('dp', 'ep'), 'tp', None)
    col_spec = P(None, None, 'tp')
    row_spec = P(None, 'tp', None)
    expert_spec = P(('tp', 'ep'), None, None)
    cache_spec = P(None, ('dp', 'ep'), 'tp', None, None)
    in_specs = (act_spec, P(), P(), col_spec, col_spec, col_spec, row_spec, row_spec,
                P(None, 'tp'), P(None, 'tp'), P('tp', None), P(), expert_spec, expert_spec, act_spec)

    def device_fn(hidden_in, ln_attn, ln_ffn, w_query, w_key, w_value, w_out, bias_table, w_gate, w_up, w_down, w_router, expert_in, expert_out, expert_ids):
        h1, h2, x0, x0t = dense_layers(hidden_in, ln_attn, ln_ffn, w_query, w_key, w_value, w_out, bias_table, w_gate, w_up, w_down)
        hidden, k_cache, v_cache, _ = moe_layer(
            h2, h1, x0, x0t, expert_ids, ln_ffn, ln_attn, w_router, expert_in, expert_out, w_key, w_value)
        return hidden.reshape(hidden_in.shape), jnp.swapaxes(k_cache, 3, 4), jnp.swapaxes(v_cache, 3, 4)

    return jax.shard_map(device_fn, mesh=mesh, in_specs=in_specs, out_specs=(act_spec, cache_spec, cache_spec), check_vma=False)
```

```python
import contextlib

import jax
import jax.numpy as jnp
from jax import lax
from jax.experimental import pallas as pl
from jax.experimental.pallas import tpu as pltpu
from jax.sharding import PartitionSpec as P

EXACT_BUCKETS = 16
THRESHOLDS = (18, 20, 23, 26, 30, 34, 39, 45, 51, 58, 66, 76, 86, 98, 112)
EPSILON = 1e-6
F32 = jnp.float32
BF16 = jnp.bfloat16
VMEM_LIMIT = 60 * 1024 * 1024
MESH = pl.DeviceIdType.MESH


def scope(name):
    return contextlib.nullcontext()


def rms_rows(rows, ln_scale):
    wide = rows.astype(F32)
    inv_rms = lax.rsqrt(jnp.mean(wide * wide, axis=-1, keepdims=True) + EPSILON)
    return (wide * inv_rms * ln_scale).astype(BF16)


def mm(a, b):
    return lax.dot_general(a, b, (((1,), (0,)), ((), ())), preferred_element_type=F32)


def mm_t(a, b):
    return lax.dot_general(a, b, (((1,), (1,)), ((), ())), preferred_element_type=F32)


def bias_rows(table, seq_len):
    at = lax.broadcasted_iota(jnp.int32, (table.shape[1], 2 * seq_len), 1)
    rel = jnp.where(at == 0, 0, 2 * seq_len - at)
    bucket = jnp.minimum(rel, EXACT_BUCKETS)
    for threshold in THRESHOLDS:
        bucket = bucket + jnp.where(rel >= threshold, 1, 0)
    hot = jnp.where(bucket == lax.broadcasted_iota(jnp.int32, bucket.shape, 0), 1.0, 0.0)
    rows = jnp.dot(table, hot, precision=lax.Precision.HIGHEST, preferred_element_type=F32)
    return jnp.where(rel[:1] < seq_len, rows, -jnp.inf)


def softmax_bf16(scores):
    top = jnp.max(scores, axis=-1, keepdims=True)
    grown = jnp.exp(scores - top)
    return (grown * (1.0 / jnp.sum(grown, axis=-1, keepdims=True))).astype(BF16)


def axis_neighbours(tp, ep):
    core = lax.rem(ep, 2)
    beside = ep + 1 - 2 * core
    return beside, lax.rem(ep + 2, 4), lax.rem(beside + 2, 4)


def remote(src, dst, send, recv, tp, ep):
    return pltpu.make_async_remote_copy(
        src_ref=src, dst_ref=dst, send_sem=send, recv_sem=recv,
        device_id=(lax.axis_index('dp'), tp, ep), device_id_type=MESH)


def layers_body(hid_ref, ln_attn_ref, ln_ffn_ref, wq_hbm, wk_hbm, wv_hbm, wo_hbm, table_ref, wg_hbm, wu_hbm, wd_hbm,
                h1_ref, h2_ref, x0_ref, x0t_ref,
                x, a_ref, acc, w, wo, gu, wd, table_other, u_rows, bias_low, bias_high, qkv, ctx, stage,
                in_sem, own_sem, out_sem, misc_send, misc_recv, y_send, y_recv, x_send, x_recv, c_send, c_recv, d_send, d_recv):
    tp, ep = lax.axis_index('tp'), lax.axis_index('ep')
    other = 1 - tp
    ep1, ep2, ep3 = axis_neighbours(tp, ep)
    seqs, seq_len, d_model = x.shape
    half = seq_len // 2
    tokens = seqs * seq_len
    quad = qkv.shape[2]

    def part(count, quarter):
        return pl.ds(pl.multiple_of(quarter * count, count), count)

    my_pos = part(half, tp)
    mine = hid_ref.at[pl.ds(tp * seqs, seqs)]
    theirs = hid_ref.at[pl.ds(other * seqs, seqs)]

    sources, places = [], []
    for layer in range(2):
        for kind, hbm in enumerate((wq_hbm, wk_hbm, wv_hbm)):
            sources.append(hbm.at[layer, part(256, ep), :])
            places.append(lambda q, layer=layer, kind=kind: w.at[layer, 1, kind, part(256, q), :])
        sources.append(wo_hbm.at[layer, part(128, ep), :])
        places.append(lambda q, layer=layer: wo.at[layer, 1, part(128, q), :])
        if layer == 0:
            for kind, hbm in enumerate((wg_hbm, wu_hbm)):
                sources.append(hbm.at[part(256, ep), :])
                places.append(lambda q, kind=kind: gu.at[1, kind, part(256, q), :])
            sources.append(wd_hbm.at[part(64, ep), :])
            places.append(lambda q: wd.at[1, part(64, q), :])

    own_x = pltpu.make_async_copy(mine, x.at[:, my_pos, :], in_sem.at[0])
    own_stage = pltpu.make_async_copy(theirs, stage, in_sem.at[1])
    own_x.start()
    own_loads = []
    for layer in range(2):
        for kind, hbm in enumerate((wq_hbm, wk_hbm, wv_hbm)):
            own_loads.append((hbm.at[layer], w.at[layer, 0, kind]))
        own_loads.append((wo_hbm.at[layer], wo.at[layer, 0]))
        if layer == 0:
            own_loads += [(wg_hbm, gu.at[0, 0]), (wu_hbm, gu.at[0, 1]), (wd_hbm, wd.at[0])]
    own_loads = [pltpu.make_async_copy(s, d, own_sem.at[n]) for n, (s, d) in enumerate(own_loads)]
    for load in own_loads:
        load.start()
    own_stage.start()

    barrier = pltpu.get_barrier_semaphore()
    for peer_tp, peer_ep in ((other, ep), (tp, ep2), (tp, ep1)):
        pl.semaphore_signal(barrier, inc=1, device_id=(lax.axis_index('dp'), peer_tp, peer_ep), device_id_type=MESH)
    pl.semaphore_wait(barrier, 3)

    def arrived(ref, sem):
        remote(ref, ref, misc_send.at[0], sem, tp, ep).wait_recv()

    pieces = range(len(sources))
    send_entry = remote(theirs, x.at[:, my_pos, :], misc_send.at[0], misc_recv.at[0], other, ep)
    send_u = remote(table_ref, table_other, misc_send.at[1], misc_recv.at[1], other, ep)
    send_rest = remote(mine, x0t_ref.at[:, my_pos, :], misc_send.at[2], misc_recv.at[2], other, ep)
    y_copies = [remote(sources[n], places[n](ep), y_send.at[n], y_recv.at[n], other, ep) for n in pieces]
    x_copies = [remote(places[n](ep), places[n](ep), x_send.at[n], x_recv.at[n], tp, ep2) for n in pieces]
    c_copies = [remote(places[n](ep), places[n](ep), c_send.at[n], c_recv.at[n], tp, ep1) for n in pieces]
    d_copies = [remote(places[n](ep2), places[n](ep2), d_send.at[n], d_recv.at[n], tp, ep1) for n in pieces]
    send_u.start()
    send_entry.start()
    for copy in y_copies:
        copy.start()
    send_rest.start()

    def pass_on(n):
        arrived(places[n](ep), y_recv.at[n])
        x_copies[n].start()
        c_copies[n].start()

    def pass_across(n):
        arrived(places[n](ep2), x_recv.at[n])
        d_copies[n].start()

    def complete(n):
        arrived(places[n](ep1), c_recv.at[n])
        arrived(places[n](ep3), d_recv.at[n])

    def build_bias(rows_ref, side):
        u_rows[...] = bias_rows(rows_ref[...].reshape(u_rows.shape[0], rows_ref.shape[2]), seq_len)

        @pl.loop(0, 8)
        def _(n):
            layer, pair = n // 4, lax.rem(n, 4)
            for sub in range(2):
                row = u_rows[pl.ds(n * 2 + sub, 1), :]
                wide = pltpu.roll(jnp.broadcast_to(row, (seq_len, 2 * seq_len)), 0, 1, stride=1, stride_axis=0)
                at = slice(sub * half, (sub + 1) * half)
                place = layer * 8 + side * 4 + pair
                bias_low[place, at, :] = wide[:half, :half]
                bias_high[place, at, :] = wide[half:, :seq_len]

    def begin_layer(layer):
        @pl.loop(0, seqs)
        def _(s):
            rows = part(seq_len, s)
            a_ref[rows, :] = rms_rows(x[s], ln_attn_ref[layer])
            acc[rows, :] = x[s].astype(F32)

    def end_layer():
        @pl.loop(0, seqs)
        def _(s):
            x[s] = acc[part(seq_len, s), :].astype(BF16)

    first = lax.broadcasted_iota(jnp.int32, (1, 128), 1) < 64

    def attend(layer, side, block):
        cols = slice(block * quad, (block + 1) * quad)
        for kind in range(3):
            qkv[kind] = mm(a_ref[...], w[layer, side, kind, :, cols]).astype(BF16)

        @pl.loop(0, seqs)
        def _(s):
            rows = part(seq_len, s)
            for pair in range(quad // 128):
                lanes = slice(pair * 128, (pair + 1) * 128)
                place = layer * 8 + side * 4 + block * (quad // 128) + pair
                q, k, v = (qkv[kind, rows, lanes] for kind in range(3))
                none = jnp.zeros_like(q[:half])
                outs = []
                for upper in range(2):
                    qs = q[half:] if upper else q[:half]
                    ks, vs = (k, v) if upper else (k[:half], v[:half])
                    both = jnp.concatenate([jnp.where(first, qs, none), jnp.where(first, none, qs)], axis=0)
                    bias = bias_high[place] if upper else bias_low[place]
                    got = mm(softmax_bf16(mm_t(both, ks) * 0.125 + bias), vs)
                    outs.append(jnp.where(first, got[:half], got[half:]))
                ctx[rows, lanes] = jnp.concatenate(outs, axis=0).astype(BF16)

    def project(layer, side, block):
        cols = slice(block * quad, (block + 1) * quad)

        @pl.loop(0, seqs)
        def _(s):
            rows = part(seq_len, s)
            acc[rows, :] += mm(ctx[rows, :], wo[layer, side, cols, :])

    def dense(s):
        h = x[s]
        b = rms_rows(h, ln_ffn_ref[0])
        total = h.astype(F32)
        for side in range(2):
            hid = (jax.nn.gelu(mm(b, gu[side, 0])) * mm(b, gu[side, 1])).astype(BF16)
            total = total + mm(hid, wd[side])
        x[s] = total.astype(BF16)

    def heads(layer, side, block):
        attend(layer, side, block)
        project(layer, side, block)

    build_bias(table_ref, 0)
    arrived(table_other, misc_recv.at[1])
    build_bias(table_other, 1)
    own_stage.wait()
    own_x0t = pltpu.make_async_copy(stage, x0t_ref.at[:, my_pos, :], out_sem.at[0])
    own_x0t.start()

    with scope("w_entry"):
        own_x.wait()
        arrived(x.at[:, part(half, other), :], misc_recv.at[0])
    out_x0 = pltpu.make_async_copy(x, x0_ref, out_sem.at[1])
    out_x0.start()
    begin_layer(0)
    for n in range(4):
        own_loads[n].wait()
    heads(0, 0, 0)
    heads(0, 0, 1)
    with scope("w_l0_y"):
        for n in range(4):
            pass_on(n)
    with scope("w_l0_x"):
        for n in range(3):
            pass_across(n)
    with scope("w_l0_all"):
        for n in range(3):
            complete(n)
    attend(0, 1, 0)
    with scope("w_l0_o"):
        pass_across(3)
        pass_on(4)
        complete(3)
        pass_on(5)
    project(0, 1, 0)
    with scope("w_ffn_y"):
        pass_on(6)
    heads(0, 1, 1)
    with scope("w_ffn_x"):
        pass_on(7)
        for n in range(4, 7):
            pass_across(n)
    out_x0.wait()
    end_layer()
    with scope("w_ffn_all"):
        for n in range(4, 7):
            own_loads[n].wait()
            complete(n)

    @pl.loop(0, seqs // 2)
    def _(s):
        dense(s)

    with scope("w_l1_k"):
        pass_on(8)

    @pl.loop(seqs // 2, seqs)
    def _(s):
        dense(s)

    out_h1 = pltpu.make_async_copy(x, h1_ref, out_sem.at[2])
    out_h1.start()
    begin_layer(1)
    for n in range(7, 11):
        own_loads[n].wait()
    attend(1, 0, 0)
    with scope("w_l1_v"):
        pass_on(9)
    project(1, 0, 0)
    heads(1, 0, 1)
    with scope("w_l1_o"):
        pass_on(10)
    with scope("w_l1_x"):
        for n in range(7, 10):
            pass_across(n)
    with scope("w_l1_all"):
        for n in range(7, 10):
            complete(n)
    attend(1, 1, 0)
    with scope("w_l1_o_all"):
        pass_across(10)
        complete(10)
    project(1, 1, 0)
    heads(1, 1, 1)
    out_h1.wait()
    end_layer()
    out_h2 = pltpu.make_async_copy(x, h2_ref, out_sem.at[3])
    out_h2.start()

    with scope("w_rest"):
        arrived(x0t_ref.at[:, part(half, other), :], misc_recv.at[2])
    own_x0t.wait()
    for copy in [send_entry, send_u, send_rest] + y_copies + x_copies + c_copies + d_copies:
        copy.wait_send()
    out_h2.wait()


def dense_layers(hidden_in, ln_attn, ln_ffn, w_query, w_key, w_value, w_out, bias_table, w_gate, w_up, w_down):
    batch, positions, d_model = hidden_in.shape
    seqs, seq_len = batch // 2, 2 * positions
    inner = w_query.shape[2]
    any_spec = pl.BlockSpec(memory_space=pl.ANY)
    vmem_spec = pl.BlockSpec(memory_space=pltpu.VMEM)
    dma = pltpu.SemaphoreType.DMA
    shape = jax.ShapeDtypeStruct((seqs, seq_len, d_model), BF16)
    return pl.pallas_call(
        layers_body,
        in_specs=[any_spec, vmem_spec, vmem_spec] + [any_spec] * 4 + [vmem_spec] + [any_spec] * 3,
        out_specs=[any_spec] * 4,
        out_shape=[shape] * 4,
        scratch_shapes=[
            pltpu.VMEM(shape.shape, BF16),
            pltpu.VMEM((seqs * seq_len, d_model), BF16),
            pltpu.VMEM((seqs * seq_len, d_model), F32),
            pltpu.VMEM((2, 2, 3, d_model, inner), BF16),
            pltpu.VMEM((2, 2, inner, d_model), BF16),
            pltpu.VMEM((2, 2) + w_gate.shape, BF16),
            pltpu.VMEM((2,) + w_down.shape, BF16),
            pltpu.VMEM(bias_table.shape, F32),
            pltpu.VMEM((bias_table.shape[0] * bias_table.shape[1], 2 * seq_len), F32),
            pltpu.VMEM((16, seq_len, seq_len // 2), F32),
            pltpu.VMEM((16, seq_len, seq_len), F32),
            pltpu.VMEM((3, seqs * seq_len, 256), BF16),
            pltpu.VMEM((seqs * seq_len, 256), BF16),
            pltpu.VMEM((seqs, positions, d_model), BF16),
            dma((2,)), dma((11,)), dma((4,)), dma((3,)), dma((3,)),
        ] + [dma((11,))] * 8,
        compiler_params=pltpu.CompilerParams(vmem_limit_bytes=VMEM_LIMIT, collective_id=1, has_side_effects=True),
        cost_estimate=pl.CostEstimate(flops=32_000_000_000, bytes_accessed=40 << 20, transcendentals=0),
        name="dense_layers",
    )(hidden_in, ln_attn, ln_ffn, w_query, w_key, w_value, w_out, bias_table, w_gate, w_up, w_down)


def moe_body(h2_ref, h1_ref, x0_ref, x0t_ref, ids_ref, ln_ffn_ref, ln_attn_ref, router_ref,
             w_in_hbm, w_out_hbm, wk_hbm, wv_hbm,
             out_ref, k_ref, v_ref, h1t_ref,
             hall, res, ret, w_in, w_out, wkv, acc, slot_row_ref, slots_all, columns_ref, gates, xbuf, kvbuf,
             in_sem, cache_sem, store_sem, slot_send, slot_recv, hs_send, hs_recv, ret_send, ret_recv, h1_send, h1_recv):
    tp, ep = lax.axis_index('tp'), lax.axis_index('ep')
    other = 1 - tp
    ep1, ep2, ep3 = axis_neighbours(tp, ep)
    me = tp * 4 + ep
    seqs, seq_len, d_model = h2_ref.shape
    tokens = acc.shape[0]
    rows = res.shape[1]
    half_pos = seq_len // 2
    experts = w_in.shape[0]
    capacity = rows // experts

    loads = [pltpu.make_async_copy(a, b, in_sem.at[n]) for n, (a, b) in enumerate((
        (x0_ref, xbuf), (wk_hbm, wkv.at[0]), (wv_hbm, wkv.at[1]), (h2_ref, hall.at[me]),
        (w_in_hbm, w_in), (w_out_hbm, w_out)))]
    for load in loads:
        load.start()

    barrier = pltpu.get_barrier_semaphore()
    peers = [(other, ep), (tp, ep2), (tp, ep1), (other, ep1), (other, ep2), (tp, ep3), (other, ep3)]
    for peer_tp, peer_ep in peers:
        pl.semaphore_signal(barrier, inc=1, device_id=(lax.axis_index('dp'), peer_tp, peer_ep), device_id_type=MESH)
    pl.semaphore_wait(barrier, len(peers))

    def half_at(k):
        return pl.ds(pl.multiple_of(k * half_pos, half_pos), half_pos)

    def block(owner, k):
        return hall.at[owner, :, half_at(k), :]

    sends = []
    for n, peer in enumerate(((other, ep), (tp, ep2), (tp, ep1))):
        for k in ((tp, other) if n == 0 else (other, tp)):
            sends.append(remote(h2_ref.at[:, half_at(k), :], block(me, k), hs_send.at[n, k], hs_recv.at[me, k], *peer))
    for copy in sends:
        copy.start()
    send_h1 = remote(h1_ref, h1t_ref, h1_send, h1_recv, other, ep)
    send_h1.start()

    def arrived(ref, sem):
        remote(ref, ref, hs_send.at[0], sem, tp, ep).wait_recv()

    def block_arrived(owner, k):
        arrived(block(owner, k), hs_recv.at[owner, k])

    def forward(n, owner, k, *peer):
        copy = remote(block(owner, k), block(owner, k), hs_send.at[n, k], hs_recv.at[owner, k], *peer)
        copy.start()
        sends.append(copy)

    num_experts = router_ref.shape[0]
    ids_row = jnp.concatenate([ids_ref[s] for s in range(ids_ref.shape[0])], axis=1)
    expert = lax.broadcasted_iota(jnp.int32, (num_experts, tokens), 0)
    hot = [jnp.where(ids_row[c:c + 1] == expert, 1.0, 0.0) for c in range(2)]
    earlier = lax.broadcasted_iota(jnp.int32, (tokens, tokens), 0) <= lax.broadcasted_iota(jnp.int32, (tokens, tokens), 1)
    upto = mm(jnp.concatenate(hot, axis=0).astype(BF16), jnp.where(earlier, 1.0, 0.0).astype(BF16))
    base = (0.0, upto[:num_experts, tokens - 1:])
    wide_ids = ids_row.astype(F32)
    slot_rows = []
    for c in range(2):
        place = jnp.sum((upto[c * num_experts:(c + 1) * num_experts] - 1.0 + base[c]) * hot[c], axis=0, keepdims=True)
        slot_rows.append(jnp.where(place < capacity, wide_ids[c:c + 1] * capacity + place, -1.0))
    packed = jnp.concatenate(slot_rows + [wide_ids, jnp.zeros((4, tokens), F32)], axis=0)
    slot_row_ref[...] = packed[:2].astype(jnp.int32)
    slots_all[me] = packed[:2].astype(jnp.int32)
    columns_ref[...] = packed.T.astype(jnp.int32)

    def cache_part(source, layer, owner, load=None):
        if load is None:
            load = pltpu.make_async_copy(source, xbuf, cache_sem)
            load.start()
        load.wait()

        @pl.loop(0, seqs)
        def _(s):
            a = rms_rows(xbuf[s], ln_attn_ref[layer])
            for n, ref in enumerate((k_ref, v_ref)):
                full = mm(a, wkv[n, layer])
                kvbuf[s, n] = full.T.astype(BF16).reshape(kvbuf.shape[2:])
                pltpu.make_async_copy(kvbuf.at[s, n], ref.at[layer, owner * seqs + s], store_sem.at[s, n]).start()

        @pl.loop(0, seqs)
        def _(s):
            for n, ref in enumerate((k_ref, v_ref)):
                pltpu.make_async_copy(kvbuf.at[s, n], ref.at[layer, owner * seqs + s], store_sem.at[s, n]).wait()

    loads[1].wait()
    loads[2].wait()
    cache_part(x0_ref, 0, tp, loads[0])
    cache_part(x0t_ref, 0, other)
    cache_part(h1_ref, 1, tp)

    slot_copies = [remote(slot_row_ref, slots_all.at[me], slot_send.at[n], slot_recv.at[me], *peer) for n, peer in enumerate(peers)]
    for copy in slot_copies:
        copy.start()

    y_owner, x_owner, c_owner = other * 4 + ep, tp * 4 + ep2, tp * 4 + ep1
    yx_owner, yc_owner, xc_owner, yxc_owner = other * 4 + ep2, other * 4 + ep1, tp * 4 + ep3, other * 4 + ep3
    for place, k in enumerate((other, tp)):
        with scope(f"w_y{place}"):
            block_arrived(y_owner, k)
        forward(3, y_owner, k, tp, ep2)
        forward(4, y_owner, k, tp, ep1)
    loads[3].wait()

    def own_tokens(owner):
        return hall[owner, :, half_at(tp), :].reshape(tokens // 2, d_model)

    for part in range(2):
        at = slice(part * (tokens // 2), (part + 1) * (tokens // 2))
        h_own = own_tokens(part * 4 + ep)
        acc[at] = h_own.astype(F32)
        b = rms_rows(h_own, ln_ffn_ref[1])
        logits = lax.dot_general(b.astype(F32), router_ref[...], (((1,), (1,)), ((), ())),
                                 precision=lax.Precision.HIGHEST, preferred_element_type=F32)
        grown = jnp.exp(logits - jnp.max(logits, axis=-1, keepdims=True))
        probs = grown / jnp.sum(grown, axis=-1, keepdims=True)
        lanes = lax.broadcasted_iota(jnp.int32, probs.shape, 1)
        picked = [jnp.sum(jnp.where(columns_ref[at, 2 + c:3 + c] == lanes, probs, 0.0), axis=-1, keepdims=True) for c in range(2)]
        both = picked[0] + picked[1]
        gates[at, 0:1] = picked[0] / both
        gates[at, 1:2] = picked[1] / both

    with scope("w_x"):
        for k in (other, tp):
            block_arrived(x_owner, k)
            forward(5, x_owner, k, tp, ep1)
    for peer_tp, peer_ep in peers:
        arrived(slots_all.at[peer_tp * 4 + peer_ep], slot_recv.at[peer_tp * 4 + peer_ep])
    loads[4].wait()
    loads[5].wait()

    def run_group(i, k):
        dest = k * 4 + i
        slots = slots_all[dest]
        want = me * rows + lax.broadcasted_iota(jnp.int32, (rows, tokens // 2), 0)
        chosen = None
        for part in range(2):
            h = hall[part * 4 + i, :, half_at(k), :].reshape(tokens // 2, d_model)
            at = slice(part * (tokens // 2), (part + 1) * (tokens // 2))
            pick = jnp.logical_or(slots[0:1, at] == want, slots[1:2, at] == want)
            term = mm(jnp.where(pick, 1.0, 0.0).astype(BF16), h)
            chosen = term if chosen is None else chosen + term
        b = rms_rows(chosen, ln_ffn_ref[1])
        for e in range(experts):
            at = slice(e * capacity, (e + 1) * capacity)
            hid = jax.nn.gelu(mm(b[at], w_in[e])).astype(BF16)
            res[dest, at] = mm(hid, w_out[e]).astype(BF16)
        return dest

    def give_back(i, k):
        dest = k * 4 + i
        return remote(res.at[dest], ret.at[me], ret_send.at[dest], ret_recv.at[me], k, i)

    def add_rows(source_ref, owner):
        step = 256

        @pl.loop(0, tokens // step)
        def _(r):
            at = pl.ds(pl.multiple_of(r * step, step), step)
            columns = owner * rows + lax.broadcasted_iota(jnp.int32, (step, rows), 1)
            total = acc[at, :]
            for c in range(2):
                pick = jnp.where(columns_ref[at, c:c + 1] == columns, 1.0, 0.0).astype(BF16)
                total = total + gates[at, c:c + 1] * mm(pick, source_ref[...])
            acc[at, :] = total

    with scope("w_yc"):
        for k in range(2):
            block_arrived(c_owner, k)
            block_arrived(yc_owner, k)

    @pl.loop(0, 4)
    def _(t):
        late = t // 2
        beside = lax.rem((t + 1) // 2, 2)
        i = ep + beside * (ep1 - ep)
        k = late * tp + (1 - late) * other
        run_group(i, k)

        @pl.when(t < 3)
        def _():
            give_back(i, k).start()

    add_rows(res.at[me], me)

    for place, k in enumerate((other, tp)):
        with scope(f"w_yx{place}"):
            block_arrived(yx_owner, k)
        forward(6, yx_owner, k, tp, ep1)
        with scope(f"w_far{place}"):
            block_arrived(xc_owner, k)
            block_arrived(yxc_owner, k)

        @pl.loop(0, 2)
        def _(t):
            i = (1 - t) * ep2 + t * ep3
            run_group(i, k)
            give_back(i, k).start()

        if place == 0:
            with scope("w_h1"):
                arrived(h1t_ref, h1_recv)
            cache_part(h1t_ref, 1, other)

    for peer_tp, peer_ep in ((tp, ep1), (other, ep), (other, ep1), (other, ep2), (other, ep3), (tp, ep2), (tp, ep3)):
        owner = peer_tp * 4 + peer_ep
        with scope("w_ret"):
            arrived(ret.at[owner], ret_recv.at[owner])
        add_rows(ret.at[owner], owner)
    out_ref[...] = acc[...].astype(BF16)

    for copy in sends + slot_copies + [send_h1]:
        copy.wait_send()
    for peer_tp, peer_ep in peers:
        give_back(peer_ep, peer_tp).wait_send()


def moe_layer(h2, h1, x0, x0t, expert_ids, ln_ffn, ln_attn, w_router, expert_in, expert_out, w_key, w_value):
    seqs, seq_len, d_model = h2.shape
    tokens = seqs * seq_len
    experts, _, d_ff = expert_in.shape
    groups = 8
    rows = experts * 4 * tokens // (experts * groups)
    inner = w_key.shape[2]
    heads = inner // 64
    any_spec = pl.BlockSpec(memory_space=pl.ANY)
    vmem_spec = pl.BlockSpec(memory_space=pltpu.VMEM)
    cache_shape = jax.ShapeDtypeStruct((2, 2 * seqs, heads, 64, seq_len), BF16)
    dma = pltpu.SemaphoreType.DMA
    return pl.pallas_call(
        moe_body,
        in_specs=[any_spec] * 4 + [vmem_spec] * 4 + [any_spec] * 4,
        out_specs=[vmem_spec, any_spec, any_spec, any_spec],
        out_shape=[jax.ShapeDtypeStruct((tokens, d_model), BF16), cache_shape, cache_shape, jax.ShapeDtypeStruct(h1.shape, BF16)],
        scratch_shapes=[
            pltpu.VMEM((groups,) + h2.shape, BF16),
            pltpu.VMEM((groups, rows, d_model), BF16),
            pltpu.VMEM((groups, rows, d_model), BF16),
            pltpu.VMEM(expert_in.shape, BF16),
            pltpu.VMEM(expert_out.shape, BF16),
            pltpu.VMEM((2, 2, d_model, inner), BF16),
            pltpu.VMEM((tokens, d_model), F32),
            pltpu.VMEM((2, tokens), jnp.int32),
            pltpu.VMEM((groups, 2, tokens), jnp.int32),
            pltpu.VMEM((tokens, 8), jnp.int32),
            pltpu.VMEM((tokens, 2), F32),
            pltpu.VMEM(h1.shape, BF16),
            pltpu.VMEM((seqs, 2, heads, 64, seq_len), BF16),
            dma((6,)), dma, dma((seqs, 2)), dma((7,)), dma((groups,)), dma((7, 2)), dma((groups, 2)),
            dma((groups,)), dma((groups,)), dma, dma,
        ],
        compiler_params=pltpu.CompilerParams(vmem_limit_bytes=67043328, collective_id=2, has_side_effects=True),
        cost_estimate=pl.CostEstimate(flops=40_000_000_000, bytes_accessed=64 << 20, transcendentals=0),
        name="moe",
    )(h2, h1, x0, x0t, jnp.swapaxes(expert_ids, 1, 2), ln_ffn, ln_attn, w_router.T, expert_in, expert_out, w_key, w_value)


def solution(mesh):
    act_spec = P(('dp', 'ep'), 'tp', None)
    col_spec = P(None, None, 'tp')
    row_spec = P(None, 'tp', None)
    expert_spec = P(('tp', 'ep'), None, None)
    cache_spec = P(None, ('dp', 'ep'), 'tp', None, None)
    in_specs = (act_spec, P(), P(), col_spec, col_spec, col_spec, row_spec, row_spec,
                P(None, 'tp'), P(None, 'tp'), P('tp', None), P(), expert_spec, expert_spec, act_spec)

    def device_fn(hidden_in, ln_attn, ln_ffn, w_query, w_key, w_value, w_out, bias_table, w_gate, w_up, w_down, w_router, expert_in, expert_out, expert_ids):
        h1, h2, x0, x0t = dense_layers(hidden_in, ln_attn, ln_ffn, w_query, w_key, w_value, w_out, bias_table, w_gate, w_up, w_down)
        hidden, k_cache, v_cache, _ = moe_layer(
            h2, h1, x0, x0t, expert_ids, ln_ffn, ln_attn, w_router, expert_in, expert_out, w_key, w_value)
        return hidden.reshape(hidden_in.shape), jnp.swapaxes(k_cache, 3, 4), jnp.swapaxes(v_cache, 3, 4)

    return jax.shard_map(device_fn, mesh=mesh, in_specs=in_specs, out_specs=(act_spec, cache_spec, cache_spec), check_vma=False)
```

```python
import contextlib

import jax
import jax.numpy as jnp
from jax import lax
from jax.experimental import pallas as pl
from jax.experimental.pallas import tpu as pltpu
from jax.sharding import PartitionSpec as P

EXACT_BUCKETS = 16
THRESHOLDS = (18, 20, 23, 26, 30, 34, 39, 45, 51, 58, 66, 76, 86, 98, 112)
EPSILON = 1e-6
F32 = jnp.float32
BF16 = jnp.bfloat16
VMEM_LIMIT = 60 * 1024 * 1024
MESH = pl.DeviceIdType.MESH


def scope(name):
    return contextlib.nullcontext()


def rms_rows(rows, ln_scale):
    wide = rows.astype(F32)
    inv_rms = lax.rsqrt(jnp.mean(wide * wide, axis=-1, keepdims=True) + EPSILON)
    return (wide * inv_rms * ln_scale).astype(BF16)


def mm(a, b):
    return lax.dot_general(a, b, (((1,), (0,)), ((), ())), preferred_element_type=F32)


def mm_t(a, b):
    return lax.dot_general(a, b, (((1,), (1,)), ((), ())), preferred_element_type=F32)


def bias_rows(table, seq_len):
    at = lax.broadcasted_iota(jnp.int32, (table.shape[1], 2 * seq_len), 1)
    rel = jnp.where(at == 0, 0, 2 * seq_len - at)
    bucket = jnp.minimum(rel, EXACT_BUCKETS)
    for threshold in THRESHOLDS:
        bucket = bucket + jnp.where(rel >= threshold, 1, 0)
    hot = jnp.where(bucket == lax.broadcasted_iota(jnp.int32, bucket.shape, 0), 1.0, 0.0)
    rows = jnp.dot(table, hot, precision=lax.Precision.HIGHEST, preferred_element_type=F32)
    return jnp.where(rel[:1] < seq_len, rows, -jnp.inf)


def softmax_bf16(scores):
    top = jnp.max(scores, axis=-1, keepdims=True)
    grown = jnp.exp(scores - top)
    return (grown * (1.0 / jnp.sum(grown, axis=-1, keepdims=True))).astype(BF16)


def axis_neighbours(tp, ep):
    core = lax.rem(ep, 2)
    beside = ep + 1 - 2 * core
    return beside, lax.rem(ep + 2, 4), lax.rem(beside + 2, 4)


def remote(src, dst, send, recv, tp, ep):
    return pltpu.make_async_remote_copy(
        src_ref=src, dst_ref=dst, send_sem=send, recv_sem=recv,
        device_id=(lax.axis_index('dp'), tp, ep), device_id_type=MESH)


def layers_body(hid_ref, ln_attn_ref, ln_ffn_ref, wq_hbm, wk_hbm, wv_hbm, wo_hbm, table_ref, wg_hbm, wu_hbm, wd_hbm,
                h1_ref, h2_ref, x0_ref, x0t_ref,
                x, a_ref, acc, w, wo, gu, wd, table_other, u_rows, bias_low, bias_high, qkv, ctx, stage,
                in_sem, own_sem, out_sem, misc_send, misc_recv, y_send, y_recv, x_send, x_recv, c_send, c_recv, d_send, d_recv):
    tp, ep = lax.axis_index('tp'), lax.axis_index('ep')
    other = 1 - tp
    ep1, ep2, ep3 = axis_neighbours(tp, ep)
    seqs, seq_len, d_model = x.shape
    half = seq_len // 2
    tokens = seqs * seq_len
    quad = qkv.shape[2]

    def part(count, quarter):
        return pl.ds(pl.multiple_of(quarter * count, count), count)

    my_pos = part(half, tp)
    mine = hid_ref.at[pl.ds(tp * seqs, seqs)]
    theirs = hid_ref.at[pl.ds(other * seqs, seqs)]

    sources, places = [], []
    for layer in range(2):
        for kind, hbm in enumerate((wq_hbm, wk_hbm, wv_hbm)):
            sources.append(hbm.at[layer, part(256, ep), :])
            places.append(lambda q, layer=layer, kind=kind: w.at[layer, 1, kind, part(256, q), :])
        sources.append(wo_hbm.at[layer, part(128, ep), :])
        places.append(lambda q, layer=layer: wo.at[layer, 1, part(128, q), :])
        if layer == 0:
            for kind, hbm in enumerate((wg_hbm, wu_hbm)):
                sources.append(hbm.at[part(256, ep), :])
                places.append(lambda q, kind=kind: gu.at[1, kind, part(256, q), :])
            sources.append(wd_hbm.at[part(64, ep), :])
            places.append(lambda q: wd.at[1, part(64, q), :])

    own_x = pltpu.make_async_copy(mine, x.at[:, my_pos, :], in_sem.at[0])
    own_stage = pltpu.make_async_copy(theirs, stage, in_sem.at[1])
    own_x.start()
    own_loads = []
    for layer in range(2):
        for kind, hbm in enumerate((wq_hbm, wk_hbm, wv_hbm)):
            own_loads.append((hbm.at[layer], w.at[layer, 0, kind]))
        own_loads.append((wo_hbm.at[layer], wo.at[layer, 0]))
        if layer == 0:
            own_loads += [(wg_hbm, gu.at[0, 0]), (wu_hbm, gu.at[0, 1]), (wd_hbm, wd.at[0])]
    own_loads = [pltpu.make_async_copy(s, d, own_sem.at[n]) for n, (s, d) in enumerate(own_loads)]
    for load in own_loads:
        load.start()
    own_stage.start()

    barrier = pltpu.get_barrier_semaphore()
    for peer_tp, peer_ep in ((other, ep), (tp, ep2), (tp, ep1)):
        pl.semaphore_signal(barrier, inc=1, device_id=(lax.axis_index('dp'), peer_tp, peer_ep), device_id_type=MESH)
    pl.semaphore_wait(barrier, 3)

    def arrived(ref, sem):
        remote(ref, ref, misc_send.at[0], sem, tp, ep).wait_recv()

    pieces = range(len(sources))
    send_entry = remote(theirs, x.at[:, my_pos, :], misc_send.at[0], misc_recv.at[0], other, ep)
    send_u = remote(table_ref, table_other, misc_send.at[1], misc_recv.at[1], other, ep)
    send_rest = remote(mine, x0t_ref.at[:, my_pos, :], misc_send.at[2], misc_recv.at[2], other, ep)
    y_copies = [remote(sources[n], places[n](ep), y_send.at[n], y_recv.at[n], other, ep) for n in pieces]
    x_copies = [remote(places[n](ep), places[n](ep), x_send.at[n], x_recv.at[n], tp, ep2) for n in pieces]
    c_copies = [remote(places[n](ep), places[n](ep), c_send.at[n], c_recv.at[n], tp, ep1) for n in pieces]
    d_copies = [remote(places[n](ep2), places[n](ep2), d_send.at[n], d_recv.at[n], tp, ep1) for n in pieces]
    send_u.start()
    send_entry.start()
    for copy in y_copies:
        copy.start()
    send_rest.start()

    def pass_on(n):
        arrived(places[n](ep), y_recv.at[n])
        x_copies[n].start()
        c_copies[n].start()

    def pass_across(n):
        arrived(places[n](ep2), x_recv.at[n])
        d_copies[n].start()

    def complete(n):
        arrived(places[n](ep1), c_recv.at[n])
        arrived(places[n](ep3), d_recv.at[n])

    def build_bias(rows_ref, side):
        u_rows[...] = bias_rows(rows_ref[...].reshape(u_rows.shape[0], rows_ref.shape[2]), seq_len)

        @pl.loop(0, 8)
        def _(n):
            layer, pair = n // 4, lax.rem(n, 4)
            for sub in range(2):
                row = u_rows[pl.ds(n * 2 + sub, 1), :]
                wide = pltpu.roll(jnp.broadcast_to(row, (seq_len, 2 * seq_len)), 0, 1, stride=1, stride_axis=0)
                at = slice(sub * half, (sub + 1) * half)
                place = layer * 8 + side * 4 + pair
                bias_low[place, at, :] = wide[:half, :half]
                bias_high[place, at, :] = wide[half:, :seq_len]

    def begin_layer(layer):
        @pl.loop(0, seqs)
        def _(s):
            rows = part(seq_len, s)
            a_ref[rows, :] = rms_rows(x[s], ln_attn_ref[layer])
            acc[rows, :] = x[s].astype(F32)

    def end_layer():
        @pl.loop(0, seqs)
        def _(s):
            x[s] = acc[part(seq_len, s), :].astype(BF16)

    first = lax.broadcasted_iota(jnp.int32, (1, 128), 1) < 64

    def attend(layer, side, block):
        cols = slice(block * quad, (block + 1) * quad)
        for kind in range(3):
            qkv[kind] = mm(a_ref[...], w[layer, side, kind, :, cols]).astype(BF16)

        @pl.loop(0, seqs)
        def _(s):
            rows = part(seq_len, s)
            for pair in range(quad // 128):
                lanes = slice(pair * 128, (pair + 1) * 128)
                place = layer * 8 + side * 4 + block * (quad // 128) + pair
                q, k, v = (qkv[kind, rows, lanes] for kind in range(3))
                none = jnp.zeros_like(q[:half])
                outs = []
                for upper in range(2):
                    qs = q[half:] if upper else q[:half]
                    ks, vs = (k, v) if upper else (k[:half], v[:half])
                    both = jnp.concatenate([jnp.where(first, qs, none), jnp.where(first, none, qs)], axis=0)
                    bias = bias_high[place] if upper else bias_low[place]
                    got = mm(softmax_bf16(mm_t(both, ks) * 0.125 + bias), vs)
                    outs.append(jnp.where(first, got[:half], got[half:]))
                ctx[rows, lanes] = jnp.concatenate(outs, axis=0).astype(BF16)

    def project(layer, side, block):
        cols = slice(block * quad, (block + 1) * quad)

        @pl.loop(0, seqs)
        def _(s):
            rows = part(seq_len, s)
            acc[rows, :] += mm(ctx[rows, :], wo[layer, side, cols, :])

    def dense(s):
        h = x[s]
        b = rms_rows(h, ln_ffn_ref[0])
        total = h.astype(F32)
        for side in range(2):
            hid = (jax.nn.gelu(mm(b, gu[side, 0])) * mm(b, gu[side, 1])).astype(BF16)
            total = total + mm(hid, wd[side])
        x[s] = total.astype(BF16)

    def heads(layer, side, block):
        attend(layer, side, block)
        project(layer, side, block)

    build_bias(table_ref, 0)
    arrived(table_other, misc_recv.at[1])
    build_bias(table_other, 1)
    own_stage.wait()
    own_x0t = pltpu.make_async_copy(stage, x0t_ref.at[:, my_pos, :], out_sem.at[0])
    own_x0t.start()

    with scope("w_entry"):
        own_x.wait()
        arrived(x.at[:, part(half, other), :], misc_recv.at[0])
    out_x0 = pltpu.make_async_copy(x, x0_ref, out_sem.at[1])
    out_x0.start()
    begin_layer(0)
    for n in range(4):
        own_loads[n].wait()
    heads(0, 0, 0)
    heads(0, 0, 1)
    with scope("w_l0_y"):
        for n in range(4):
            pass_on(n)
    with scope("w_l0_x"):
        for n in range(3):
            pass_across(n)
    with scope("w_l0_all"):
        for n in range(3):
            complete(n)
    attend(0, 1, 0)
    with scope("w_l0_o"):
        pass_across(3)
        pass_on(4)
        complete(3)
        pass_on(5)
    project(0, 1, 0)
    with scope("w_ffn_y"):
        pass_on(6)
    heads(0, 1, 1)
    with scope("w_ffn_x"):
        pass_on(7)
        for n in range(4, 7):
            pass_across(n)
    out_x0.wait()
    end_layer()
    with scope("w_ffn_all"):
        for n in range(4, 7):
            own_loads[n].wait()
            complete(n)

    @pl.loop(0, seqs // 2)
    def _(s):
        dense(s)

    with scope("w_l1_k"):
        pass_on(8)

    @pl.loop(seqs // 2, seqs)
    def _(s):
        dense(s)

    out_h1 = pltpu.make_async_copy(x, h1_ref, out_sem.at[2])
    out_h1.start()
    begin_layer(1)
    for n in range(7, 11):
        own_loads[n].wait()
    attend(1, 0, 0)
    with scope("w_l1_v"):
        pass_on(9)
    project(1, 0, 0)
    heads(1, 0, 1)
    with scope("w_l1_o"):
        pass_on(10)
    with scope("w_l1_x"):
        for n in range(7, 10):
            pass_across(n)
    with scope("w_l1_all"):
        for n in range(7, 10):
            complete(n)
    attend(1, 1, 0)
    with scope("w_l1_o_all"):
        pass_across(10)
        complete(10)
    project(1, 1, 0)
    heads(1, 1, 1)
    out_h1.wait()
    end_layer()
    out_h2 = pltpu.make_async_copy(x, h2_ref, out_sem.at[3])
    out_h2.start()

    with scope("w_rest"):
        arrived(x0t_ref.at[:, part(half, other), :], misc_recv.at[2])
    own_x0t.wait()
    for copy in [send_entry, send_u, send_rest] + y_copies + x_copies + c_copies + d_copies:
        copy.wait_send()
    out_h2.wait()


def dense_layers(hidden_in, ln_attn, ln_ffn, w_query, w_key, w_value, w_out, bias_table, w_gate, w_up, w_down):
    batch, positions, d_model = hidden_in.shape
    seqs, seq_len = batch // 2, 2 * positions
    inner = w_query.shape[2]
    any_spec = pl.BlockSpec(memory_space=pl.ANY)
    vmem_spec = pl.BlockSpec(memory_space=pltpu.VMEM)
    dma = pltpu.SemaphoreType.DMA
    shape = jax.ShapeDtypeStruct((seqs, seq_len, d_model), BF16)
    return pl.pallas_call(
        layers_body,
        in_specs=[any_spec, vmem_spec, vmem_spec] + [any_spec] * 4 + [vmem_spec] + [any_spec] * 3,
        out_specs=[any_spec] * 4,
        out_shape=[shape] * 4,
        scratch_shapes=[
            pltpu.VMEM(shape.shape, BF16),
            pltpu.VMEM((seqs * seq_len, d_model), BF16),
            pltpu.VMEM((seqs * seq_len, d_model), F32),
            pltpu.VMEM((2, 2, 3, d_model, inner), BF16),
            pltpu.VMEM((2, 2, inner, d_model), BF16),
            pltpu.VMEM((2, 2) + w_gate.shape, BF16),
            pltpu.VMEM((2,) + w_down.shape, BF16),
            pltpu.VMEM(bias_table.shape, F32),
            pltpu.VMEM((bias_table.shape[0] * bias_table.shape[1], 2 * seq_len), F32),
            pltpu.VMEM((16, seq_len, seq_len // 2), F32),
            pltpu.VMEM((16, seq_len, seq_len), F32),
            pltpu.VMEM((3, seqs * seq_len, 256), BF16),
            pltpu.VMEM((seqs * seq_len, 256), BF16),
            pltpu.VMEM((seqs, positions, d_model), BF16),
            dma((2,)), dma((11,)), dma((4,)), dma((3,)), dma((3,)),
        ] + [dma((11,))] * 8,
        compiler_params=pltpu.CompilerParams(vmem_limit_bytes=VMEM_LIMIT, collective_id=1, has_side_effects=True),
        cost_estimate=pl.CostEstimate(flops=32_000_000_000, bytes_accessed=40 << 20, transcendentals=0),
        name="dense_layers",
    )(hidden_in, ln_attn, ln_ffn, w_query, w_key, w_value, w_out, bias_table, w_gate, w_up, w_down)


def moe_body(h2_ref, h1_ref, x0_ref, x0t_ref, ids_ref, ln_ffn_ref, ln_attn_ref, router_ref,
             w_in_hbm, w_out_hbm, wk_hbm, wv_hbm,
             out_ref, k_ref, v_ref, h1t_ref,
             hall, res, ret, w_in, w_out, wkv, acc, slot_row_ref, slots_all, columns_ref, gates, xbuf, kvbuf,
             in_sem, cache_sem, store_sem, slot_send, slot_recv, hs_send, hs_recv, ret_send, ret_recv, h1_send, h1_recv):
    tp, ep = lax.axis_index('tp'), lax.axis_index('ep')
    other = 1 - tp
    ep1, ep2, ep3 = axis_neighbours(tp, ep)
    me = tp * 4 + ep
    seqs, seq_len, d_model = h2_ref.shape
    tokens = acc.shape[0]
    rows = res.shape[1]
    half_pos = seq_len // 2
    experts = w_in.shape[0]
    capacity = rows // experts

    loads = [pltpu.make_async_copy(a, b, in_sem.at[n]) for n, (a, b) in enumerate((
        (x0_ref, xbuf), (wk_hbm, wkv.at[0]), (wv_hbm, wkv.at[1]), (h2_ref, hall.at[me]),
        (w_in_hbm, w_in), (w_out_hbm, w_out)))]
    for load in loads:
        load.start()

    barrier = pltpu.get_barrier_semaphore()
    peers = [(other, ep), (tp, ep2), (tp, ep1), (other, ep1), (other, ep2), (tp, ep3), (other, ep3)]
    for peer_tp, peer_ep in peers:
        pl.semaphore_signal(barrier, inc=1, device_id=(lax.axis_index('dp'), peer_tp, peer_ep), device_id_type=MESH)
    pl.semaphore_wait(barrier, len(peers))

    def half_at(k):
        return pl.ds(pl.multiple_of(k * half_pos, half_pos), half_pos)

    def block(owner, k):
        return hall.at[owner, :, half_at(k), :]

    sends = []
    for n, peer in enumerate(((other, ep), (tp, ep2), (tp, ep1))):
        for k in ((other, tp) if n == 0 else (tp, other)):
            sends.append(remote(h2_ref.at[:, half_at(k), :], block(me, k), hs_send.at[n, k], hs_recv.at[me, k], *peer))
    for copy in sends:
        copy.start()
    send_h1 = remote(h1_ref, h1t_ref, h1_send, h1_recv, other, ep)
    send_h1.start()

    def arrived(ref, sem):
        remote(ref, ref, hs_send.at[0], sem, tp, ep).wait_recv()

    def block_arrived(owner, k):
        arrived(block(owner, k), hs_recv.at[owner, k])

    def forward(n, owner, k, *peer):
        copy = remote(block(owner, k), block(owner, k), hs_send.at[n, k], hs_recv.at[owner, k], *peer)
        copy.start()
        sends.append(copy)

    num_experts = router_ref.shape[0]
    ids_row = jnp.concatenate([ids_ref[s] for s in range(ids_ref.shape[0])], axis=1)
    expert = lax.broadcasted_iota(jnp.int32, (num_experts, tokens), 0)
    hot = [jnp.where(ids_row[c:c + 1] == expert, 1.0, 0.0) for c in range(2)]
    earlier = lax.broadcasted_iota(jnp.int32, (tokens, tokens), 0) <= lax.broadcasted_iota(jnp.int32, (tokens, tokens), 1)
    upto = mm(jnp.concatenate(hot, axis=0).astype(BF16), jnp.where(earlier, 1.0, 0.0).astype(BF16))
    base = (0.0, upto[:num_experts, tokens - 1:])
    wide_ids = ids_row.astype(F32)
    slot_rows = []
    for c in range(2):
        place = jnp.sum((upto[c * num_experts:(c + 1) * num_experts] - 1.0 + base[c]) * hot[c], axis=0, keepdims=True)
        slot_rows.append(jnp.where(place < capacity, wide_ids[c:c + 1] * capacity + place, -1.0))
    packed = jnp.concatenate(slot_rows + [wide_ids, jnp.zeros((4, tokens), F32)], axis=0)
    slot_row_ref[...] = packed[:2].astype(jnp.int32)
    slots_all[me] = packed[:2].astype(jnp.int32)
    columns_ref[...] = packed.T.astype(jnp.int32)

    def cache_part(source, layer, owner, load=None):
        if load is None:
            load = pltpu.make_async_copy(source, xbuf, cache_sem)
            load.start()
        load.wait()

        @pl.loop(0, seqs)
        def _(s):
            a = rms_rows(xbuf[s], ln_attn_ref[layer])
            for n, ref in enumerate((k_ref, v_ref)):
                full = mm(a, wkv[n, layer])
                kvbuf[s, n] = full.T.astype(BF16).reshape(kvbuf.shape[2:])
                pltpu.make_async_copy(kvbuf.at[s, n], ref.at[layer, owner * seqs + s], store_sem.at[s, n]).start()

        @pl.loop(0, seqs)
        def _(s):
            for n, ref in enumerate((k_ref, v_ref)):
                pltpu.make_async_copy(kvbuf.at[s, n], ref.at[layer, owner * seqs + s], store_sem.at[s, n]).wait()

    loads[1].wait()
    loads[2].wait()
    cache_part(x0_ref, 0, tp, loads[0])
    cache_part(x0t_ref, 0, other)
    cache_part(h1_ref, 1, tp)

    slot_copies = [remote(slot_row_ref, slots_all.at[me], slot_send.at[n], slot_recv.at[me], *peer) for n, peer in enumerate(peers)]
    for copy in slot_copies:
        copy.start()

    y_owner, x_owner, c_owner = other * 4 + ep, tp * 4 + ep2, tp * 4 + ep1
    yx_owner, yc_owner, xc_owner, yxc_owner = other * 4 + ep2, other * 4 + ep1, tp * 4 + ep3, other * 4 + ep3
    for place, k in enumerate((tp, other)):
        with scope(f"w_y{place}"):
            block_arrived(y_owner, k)
        forward(3, y_owner, k, tp, ep2)
        forward(4, y_owner, k, tp, ep1)
    loads[3].wait()

    def own_tokens(owner):
        return hall[owner, :, half_at(tp), :].reshape(tokens // 2, d_model)

    for part in range(2):
        at = slice(part * (tokens // 2), (part + 1) * (tokens // 2))
        h_own = own_tokens(part * 4 + ep)
        acc[at] = h_own.astype(F32)
        b = rms_rows(h_own, ln_ffn_ref[1])
        logits = lax.dot_general(b.astype(F32), router_ref[...], (((1,), (1,)), ((), ())),
                                 precision=lax.Precision.HIGHEST, preferred_element_type=F32)
        grown = jnp.exp(logits - jnp.max(logits, axis=-1, keepdims=True))
        probs = grown / jnp.sum(grown, axis=-1, keepdims=True)
        lanes = lax.broadcasted_iota(jnp.int32, probs.shape, 1)
        picked = [jnp.sum(jnp.where(columns_ref[at, 2 + c:3 + c] == lanes, probs, 0.0), axis=-1, keepdims=True) for c in range(2)]
        both = picked[0] + picked[1]
        gates[at, 0:1] = picked[0] / both
        gates[at, 1:2] = picked[1] / both

    with scope("w_x"):
        for k in (tp, other):
            block_arrived(x_owner, k)
            forward(5, x_owner, k, tp, ep1)
    for peer_tp, peer_ep in peers:
        arrived(slots_all.at[peer_tp * 4 + peer_ep], slot_recv.at[peer_tp * 4 + peer_ep])
    loads[4].wait()
    loads[5].wait()

    def run_group(i, k):
        dest = k * 4 + i
        slots = slots_all[dest]
        want = me * rows + lax.broadcasted_iota(jnp.int32, (rows, tokens // 2), 0)
        chosen = None
        for part in range(2):
            h = hall[part * 4 + i, :, half_at(k), :].reshape(tokens // 2, d_model)
            at = slice(part * (tokens // 2), (part + 1) * (tokens // 2))
            pick = jnp.logical_or(slots[0:1, at] == want, slots[1:2, at] == want)
            term = mm(jnp.where(pick, 1.0, 0.0).astype(BF16), h)
            chosen = term if chosen is None else chosen + term
        b = rms_rows(chosen, ln_ffn_ref[1])
        for e in range(experts):
            at = slice(e * capacity, (e + 1) * capacity)
            hid = jax.nn.gelu(mm(b[at], w_in[e])).astype(BF16)
            res[dest, at] = mm(hid, w_out[e]).astype(BF16)
        return dest

    def give_back(i, k):
        dest = k * 4 + i
        return remote(res.at[dest], ret.at[me], ret_send.at[dest], ret_recv.at[me], k, i)

    def add_rows(source_ref, owner):
        step = 256

        @pl.loop(0, tokens // step)
        def _(r):
            at = pl.ds(pl.multiple_of(r * step, step), step)
            columns = owner * rows + lax.broadcasted_iota(jnp.int32, (step, rows), 1)
            total = acc[at, :]
            for c in range(2):
                pick = jnp.where(columns_ref[at, c:c + 1] == columns, 1.0, 0.0).astype(BF16)
                total = total + gates[at, c:c + 1] * mm(pick, source_ref[...])
            acc[at, :] = total

    with scope("w_yc"):
        for k in range(2):
            block_arrived(c_owner, k)
            block_arrived(yc_owner, k)

    @pl.loop(0, 4)
    def _(t):
        late = t // 2
        beside = lax.rem((t + 1) // 2, 2)
        i = ep + beside * (ep1 - ep)
        k = late * tp + (1 - late) * other
        run_group(i, k)

        @pl.when(t < 3)
        def _():
            give_back(i, k).start()

    add_rows(res.at[me], me)

    for place, k in enumerate((tp, other)):
        with scope(f"w_yx{place}"):
            block_arrived(yx_owner, k)
        forward(6, yx_owner, k, tp, ep1)
        with scope(f"w_far{place}"):
            block_arrived(xc_owner, k)
            block_arrived(yxc_owner, k)

        @pl.loop(0, 2)
        def _(t):
            i = (1 - t) * ep2 + t * ep3
            run_group(i, k)
            give_back(i, k).start()

        if place == 0:
            with scope("w_h1"):
                arrived(h1t_ref, h1_recv)
            cache_part(h1t_ref, 1, other)

    for peer_tp, peer_ep in ((tp, ep1), (other, ep), (other, ep1), (tp, ep2), (tp, ep3), (other, ep2), (other, ep3)):
        owner = peer_tp * 4 + peer_ep
        with scope("w_ret"):
            arrived(ret.at[owner], ret_recv.at[owner])
        add_rows(ret.at[owner], owner)
    out_ref[...] = acc[...].astype(BF16)

    for copy in sends + slot_copies + [send_h1]:
        copy.wait_send()
    for peer_tp, peer_ep in peers:
        give_back(peer_ep, peer_tp).wait_send()


def moe_layer(h2, h1, x0, x0t, expert_ids, ln_ffn, ln_attn, w_router, expert_in, expert_out, w_key, w_value):
    seqs, seq_len, d_model = h2.shape
    tokens = seqs * seq_len
    experts, _, d_ff = expert_in.shape
    groups = 8
    rows = experts * 4 * tokens // (experts * groups)
    inner = w_key.shape[2]
    heads = inner // 64
    any_spec = pl.BlockSpec(memory_space=pl.ANY)
    vmem_spec = pl.BlockSpec(memory_space=pltpu.VMEM)
    cache_shape = jax.ShapeDtypeStruct((2, 2 * seqs, heads, 64, seq_len), BF16)
    dma = pltpu.SemaphoreType.DMA
    return pl.pallas_call(
        moe_body,
        in_specs=[any_spec] * 4 + [vmem_spec] * 4 + [any_spec] * 4,
        out_specs=[vmem_spec, any_spec, any_spec, any_spec],
        out_shape=[jax.ShapeDtypeStruct((tokens, d_model), BF16), cache_shape, cache_shape, jax.ShapeDtypeStruct(h1.shape, BF16)],
        scratch_shapes=[
            pltpu.VMEM((groups,) + h2.shape, BF16),
            pltpu.VMEM((groups, rows, d_model), BF16),
            pltpu.VMEM((groups, rows, d_model), BF16),
            pltpu.VMEM(expert_in.shape, BF16),
            pltpu.VMEM(expert_out.shape, BF16),
            pltpu.VMEM((2, 2, d_model, inner), BF16),
            pltpu.VMEM((tokens, d_model), F32),
            pltpu.VMEM((2, tokens), jnp.int32),
            pltpu.VMEM((groups, 2, tokens), jnp.int32),
            pltpu.VMEM((tokens, 8), jnp.int32),
            pltpu.VMEM((tokens, 2), F32),
            pltpu.VMEM(h1.shape, BF16),
            pltpu.VMEM((seqs, 2, heads, 64, seq_len), BF16),
            dma((6,)), dma, dma((seqs, 2)), dma((7,)), dma((groups,)), dma((7, 2)), dma((groups, 2)),
            dma((groups,)), dma((groups,)), dma, dma,
        ],
        compiler_params=pltpu.CompilerParams(vmem_limit_bytes=67043328, collective_id=2, has_side_effects=True),
        cost_estimate=pl.CostEstimate(flops=40_000_000_000, bytes_accessed=64 << 20, transcendentals=0),
        name="moe",
    )(h2, h1, x0, x0t, jnp.swapaxes(expert_ids, 1, 2), ln_ffn, ln_attn, w_router.T, expert_in, expert_out, w_key, w_value)


def solution(mesh):
    act_spec = P(('dp', 'ep'), 'tp', None)
    col_spec = P(None, None, 'tp')
    row_spec = P(None, 'tp', None)
    expert_spec = P(('tp', 'ep'), None, None)
    cache_spec = P(None, ('dp', 'ep'), 'tp', None, None)
    in_specs = (act_spec, P(), P(), col_spec, col_spec, col_spec, row_spec, row_spec,
                P(None, 'tp'), P(None, 'tp'), P('tp', None), P(), expert_spec, expert_spec, act_spec)

    def device_fn(hidden_in, ln_attn, ln_ffn, w_query, w_key, w_value, w_out, bias_table, w_gate, w_up, w_down, w_router, expert_in, expert_out, expert_ids):
        h1, h2, x0, x0t = dense_layers(hidden_in, ln_attn, ln_ffn, w_query, w_key, w_value, w_out, bias_table, w_gate, w_up, w_down)
        hidden, k_cache, v_cache, _ = moe_layer(
            h2, h1, x0, x0t, expert_ids, ln_ffn, ln_attn, w_router, expert_in, expert_out, w_key, w_value)
        return hidden.reshape(hidden_in.shape), jnp.swapaxes(k_cache, 3, 4), jnp.swapaxes(v_cache, 3, 4)

    return jax.shard_map(device_fn, mesh=mesh, in_specs=in_specs, out_specs=(act_spec, cache_spec, cache_spec), check_vma=False)
```

```python
import contextlib

import jax
import jax.numpy as jnp
from jax import lax
from jax.experimental import pallas as pl
from jax.experimental.pallas import tpu as pltpu
from jax.sharding import PartitionSpec as P

EXACT_BUCKETS = 16
THRESHOLDS = (18, 20, 23, 26, 30, 34, 39, 45, 51, 58, 66, 76, 86, 98, 112)
EPSILON = 1e-6
F32 = jnp.float32
BF16 = jnp.bfloat16
VMEM_LIMIT = 60 * 1024 * 1024
MESH = pl.DeviceIdType.MESH


def scope(name):
    return contextlib.nullcontext()


def rms_rows(rows, ln_scale):
    wide = rows.astype(F32)
    inv_rms = lax.rsqrt(jnp.mean(wide * wide, axis=-1, keepdims=True) + EPSILON)
    return (wide * inv_rms * ln_scale).astype(BF16)


def mm(a, b):
    return lax.dot_general(a, b, (((1,), (0,)), ((), ())), preferred_element_type=F32)


def mm_t(a, b):
    return lax.dot_general(a, b, (((1,), (1,)), ((), ())), preferred_element_type=F32)


def bias_rows(table, seq_len):
    at = lax.broadcasted_iota(jnp.int32, (table.shape[1], 2 * seq_len), 1)
    rel = jnp.where(at == 0, 0, 2 * seq_len - at)
    bucket = jnp.minimum(rel, EXACT_BUCKETS)
    for threshold in THRESHOLDS:
        bucket = bucket + jnp.where(rel >= threshold, 1, 0)
    hot = jnp.where(bucket == lax.broadcasted_iota(jnp.int32, bucket.shape, 0), 1.0, 0.0)
    rows = jnp.dot(table, hot, precision=lax.Precision.HIGHEST, preferred_element_type=F32)
    return jnp.where(rel[:1] < seq_len, rows, -jnp.inf)


def softmax_bf16(scores):
    top = jnp.max(scores, axis=-1, keepdims=True)
    grown = jnp.exp(scores - top)
    return (grown * (1.0 / jnp.sum(grown, axis=-1, keepdims=True))).astype(BF16)


def axis_neighbours(tp, ep):
    core = lax.rem(ep, 2)
    beside = ep + 1 - 2 * core
    return beside, lax.rem(ep + 2, 4), lax.rem(beside + 2, 4)


def remote(src, dst, send, recv, tp, ep):
    return pltpu.make_async_remote_copy(
        src_ref=src, dst_ref=dst, send_sem=send, recv_sem=recv,
        device_id=(lax.axis_index('dp'), tp, ep), device_id_type=MESH)


def layers_body(hid_ref, ln_attn_ref, ln_ffn_ref, wq_hbm, wk_hbm, wv_hbm, wo_hbm, table_ref, wg_hbm, wu_hbm, wd_hbm,
                h1_ref, h2_ref, x0_ref, x0t_ref,
                x, a_ref, acc, w, wo, gu, wd, table_other, u_rows, bias_low, bias_high, qkv, ctx, stage,
                in_sem, own_sem, out_sem, misc_send, misc_recv, y_send, y_recv, x_send, x_recv, c_send, c_recv, d_send, d_recv):
    tp, ep = lax.axis_index('tp'), lax.axis_index('ep')
    other = 1 - tp
    ep1, ep2, ep3 = axis_neighbours(tp, ep)
    seqs, seq_len, d_model = x.shape
    half = seq_len // 2
    tokens = seqs * seq_len
    quad = qkv.shape[2]

    def part(count, quarter):
        return pl.ds(pl.multiple_of(quarter * count, count), count)

    my_pos = part(half, tp)
    mine = hid_ref.at[pl.ds(tp * seqs, seqs)]
    theirs = hid_ref.at[pl.ds(other * seqs, seqs)]

    sources, places = [], []
    for layer in range(2):
        for kind, hbm in enumerate((wq_hbm, wk_hbm, wv_hbm)):
            sources.append(hbm.at[layer, part(256, ep), :])
            places.append(lambda q, layer=layer, kind=kind: w.at[layer, 1, kind, part(256, q), :])
        sources.append(wo_hbm.at[layer, part(128, ep), :])
        places.append(lambda q, layer=layer: wo.at[layer, 1, part(128, q), :])
        if layer == 0:
            for kind, hbm in enumerate((wg_hbm, wu_hbm)):
                sources.append(hbm.at[part(256, ep), :])
                places.append(lambda q, kind=kind: gu.at[1, kind, part(256, q), :])
            sources.append(wd_hbm.at[part(64, ep), :])
            places.append(lambda q: wd.at[1, part(64, q), :])

    own_x = pltpu.make_async_copy(mine, x.at[:, my_pos, :], in_sem.at[0])
    own_stage = pltpu.make_async_copy(theirs, stage, in_sem.at[1])
    own_x.start()
    own_loads = []
    for layer in range(2):
        for kind, hbm in enumerate((wq_hbm, wk_hbm, wv_hbm)):
            own_loads.append((hbm.at[layer], w.at[layer, 0, kind]))
        own_loads.append((wo_hbm.at[layer], wo.at[layer, 0]))
        if layer == 0:
            own_loads += [(wg_hbm, gu.at[0, 0]), (wu_hbm, gu.at[0, 1]), (wd_hbm, wd.at[0])]
    own_loads = [pltpu.make_async_copy(s, d, own_sem.at[n]) for n, (s, d) in enumerate(own_loads)]
    for load in own_loads:
        load.start()
    own_stage.start()

    barrier = pltpu.get_barrier_semaphore()
    for peer_tp, peer_ep in ((other, ep), (tp, ep2), (tp, ep1)):
        pl.semaphore_signal(barrier, inc=1, device_id=(lax.axis_index('dp'), peer_tp, peer_ep), device_id_type=MESH)
    pl.semaphore_wait(barrier, 3)

    def arrived(ref, sem):
        remote(ref, ref, misc_send.at[0], sem, tp, ep).wait_recv()

    pieces = range(len(sources))
    send_entry = remote(theirs, x.at[:, my_pos, :], misc_send.at[0], misc_recv.at[0], other, ep)
    send_u = remote(table_ref, table_other, misc_send.at[1], misc_recv.at[1], other, ep)
    send_rest = remote(mine, x0t_ref.at[:, my_pos, :], misc_send.at[2], misc_recv.at[2], other, ep)
    y_copies = [remote(sources[n], places[n](ep), y_send.at[n], y_recv.at[n], other, ep) for n in pieces]
    x_copies = [remote(places[n](ep), places[n](ep), x_send.at[n], x_recv.at[n], tp, ep2) for n in pieces]
    c_copies = [remote(places[n](ep), places[n](ep), c_send.at[n], c_recv.at[n], tp, ep1) for n in pieces]
    d_copies = [remote(places[n](ep2), places[n](ep2), d_send.at[n], d_recv.at[n], tp, ep1) for n in pieces]
    send_u.start()
    send_entry.start()
    for copy in y_copies:
        copy.start()
    send_rest.start()

    def pass_on(n):
        arrived(places[n](ep), y_recv.at[n])
        x_copies[n].start()
        c_copies[n].start()

    def pass_across(n):
        arrived(places[n](ep2), x_recv.at[n])
        d_copies[n].start()

    def complete(n):
        arrived(places[n](ep1), c_recv.at[n])
        arrived(places[n](ep3), d_recv.at[n])

    def build_bias(rows_ref, side):
        u_rows[...] = bias_rows(rows_ref[...].reshape(u_rows.shape[0], rows_ref.shape[2]), seq_len)

        @pl.loop(0, 8)
        def _(n):
            layer, pair = n // 4, lax.rem(n, 4)
            for sub in range(2):
                row = u_rows[pl.ds(n * 2 + sub, 1), :]
                wide = pltpu.roll(jnp.broadcast_to(row, (seq_len, 2 * seq_len)), 0, 1, stride=1, stride_axis=0)
                at = slice(sub * half, (sub + 1) * half)
                place = layer * 8 + side * 4 + pair
                bias_low[place, at, :] = wide[:half, :half]
                bias_high[place, at, :] = wide[half:, :seq_len]

    def begin_layer(layer):
        @pl.loop(0, seqs)
        def _(s):
            rows = part(seq_len, s)
            a_ref[rows, :] = rms_rows(x[s], ln_attn_ref[layer])
            acc[rows, :] = x[s].astype(F32)

    def end_layer():
        @pl.loop(0, seqs)
        def _(s):
            x[s] = acc[part(seq_len, s), :].astype(BF16)

    first = lax.broadcasted_iota(jnp.int32, (1, 128), 1) < 64

    def attend(layer, side, block):
        cols = slice(block * quad, (block + 1) * quad)
        for kind in range(3):
            qkv[kind] = mm(a_ref[...], w[layer, side, kind, :, cols]).astype(BF16)

        @pl.loop(0, seqs)
        def _(s):
            rows = part(seq_len, s)
            for pair in range(quad // 128):
                lanes = slice(pair * 128, (pair + 1) * 128)
                place = layer * 8 + side * 4 + block * (quad // 128) + pair
                q, k, v = (qkv[kind, rows, lanes] for kind in range(3))
                none = jnp.zeros_like(q[:half])
                outs = []
                for upper in range(2):
                    qs = q[half:] if upper else q[:half]
                    ks, vs = (k, v) if upper else (k[:half], v[:half])
                    both = jnp.concatenate([jnp.where(first, qs, none), jnp.where(first, none, qs)], axis=0)
                    bias = bias_high[place] if upper else bias_low[place]
                    got = mm(softmax_bf16(mm_t(both, ks) * 0.125 + bias), vs)
                    outs.append(jnp.where(first, got[:half], got[half:]))
                ctx[rows, lanes] = jnp.concatenate(outs, axis=0).astype(BF16)

    def project(layer, side, block):
        cols = slice(block * quad, (block + 1) * quad)

        @pl.loop(0, seqs)
        def _(s):
            rows = part(seq_len, s)
            acc[rows, :] += mm(ctx[rows, :], wo[layer, side, cols, :])

    def dense(s):
        h = x[s]
        b = rms_rows(h, ln_ffn_ref[0])
        total = h.astype(F32)
        for side in range(2):
            hid = (jax.nn.gelu(mm(b, gu[side, 0])) * mm(b, gu[side, 1])).astype(BF16)
            total = total + mm(hid, wd[side])
        x[s] = total.astype(BF16)

    def heads(layer, side, block):
        attend(layer, side, block)
        project(layer, side, block)

    build_bias(table_ref, 0)
    arrived(table_other, misc_recv.at[1])
    build_bias(table_other, 1)
    own_stage.wait()
    own_x0t = pltpu.make_async_copy(stage, x0t_ref.at[:, my_pos, :], out_sem.at[0])
    own_x0t.start()

    with scope("w_entry"):
        own_x.wait()
        arrived(x.at[:, part(half, other), :], misc_recv.at[0])
    out_x0 = pltpu.make_async_copy(x, x0_ref, out_sem.at[1])
    out_x0.start()
    begin_layer(0)
    for n in range(4):
        own_loads[n].wait()
    heads(0, 0, 0)
    heads(0, 0, 1)
    with scope("w_l0_y"):
        for n in range(4):
            pass_on(n)
    with scope("w_l0_x"):
        for n in range(3):
            pass_across(n)
    with scope("w_l0_all"):
        for n in range(3):
            complete(n)
    attend(0, 1, 0)
    with scope("w_l0_o"):
        pass_across(3)
        pass_on(4)
        complete(3)
        pass_on(5)
    project(0, 1, 0)
    with scope("w_ffn_y"):
        pass_on(6)
    heads(0, 1, 1)
    with scope("w_ffn_x"):
        pass_on(7)
        for n in range(4, 7):
            pass_across(n)
    out_x0.wait()
    end_layer()
    with scope("w_ffn_all"):
        for n in range(4, 7):
            own_loads[n].wait()
            complete(n)

    @pl.loop(0, seqs // 2)
    def _(s):
        dense(s)

    with scope("w_l1_k"):
        pass_on(8)

    @pl.loop(seqs // 2, seqs)
    def _(s):
        dense(s)

    out_h1 = pltpu.make_async_copy(x, h1_ref, out_sem.at[2])
    out_h1.start()
    begin_layer(1)
    for n in range(7, 11):
        own_loads[n].wait()
    attend(1, 0, 0)
    with scope("w_l1_v"):
        pass_on(9)
    project(1, 0, 0)
    heads(1, 0, 1)
    with scope("w_l1_o"):
        pass_on(10)
    with scope("w_l1_x"):
        for n in range(7, 10):
            pass_across(n)
    with scope("w_l1_all"):
        for n in range(7, 10):
            complete(n)
    attend(1, 1, 0)
    with scope("w_l1_o_all"):
        pass_across(10)
        complete(10)
    project(1, 1, 0)
    heads(1, 1, 1)
    out_h1.wait()
    end_layer()
    out_h2 = pltpu.make_async_copy(x, h2_ref, out_sem.at[3])
    out_h2.start()

    with scope("w_rest"):
        arrived(x0t_ref.at[:, part(half, other), :], misc_recv.at[2])
    own_x0t.wait()
    for copy in [send_entry, send_u, send_rest] + y_copies + x_copies + c_copies + d_copies:
        copy.wait_send()
    out_h2.wait()


def dense_layers(hidden_in, ln_attn, ln_ffn, w_query, w_key, w_value, w_out, bias_table, w_gate, w_up, w_down):
    batch, positions, d_model = hidden_in.shape
    seqs, seq_len = batch // 2, 2 * positions
    inner = w_query.shape[2]
    any_spec = pl.BlockSpec(memory_space=pl.ANY)
    vmem_spec = pl.BlockSpec(memory_space=pltpu.VMEM)
    dma = pltpu.SemaphoreType.DMA
    shape = jax.ShapeDtypeStruct((seqs, seq_len, d_model), BF16)
    return pl.pallas_call(
        layers_body,
        in_specs=[any_spec, vmem_spec, vmem_spec] + [any_spec] * 4 + [vmem_spec] + [any_spec] * 3,
        out_specs=[any_spec] * 4,
        out_shape=[shape] * 4,
        scratch_shapes=[
            pltpu.VMEM(shape.shape, BF16),
            pltpu.VMEM((seqs * seq_len, d_model), BF16),
            pltpu.VMEM((seqs * seq_len, d_model), F32),
            pltpu.VMEM((2, 2, 3, d_model, inner), BF16),
            pltpu.VMEM((2, 2, inner, d_model), BF16),
            pltpu.VMEM((2, 2) + w_gate.shape, BF16),
            pltpu.VMEM((2,) + w_down.shape, BF16),
            pltpu.VMEM(bias_table.shape, F32),
            pltpu.VMEM((bias_table.shape[0] * bias_table.shape[1], 2 * seq_len), F32),
            pltpu.VMEM((16, seq_len, seq_len // 2), F32),
            pltpu.VMEM((16, seq_len, seq_len), F32),
            pltpu.VMEM((3, seqs * seq_len, 256), BF16),
            pltpu.VMEM((seqs * seq_len, 256), BF16),
            pltpu.VMEM((seqs, positions, d_model), BF16),
            dma((2,)), dma((11,)), dma((4,)), dma((3,)), dma((3,)),
        ] + [dma((11,))] * 8,
        compiler_params=pltpu.CompilerParams(vmem_limit_bytes=VMEM_LIMIT, collective_id=1, has_side_effects=True),
        cost_estimate=pl.CostEstimate(flops=32_000_000_000, bytes_accessed=40 << 20, transcendentals=0),
        name="dense_layers",
    )(hidden_in, ln_attn, ln_ffn, w_query, w_key, w_value, w_out, bias_table, w_gate, w_up, w_down)


def moe_body(h2_ref, h1_ref, x0_ref, x0t_ref, ids_ref, ln_ffn_ref, ln_attn_ref, router_ref,
             w_in_hbm, w_out_hbm, wk_hbm, wv_hbm,
             out_ref, k_ref, v_ref, h1t_ref,
             hall, res, ret, w_in, w_out, wkv, acc, slot_row_ref, slots_all, columns_ref, gates, xbuf, kvbuf,
             in_sem, cache_sem, store_sem, slot_send, slot_recv, hs_send, hs_recv, ret_send, ret_recv, h1_send, h1_recv):
    tp, ep = lax.axis_index('tp'), lax.axis_index('ep')
    other = 1 - tp
    ep1, ep2, ep3 = axis_neighbours(tp, ep)
    me = tp * 4 + ep
    seqs, seq_len, d_model = h2_ref.shape
    tokens = acc.shape[0]
    rows = res.shape[1]
    half_pos = seq_len // 2
    experts = w_in.shape[0]
    capacity = rows // experts

    loads = [pltpu.make_async_copy(a, b, in_sem.at[n]) for n, (a, b) in enumerate((
        (x0_ref, xbuf), (wk_hbm, wkv.at[0]), (wv_hbm, wkv.at[1]), (h2_ref, hall.at[me]),
        (w_in_hbm, w_in), (w_out_hbm, w_out)))]
    for load in loads:
        load.start()

    barrier = pltpu.get_barrier_semaphore()
    peers = [(other, ep), (tp, ep2), (tp, ep1), (other, ep1), (other, ep2), (tp, ep3), (other, ep3)]
    for peer_tp, peer_ep in peers:
        pl.semaphore_signal(barrier, inc=1, device_id=(lax.axis_index('dp'), peer_tp, peer_ep), device_id_type=MESH)
    pl.semaphore_wait(barrier, len(peers))

    def half_at(k):
        return pl.ds(pl.multiple_of(k * half_pos, half_pos), half_pos)

    def block(owner, k):
        return hall.at[owner, :, half_at(k), :]

    sends = []
    for n, peer in enumerate(((other, ep), (tp, ep2), (tp, ep1))):
        for k in ((other, tp) if n == 0 else (tp, other)):
            sends.append(remote(h2_ref.at[:, half_at(k), :], block(me, k), hs_send.at[n, k], hs_recv.at[me, k], *peer))
    for copy in sends:
        copy.start()

    def arrived(ref, sem):
        remote(ref, ref, hs_send.at[0], sem, tp, ep).wait_recv()

    def block_arrived(owner, k):
        arrived(block(owner, k), hs_recv.at[owner, k])

    def forward(n, owner, k, *peer):
        copy = remote(block(owner, k), block(owner, k), hs_send.at[n, k], hs_recv.at[owner, k], *peer)
        copy.start()
        sends.append(copy)

    num_experts = router_ref.shape[0]
    ids_row = jnp.concatenate([ids_ref[s] for s in range(ids_ref.shape[0])], axis=1)
    expert = lax.broadcasted_iota(jnp.int32, (num_experts, tokens), 0)
    hot = [jnp.where(ids_row[c:c + 1] == expert, 1.0, 0.0) for c in range(2)]
    earlier = lax.broadcasted_iota(jnp.int32, (tokens, tokens), 0) <= lax.broadcasted_iota(jnp.int32, (tokens, tokens), 1)
    upto = mm(jnp.concatenate(hot, axis=0).astype(BF16), jnp.where(earlier, 1.0, 0.0).astype(BF16))
    base = (0.0, upto[:num_experts, tokens - 1:])
    wide_ids = ids_row.astype(F32)
    slot_rows = []
    for c in range(2):
        place = jnp.sum((upto[c * num_experts:(c + 1) * num_experts] - 1.0 + base[c]) * hot[c], axis=0, keepdims=True)
        slot_rows.append(jnp.where(place < capacity, wide_ids[c:c + 1] * capacity + place, -1.0))
    packed = jnp.concatenate(slot_rows + [wide_ids, jnp.zeros((4, tokens), F32)], axis=0)
    slot_row_ref[...] = packed[:2].astype(jnp.int32)
    slots_all[me] = packed[:2].astype(jnp.int32)
    columns_ref[...] = packed.T.astype(jnp.int32)
    slot_copies = [remote(slot_row_ref, slots_all.at[me], slot_send.at[n], slot_recv.at[me], *peer) for n, peer in enumerate(peers)]
    for copy in slot_copies:
        copy.start()
    send_h1 = remote(h1_ref, h1t_ref, h1_send, h1_recv, other, ep)
    send_h1.start()

    def cache_part(source, layer, owner, load=None):
        if load is None:
            load = pltpu.make_async_copy(source, xbuf, cache_sem)
            load.start()
        load.wait()

        @pl.loop(0, seqs)
        def _(s):
            a = rms_rows(xbuf[s], ln_attn_ref[layer])
            for n, ref in enumerate((k_ref, v_ref)):
                full = mm(a, wkv[n, layer])
                kvbuf[s, n] = full.T.astype(BF16).reshape(kvbuf.shape[2:])
                pltpu.make_async_copy(kvbuf.at[s, n], ref.at[layer, owner * seqs + s], store_sem.at[s, n]).start()

        @pl.loop(0, seqs)
        def _(s):
            for n, ref in enumerate((k_ref, v_ref)):
                pltpu.make_async_copy(kvbuf.at[s, n], ref.at[layer, owner * seqs + s], store_sem.at[s, n]).wait()

    loads[1].wait()
    loads[2].wait()
    cache_part(x0_ref, 0, tp, loads[0])
    cache_part(x0t_ref, 0, other)
    cache_part(h1_ref, 1, tp)

    y_owner, x_owner, c_owner = other * 4 + ep, tp * 4 + ep2, tp * 4 + ep1
    yx_owner, yc_owner, xc_owner, yxc_owner = other * 4 + ep2, other * 4 + ep1, tp * 4 + ep3, other * 4 + ep3
    for place, k in enumerate((tp, other)):
        with scope(f"w_y{place}"):
            block_arrived(y_owner, k)
        forward(3, y_owner, k, tp, ep2)
        forward(4, y_owner, k, tp, ep1)
    loads[3].wait()

    def own_tokens(owner):
        return hall[owner, :, half_at(tp), :].reshape(tokens // 2, d_model)

    for part in range(2):
        at = slice(part * (tokens // 2), (part + 1) * (tokens // 2))
        h_own = own_tokens(part * 4 + ep)
        acc[at] = h_own.astype(F32)
        b = rms_rows(h_own, ln_ffn_ref[1])
        logits = lax.dot_general(b.astype(F32), router_ref[...], (((1,), (1,)), ((), ())),
                                 precision=lax.Precision.HIGHEST, preferred_element_type=F32)
        grown = jnp.exp(logits - jnp.max(logits, axis=-1, keepdims=True))
        probs = grown / jnp.sum(grown, axis=-1, keepdims=True)
        lanes = lax.broadcasted_iota(jnp.int32, probs.shape, 1)
        picked = [jnp.sum(jnp.where(columns_ref[at, 2 + c:3 + c] == lanes, probs, 0.0), axis=-1, keepdims=True) for c in range(2)]
        both = picked[0] + picked[1]
        gates[at, 0:1] = picked[0] / both
        gates[at, 1:2] = picked[1] / both

    with scope("w_x"):
        for k in (tp, other):
            block_arrived(x_owner, k)
            forward(5, x_owner, k, tp, ep1)
    for peer_tp, peer_ep in peers:
        arrived(slots_all.at[peer_tp * 4 + peer_ep], slot_recv.at[peer_tp * 4 + peer_ep])
    loads[4].wait()
    loads[5].wait()

    def run_group(i, k):
        dest = k * 4 + i
        slots = slots_all[dest]
        want = me * rows + lax.broadcasted_iota(jnp.int32, (rows, tokens // 2), 0)
        chosen = None
        for part in range(2):
            h = hall[part * 4 + i, :, half_at(k), :].reshape(tokens // 2, d_model)
            at = slice(part * (tokens // 2), (part + 1) * (tokens // 2))
            pick = jnp.logical_or(slots[0:1, at] == want, slots[1:2, at] == want)
            term = mm(jnp.where(pick, 1.0, 0.0).astype(BF16), h)
            chosen = term if chosen is None else chosen + term
        b = rms_rows(chosen, ln_ffn_ref[1])
        for e in range(experts):
            at = slice(e * capacity, (e + 1) * capacity)
            hid = jax.nn.gelu(mm(b[at], w_in[e])).astype(BF16)
            res[dest, at] = mm(hid, w_out[e]).astype(BF16)
        return dest

    def give_back(i, k):
        dest = k * 4 + i
        return remote(res.at[dest], ret.at[me], ret_send.at[dest], ret_recv.at[me], k, i)

    def add_rows(source_ref, owner):
        step = 256

        @pl.loop(0, tokens // step)
        def _(r):
            at = pl.ds(pl.multiple_of(r * step, step), step)
            columns = owner * rows + lax.broadcasted_iota(jnp.int32, (step, rows), 1)
            total = acc[at, :]
            for c in range(2):
                pick = jnp.where(columns_ref[at, c:c + 1] == columns, 1.0, 0.0).astype(BF16)
                total = total + gates[at, c:c + 1] * mm(pick, source_ref[...])
            acc[at, :] = total

    with scope("w_yc"):
        for k in range(2):
            block_arrived(c_owner, k)
            block_arrived(yc_owner, k)

    @pl.loop(0, 4)
    def _(t):
        late = t // 2
        beside = lax.rem((t + 1) // 2, 2)
        i = ep + beside * (ep1 - ep)
        k = late * tp + (1 - late) * other
        run_group(i, k)

        @pl.when(t < 3)
        def _():
            give_back(i, k).start()

    add_rows(res.at[me], me)

    for place, k in enumerate((tp, other)):
        with scope(f"w_yx{place}"):
            block_arrived(yx_owner, k)
        forward(6, yx_owner, k, tp, ep1)
        with scope(f"w_far{place}"):
            block_arrived(xc_owner, k)
            block_arrived(yxc_owner, k)

        @pl.loop(0, 2)
        def _(t):
            i = (1 - t) * ep2 + t * ep3
            run_group(i, k)
            give_back(i, k).start()

        if place == 0:
            with scope("w_h1"):
                arrived(h1t_ref, h1_recv)
            cache_part(h1t_ref, 1, other)

    for peer_tp, peer_ep in ((tp, ep1), (other, ep), (other, ep1), (tp, ep2), (tp, ep3), (other, ep2), (other, ep3)):
        owner = peer_tp * 4 + peer_ep
        with scope("w_ret"):
            arrived(ret.at[owner], ret_recv.at[owner])
        add_rows(ret.at[owner], owner)
    out_ref[...] = acc[...].astype(BF16)

    for copy in sends + slot_copies + [send_h1]:
        copy.wait_send()
    for peer_tp, peer_ep in peers:
        give_back(peer_ep, peer_tp).wait_send()


def moe_layer(h2, h1, x0, x0t, expert_ids, ln_ffn, ln_attn, w_router, expert_in, expert_out, w_key, w_value):
    seqs, seq_len, d_model = h2.shape
    tokens = seqs * seq_len
    experts, _, d_ff = expert_in.shape
    groups = 8
    rows = experts * 4 * tokens // (experts * groups)
    inner = w_key.shape[2]
    heads = inner // 64
    any_spec = pl.BlockSpec(memory_space=pl.ANY)
    vmem_spec = pl.BlockSpec(memory_space=pltpu.VMEM)
    cache_shape = jax.ShapeDtypeStruct((2, 2 * seqs, heads, 64, seq_len), BF16)
    dma = pltpu.SemaphoreType.DMA
    return pl.pallas_call(
        moe_body,
        in_specs=[any_spec] * 4 + [vmem_spec] * 4 + [any_spec] * 4,
        out_specs=[vmem_spec, any_spec, any_spec, any_spec],
        out_shape=[jax.ShapeDtypeStruct((tokens, d_model), BF16), cache_shape, cache_shape, jax.ShapeDtypeStruct(h1.shape, BF16)],
        scratch_shapes=[
            pltpu.VMEM((groups,) + h2.shape, BF16),
            pltpu.VMEM((groups, rows, d_model), BF16),
            pltpu.VMEM((groups, rows, d_model), BF16),
            pltpu.VMEM(expert_in.shape, BF16),
            pltpu.VMEM(expert_out.shape, BF16),
            pltpu.VMEM((2, 2, d_model, inner), BF16),
            pltpu.VMEM((tokens, d_model), F32),
            pltpu.VMEM((2, tokens), jnp.int32),
            pltpu.VMEM((groups, 2, tokens), jnp.int32),
            pltpu.VMEM((tokens, 8), jnp.int32),
            pltpu.VMEM((tokens, 2), F32),
            pltpu.VMEM(h1.shape, BF16),
            pltpu.VMEM((seqs, 2, heads, 64, seq_len), BF16),
            dma((6,)), dma, dma((seqs, 2)), dma((7,)), dma((groups,)), dma((7, 2)), dma((groups, 2)),
            dma((groups,)), dma((groups,)), dma, dma,
        ],
        compiler_params=pltpu.CompilerParams(vmem_limit_bytes=67043328, collective_id=2, has_side_effects=True),
        cost_estimate=pl.CostEstimate(flops=40_000_000_000, bytes_accessed=64 << 20, transcendentals=0),
        name="moe",
    )(h2, h1, x0, x0t, jnp.swapaxes(expert_ids, 1, 2), ln_ffn, ln_attn, w_router.T, expert_in, expert_out, w_key, w_value)


def solution(mesh):
    act_spec = P(('dp', 'ep'), 'tp', None)
    col_spec = P(None, None, 'tp')
    row_spec = P(None, 'tp', None)
    expert_spec = P(('tp', 'ep'), None, None)
    cache_spec = P(None, ('dp', 'ep'), 'tp', None, None)
    in_specs = (act_spec, P(), P(), col_spec, col_spec, col_spec, row_spec, row_spec,
                P(None, 'tp'), P(None, 'tp'), P('tp', None), P(), expert_spec, expert_spec, act_spec)

    def device_fn(hidden_in, ln_attn, ln_ffn, w_query, w_key, w_value, w_out, bias_table, w_gate, w_up, w_down, w_router, expert_in, expert_out, expert_ids):
        h1, h2, x0, x0t = dense_layers(hidden_in, ln_attn, ln_ffn, w_query, w_key, w_value, w_out, bias_table, w_gate, w_up, w_down)
        hidden, k_cache, v_cache, _ = moe_layer(
            h2, h1, x0, x0t, expert_ids, ln_ffn, ln_attn, w_router, expert_in, expert_out, w_key, w_value)
        return hidden.reshape(hidden_in.shape), jnp.swapaxes(k_cache, 3, 4), jnp.swapaxes(v_cache, 3, 4)

    return jax.shard_map(device_fn, mesh=mesh, in_specs=in_specs, out_specs=(act_spec, cache_spec, cache_spec), check_vma=False)
```

```python
import contextlib

import jax
import jax.numpy as jnp
from jax import lax
from jax.experimental import pallas as pl
from jax.experimental.pallas import tpu as pltpu
from jax.sharding import PartitionSpec as P

EXACT_BUCKETS = 16
THRESHOLDS = (18, 20, 23, 26, 30, 34, 39, 45, 51, 58, 66, 76, 86, 98, 112)
EPSILON = 1e-6
F32 = jnp.float32
BF16 = jnp.bfloat16
VMEM_LIMIT = 60 * 1024 * 1024
MESH = pl.DeviceIdType.MESH


def scope(name):
    return contextlib.nullcontext()


def rms_rows(rows, ln_scale):
    wide = rows.astype(F32)
    inv_rms = lax.rsqrt(jnp.mean(wide * wide, axis=-1, keepdims=True) + EPSILON)
    return (wide * inv_rms * ln_scale).astype(BF16)


def mm(a, b):
    return lax.dot_general(a, b, (((1,), (0,)), ((), ())), preferred_element_type=F32)


def mm_t(a, b):
    return lax.dot_general(a, b, (((1,), (1,)), ((), ())), preferred_element_type=F32)


def bias_rows(table, seq_len):
    at = lax.broadcasted_iota(jnp.int32, (table.shape[1], 2 * seq_len), 1)
    rel = jnp.where(at == 0, 0, 2 * seq_len - at)
    bucket = jnp.minimum(rel, EXACT_BUCKETS)
    for threshold in THRESHOLDS:
        bucket = bucket + jnp.where(rel >= threshold, 1, 0)
    hot = jnp.where(bucket == lax.broadcasted_iota(jnp.int32, bucket.shape, 0), 1.0, 0.0)
    rows = jnp.dot(table, hot, precision=lax.Precision.HIGHEST, preferred_element_type=F32)
    return jnp.where(rel[:1] < seq_len, rows, -jnp.inf)


def softmax_bf16(scores):
    top = jnp.max(scores, axis=-1, keepdims=True)
    grown = jnp.exp(scores - top)
    return (grown * (1.0 / jnp.sum(grown, axis=-1, keepdims=True))).astype(BF16)


def axis_neighbours(tp, ep):
    core = lax.rem(ep, 2)
    beside = ep + 1 - 2 * core
    return beside, lax.rem(ep + 2, 4), lax.rem(beside + 2, 4)


def remote(src, dst, send, recv, tp, ep):
    return pltpu.make_async_remote_copy(
        src_ref=src, dst_ref=dst, send_sem=send, recv_sem=recv,
        device_id=(lax.axis_index('dp'), tp, ep), device_id_type=MESH)


def layers_body(hid_ref, ln_attn_ref, ln_ffn_ref, wq_hbm, wk_hbm, wv_hbm, wo_hbm, table_ref, wg_hbm, wu_hbm, wd_hbm,
                h1_ref, h2_ref, x0_ref, x0t_ref,
                x, a_ref, acc, w, wo, gu, wd, table_other, u_rows, bias_low, bias_high, qkv, ctx, stage,
                in_sem, own_sem, out_sem, x0_sem, entry_send, entry_recv, misc_send, misc_recv, y_send, y_recv, x_send, x_recv, c_send, c_recv, d_send, d_recv):
    tp, ep = lax.axis_index('tp'), lax.axis_index('ep')
    other = 1 - tp
    ep1, ep2, ep3 = axis_neighbours(tp, ep)
    seqs, seq_len, d_model = x.shape
    half = seq_len // 2
    tokens = seqs * seq_len
    quad = qkv.shape[2]

    def part(count, quarter):
        return pl.ds(pl.multiple_of(quarter * count, count), count)

    my_pos = part(half, tp)
    mine = hid_ref.at[pl.ds(tp * seqs, seqs)]
    theirs = hid_ref.at[pl.ds(other * seqs, seqs)]

    sources, places = [], []
    for layer in range(2):
        for kind, hbm in enumerate((wq_hbm, wk_hbm, wv_hbm)):
            sources.append(hbm.at[layer, part(256, ep), :])
            places.append(lambda q, layer=layer, kind=kind: w.at[layer, 1, kind, part(256, q), :])
        sources.append(wo_hbm.at[layer, part(128, ep), :])
        places.append(lambda q, layer=layer: wo.at[layer, 1, part(128, q), :])
        if layer == 0:
            for kind, hbm in enumerate((wg_hbm, wu_hbm)):
                sources.append(hbm.at[part(256, ep), :])
                places.append(lambda q, kind=kind: gu.at[1, kind, part(256, q), :])
            sources.append(wd_hbm.at[part(64, ep), :])
            places.append(lambda q: wd.at[1, part(64, q), :])

    own_x = pltpu.make_async_copy(mine, x.at[:, my_pos, :], in_sem.at[0])
    own_stage = pltpu.make_async_copy(theirs, stage, in_sem.at[1])
    own_x.start()
    own_loads = []
    for layer in range(2):
        for kind, hbm in enumerate((wq_hbm, wk_hbm, wv_hbm)):
            own_loads.append((hbm.at[layer], w.at[layer, 0, kind]))
        own_loads.append((wo_hbm.at[layer], wo.at[layer, 0]))
        if layer == 0:
            own_loads += [(wg_hbm, gu.at[0, 0]), (wu_hbm, gu.at[0, 1]), (wd_hbm, wd.at[0])]
    own_loads = [pltpu.make_async_copy(s, d, own_sem.at[n]) for n, (s, d) in enumerate(own_loads)]
    for load in own_loads:
        load.start()
    own_stage.start()

    barrier = pltpu.get_barrier_semaphore()
    for peer_tp, peer_ep in ((other, ep), (tp, ep2), (tp, ep1)):
        pl.semaphore_signal(barrier, inc=1, device_id=(lax.axis_index('dp'), peer_tp, peer_ep), device_id_type=MESH)
    pl.semaphore_wait(barrier, 3)

    def arrived(ref, sem):
        remote(ref, ref, misc_send.at[0], sem, tp, ep).wait_recv()

    pieces = range(len(sources))
    entry_copies = [remote(hid_ref.at[other * seqs + s], x.at[s, my_pos, :], entry_send.at[s], entry_recv.at[s], other, ep) for s in range(seqs)]
    send_u = remote(table_ref, table_other, misc_send.at[1], misc_recv.at[1], other, ep)
    send_rest = remote(mine, x0t_ref.at[:, my_pos, :], misc_send.at[2], misc_recv.at[2], other, ep)
    y_copies = [remote(sources[n], places[n](ep), y_send.at[n], y_recv.at[n], other, ep) for n in pieces]
    x_copies = [remote(places[n](ep), places[n](ep), x_send.at[n], x_recv.at[n], tp, ep2) for n in pieces]
    c_copies = [remote(places[n](ep), places[n](ep), c_send.at[n], c_recv.at[n], tp, ep1) for n in pieces]
    d_copies = [remote(places[n](ep2), places[n](ep2), d_send.at[n], d_recv.at[n], tp, ep1) for n in pieces]
    send_u.start()
    for copy in y_copies[:4] + entry_copies + y_copies[4:] + [send_rest]:
        copy.start()

    def pass_on(n):
        arrived(places[n](ep), y_recv.at[n])
        x_copies[n].start()
        c_copies[n].start()

    def pass_across(n):
        arrived(places[n](ep2), x_recv.at[n])
        d_copies[n].start()

    def complete(n):
        arrived(places[n](ep1), c_recv.at[n])
        arrived(places[n](ep3), d_recv.at[n])

    def build_bias(rows_ref, side):
        u_rows[...] = bias_rows(rows_ref[...].reshape(u_rows.shape[0], rows_ref.shape[2]), seq_len)

        @pl.loop(0, 8)
        def _(n):
            layer, pair = n // 4, lax.rem(n, 4)
            for sub in range(2):
                row = u_rows[pl.ds(n * 2 + sub, 1), :]
                wide = pltpu.roll(jnp.broadcast_to(row, (seq_len, 2 * seq_len)), 0, 1, stride=1, stride_axis=0)
                at = slice(sub * half, (sub + 1) * half)
                place = layer * 8 + side * 4 + pair
                bias_low[place, at, :] = wide[:half, :half]
                bias_high[place, at, :] = wide[half:, :seq_len]

    def begin_seq(layer, s):
        rows = part(seq_len, s)
        a_ref[rows, :] = rms_rows(x[s], ln_attn_ref[layer])
        acc[rows, :] = x[s].astype(F32)

    def end_seq(s):
        x[s] = acc[part(seq_len, s), :].astype(BF16)

    def each_seq(step, *args):
        @pl.loop(0, seqs)
        def _(s):
            step(*args, s)

    first = lax.broadcasted_iota(jnp.int32, (1, 128), 1) < 64

    def products(layer, side, block, rows):
        for kind in range(3):
            qkv[kind, rows, :] = mm(a_ref[rows, :], w[layer, side, kind, :, block * quad:(block + 1) * quad]).astype(BF16)

    def attend_seq(layer, side, block, s):
        rows = part(seq_len, s)
        for pair in range(quad // 128):
            lanes = slice(pair * 128, (pair + 1) * 128)
            place = layer * 8 + side * 4 + block * (quad // 128) + pair
            q, k, v = (qkv[kind, rows, lanes] for kind in range(3))
            none = jnp.zeros_like(q[:half])
            outs = []
            for upper in range(2):
                qs = q[half:] if upper else q[:half]
                ks, vs = (k, v) if upper else (k[:half], v[:half])
                both = jnp.concatenate([jnp.where(first, qs, none), jnp.where(first, none, qs)], axis=0)
                bias = bias_high[place] if upper else bias_low[place]
                got = mm(softmax_bf16(mm_t(both, ks) * 0.125 + bias), vs)
                outs.append(jnp.where(first, got[:half], got[half:]))
            ctx[rows, lanes] = jnp.concatenate(outs, axis=0).astype(BF16)

    def project_seq(layer, side, block, s):
        rows = part(seq_len, s)
        acc[rows, :] += mm(ctx[rows, :], wo[layer, side, block * quad:(block + 1) * quad, :])

    def attend(layer, side, block):
        products(layer, side, block, slice(None))
        each_seq(attend_seq, layer, side, block)

    def project(layer, side, block):
        each_seq(project_seq, layer, side, block)

    def dense(s):
        h = x[s]
        b = rms_rows(h, ln_ffn_ref[0])
        total = h.astype(F32)
        for side in range(2):
            hid = (jax.nn.gelu(mm(b, gu[side, 0])) * mm(b, gu[side, 1])).astype(BF16)
            total = total + mm(hid, wd[side])
        x[s] = total.astype(BF16)

    def heads(layer, side, block):
        attend(layer, side, block)
        project(layer, side, block)

    build_bias(table_ref, 0)
    arrived(table_other, misc_recv.at[1])
    build_bias(table_other, 1)
    own_stage.wait()
    own_x0t = pltpu.make_async_copy(stage, x0t_ref.at[:, my_pos, :], out_sem.at[0])
    own_x0t.start()

    with scope("w_l0_y"):
        for n in range(4):
            pass_on(n)
    with scope("w_l0_x"):
        for n in range(4):
            pass_across(n)
    own_x.wait()
    for n in range(4):
        own_loads[n].wait()
        complete(n)

    def x0_copy(s):
        return pltpu.make_async_copy(x.at[s], x0_ref.at[s], x0_sem.at[s])

    @pl.loop(0, seqs)
    def _(s):
        with scope("w_entry"):
            arrived(x.at[s, part(half, other), :], entry_recv.at[s])
        x0_copy(s).start()
        begin_seq(0, s)
        for side in range(2):
            for block in range(2):
                products(0, side, block, part(seq_len, s))
                attend_seq(0, side, block, s)
                project_seq(0, side, block, s)
        x0_copy(s).wait()
        end_seq(s)

        @pl.when(s == seqs - 2)
        def _():
            pass_on(4)

    with scope("w_ffn_y"):
        for n in range(5, 7):
            pass_on(n)
        pass_on(7)
    with scope("w_ffn_x"):
        for n in range(4, 7):
            pass_across(n)
    with scope("w_ffn_all"):
        for n in range(4, 7):
            own_loads[n].wait()
            complete(n)

    @pl.loop(0, seqs // 2)
    def _(s):
        dense(s)

    with scope("w_l1_k"):
        pass_on(8)

    @pl.loop(seqs // 2, seqs)
    def _(s):
        dense(s)

    out_h1 = pltpu.make_async_copy(x, h1_ref, out_sem.at[2])
    out_h1.start()
    each_seq(begin_seq, 1)
    for n in range(7, 11):
        own_loads[n].wait()
    attend(1, 0, 0)
    with scope("w_l1_v"):
        pass_on(9)
    project(1, 0, 0)
    heads(1, 0, 1)
    with scope("w_l1_o"):
        pass_on(10)
    with scope("w_l1_x"):
        for n in range(7, 10):
            pass_across(n)
    with scope("w_l1_all"):
        for n in range(7, 10):
            complete(n)
    attend(1, 1, 0)
    with scope("w_l1_o_all"):
        pass_across(10)
        complete(10)
    project(1, 1, 0)
    heads(1, 1, 1)
    out_h1.wait()
    each_seq(end_seq)
    out_h2 = pltpu.make_async_copy(x, h2_ref, out_sem.at[3])
    out_h2.start()

    with scope("w_rest"):
        arrived(x0t_ref.at[:, part(half, other), :], misc_recv.at[2])
    own_x0t.wait()
    for copy in entry_copies + [send_u, send_rest] + y_copies + x_copies + c_copies + d_copies:
        copy.wait_send()
    out_h2.wait()


def dense_layers(hidden_in, ln_attn, ln_ffn, w_query, w_key, w_value, w_out, bias_table, w_gate, w_up, w_down):
    batch, positions, d_model = hidden_in.shape
    seqs, seq_len = batch // 2, 2 * positions
    inner = w_query.shape[2]
    any_spec = pl.BlockSpec(memory_space=pl.ANY)
    vmem_spec = pl.BlockSpec(memory_space=pltpu.VMEM)
    dma = pltpu.SemaphoreType.DMA
    shape = jax.ShapeDtypeStruct((seqs, seq_len, d_model), BF16)
    return pl.pallas_call(
        layers_body,
        in_specs=[any_spec, vmem_spec, vmem_spec] + [any_spec] * 4 + [vmem_spec] + [any_spec] * 3,
        out_specs=[any_spec] * 4,
        out_shape=[shape] * 4,
        scratch_shapes=[
            pltpu.VMEM(shape.shape, BF16),
            pltpu.VMEM((seqs * seq_len, d_model), BF16),
            pltpu.VMEM((seqs * seq_len, d_model), F32),
            pltpu.VMEM((2, 2, 3, d_model, inner), BF16),
            pltpu.VMEM((2, 2, inner, d_model), BF16),
            pltpu.VMEM((2, 2) + w_gate.shape, BF16),
            pltpu.VMEM((2,) + w_down.shape, BF16),
            pltpu.VMEM(bias_table.shape, F32),
            pltpu.VMEM((bias_table.shape[0] * bias_table.shape[1], 2 * seq_len), F32),
            pltpu.VMEM((16, seq_len, seq_len // 2), F32),
            pltpu.VMEM((16, seq_len, seq_len), F32),
            pltpu.VMEM((3, seqs * seq_len, 256), BF16),
            pltpu.VMEM((seqs * seq_len, 256), BF16),
            pltpu.VMEM((seqs, positions, d_model), BF16),
            dma((2,)), dma((11,)), dma((4,)), dma((seqs,)), dma((seqs,)), dma((seqs,)), dma((3,)), dma((3,)),
        ] + [dma((11,))] * 8,
        compiler_params=pltpu.CompilerParams(vmem_limit_bytes=VMEM_LIMIT, collective_id=1, has_side_effects=True),
        cost_estimate=pl.CostEstimate(flops=32_000_000_000, bytes_accessed=40 << 20, transcendentals=0),
        name="dense_layers",
    )(hidden_in, ln_attn, ln_ffn, w_query, w_key, w_value, w_out, bias_table, w_gate, w_up, w_down)


def moe_body(h2_ref, h1_ref, x0_ref, x0t_ref, ids_ref, ln_ffn_ref, ln_attn_ref, router_ref,
             w_in_hbm, w_out_hbm, wk_hbm, wv_hbm,
             out_ref, k_ref, v_ref, h1t_ref,
             hall, res, ret, w_in, w_out, wkv, acc, slot_row_ref, slots_all, columns_ref, gates, xbuf, kvbuf,
             in_sem, cache_sem, store_sem, slot_send, slot_recv, hs_send, hs_recv, ret_send, ret_recv, h1_send, h1_recv):
    tp, ep = lax.axis_index('tp'), lax.axis_index('ep')
    other = 1 - tp
    ep1, ep2, ep3 = axis_neighbours(tp, ep)
    me = tp * 4 + ep
    seqs, seq_len, d_model = h2_ref.shape
    tokens = acc.shape[0]
    rows = res.shape[1]
    half_pos = seq_len // 2
    experts = w_in.shape[0]
    capacity = rows // experts

    loads = [pltpu.make_async_copy(a, b, in_sem.at[n]) for n, (a, b) in enumerate((
        (x0_ref, xbuf), (wk_hbm, wkv.at[0]), (wv_hbm, wkv.at[1]), (h2_ref, hall.at[me]),
        (w_in_hbm, w_in), (w_out_hbm, w_out)))]
    for load in loads:
        load.start()

    barrier = pltpu.get_barrier_semaphore()
    peers = [(other, ep), (tp, ep2), (tp, ep1), (other, ep1), (other, ep2), (tp, ep3), (other, ep3)]
    for peer_tp, peer_ep in peers:
        pl.semaphore_signal(barrier, inc=1, device_id=(lax.axis_index('dp'), peer_tp, peer_ep), device_id_type=MESH)
    pl.semaphore_wait(barrier, len(peers))

    def half_at(k):
        return pl.ds(pl.multiple_of(k * half_pos, half_pos), half_pos)

    def block(owner, k):
        return hall.at[owner, :, half_at(k), :]

    sends = []
    for n, peer in enumerate(((other, ep), (tp, ep2), (tp, ep1))):
        for k in ((other, tp) if n == 0 else (tp, other)):
            sends.append(remote(h2_ref.at[:, half_at(k), :], block(me, k), hs_send.at[n, k], hs_recv.at[me, k], *peer))
    for copy in sends:
        copy.start()

    def arrived(ref, sem):
        remote(ref, ref, hs_send.at[0], sem, tp, ep).wait_recv()

    def block_arrived(owner, k):
        arrived(block(owner, k), hs_recv.at[owner, k])

    def forward(n, owner, k, *peer):
        copy = remote(block(owner, k), block(owner, k), hs_send.at[n, k], hs_recv.at[owner, k], *peer)
        copy.start()
        sends.append(copy)

    num_experts = router_ref.shape[0]
    ids_row = jnp.concatenate([ids_ref[s] for s in range(ids_ref.shape[0])], axis=1)
    expert = lax.broadcasted_iota(jnp.int32, (num_experts, tokens), 0)
    hot = [jnp.where(ids_row[c:c + 1] == expert, 1.0, 0.0) for c in range(2)]
    earlier = lax.broadcasted_iota(jnp.int32, (tokens, tokens), 0) <= lax.broadcasted_iota(jnp.int32, (tokens, tokens), 1)
    upto = mm(jnp.concatenate(hot, axis=0).astype(BF16), jnp.where(earlier, 1.0, 0.0).astype(BF16))
    base = (0.0, upto[:num_experts, tokens - 1:])
    wide_ids = ids_row.astype(F32)
    slot_rows = []
    for c in range(2):
        place = jnp.sum((upto[c * num_experts:(c + 1) * num_experts] - 1.0 + base[c]) * hot[c], axis=0, keepdims=True)
        slot_rows.append(jnp.where(place < capacity, wide_ids[c:c + 1] * capacity + place, -1.0))
    packed = jnp.concatenate(slot_rows + [wide_ids, jnp.zeros((4, tokens), F32)], axis=0)
    slot_row_ref[...] = packed[:2].astype(jnp.int32)
    slots_all[me] = packed[:2].astype(jnp.int32)
    columns_ref[...] = packed.T.astype(jnp.int32)
    slot_copies = [remote(slot_row_ref, slots_all.at[me], slot_send.at[n], slot_recv.at[me], *peer) for n, peer in enumerate(peers)]
    for copy in slot_copies:
        copy.start()
    send_h1 = remote(h1_ref, h1t_ref, h1_send, h1_recv, other, ep)
    send_h1.start()

    def cache_part(source, layer, owner, load=None):
        if load is None:
            load = pltpu.make_async_copy(source, xbuf, cache_sem)
            load.start()
        load.wait()

        @pl.loop(0, seqs)
        def _(s):
            a = rms_rows(xbuf[s], ln_attn_ref[layer])
            for n, ref in enumerate((k_ref, v_ref)):
                full = mm(a, wkv[n, layer])
                kvbuf[s, n] = full.T.astype(BF16).reshape(kvbuf.shape[2:])
                pltpu.make_async_copy(kvbuf.at[s, n], ref.at[layer, owner * seqs + s], store_sem.at[s, n]).start()

        @pl.loop(0, seqs)
        def _(s):
            for n, ref in enumerate((k_ref, v_ref)):
                pltpu.make_async_copy(kvbuf.at[s, n], ref.at[layer, owner * seqs + s], store_sem.at[s, n]).wait()

    loads[1].wait()
    loads[2].wait()
    cache_part(x0_ref, 0, tp, loads[0])
    cache_part(x0t_ref, 0, other)
    cache_part(h1_ref, 1, tp)

    y_owner, x_owner, c_owner = other * 4 + ep, tp * 4 + ep2, tp * 4 + ep1
    yx_owner, yc_owner, xc_owner, yxc_owner = other * 4 + ep2, other * 4 + ep1, tp * 4 + ep3, other * 4 + ep3
    for place, k in enumerate((tp, other)):
        with scope(f"w_y{place}"):
            block_arrived(y_owner, k)
        forward(3, y_owner, k, tp, ep2)
        forward(4, y_owner, k, tp, ep1)
    loads[3].wait()

    def own_tokens(owner):
        return hall[owner, :, half_at(tp), :].reshape(tokens // 2, d_model)

    for part in range(2):
        at = slice(part * (tokens // 2), (part + 1) * (tokens // 2))
        h_own = own_tokens(part * 4 + ep)
        acc[at] = h_own.astype(F32)
        b = rms_rows(h_own, ln_ffn_ref[1])
        logits = lax.dot_general(b.astype(F32), router_ref[...], (((1,), (1,)), ((), ())),
                                 precision=lax.Precision.HIGHEST, preferred_element_type=F32)
        grown = jnp.exp(logits - jnp.max(logits, axis=-1, keepdims=True))
        probs = grown / jnp.sum(grown, axis=-1, keepdims=True)
        lanes = lax.broadcasted_iota(jnp.int32, probs.shape, 1)
        picked = [jnp.sum(jnp.where(columns_ref[at, 2 + c:3 + c] == lanes, probs, 0.0), axis=-1, keepdims=True) for c in range(2)]
        both = picked[0] + picked[1]
        gates[at, 0:1] = picked[0] / both
        gates[at, 1:2] = picked[1] / both

    with scope("w_x"):
        for k in (tp, other):
            block_arrived(x_owner, k)
            forward(5, x_owner, k, tp, ep1)
    for peer_tp, peer_ep in peers:
        arrived(slots_all.at[peer_tp * 4 + peer_ep], slot_recv.at[peer_tp * 4 + peer_ep])
    loads[4].wait()
    loads[5].wait()

    def run_group(i, k):
        dest = k * 4 + i
        slots = slots_all[dest]
        want = me * rows + lax.broadcasted_iota(jnp.int32, (rows, tokens // 2), 0)
        chosen = None
        for part in range(2):
            h = hall[part * 4 + i, :, half_at(k), :].reshape(tokens // 2, d_model)
            at = slice(part * (tokens // 2), (part + 1) * (tokens // 2))
            pick = jnp.logical_or(slots[0:1, at] == want, slots[1:2, at] == want)
            term = mm(jnp.where(pick, 1.0, 0.0).astype(BF16), h)
            chosen = term if chosen is None else chosen + term
        b = rms_rows(chosen, ln_ffn_ref[1])
        for e in range(experts):
            at = slice(e * capacity, (e + 1) * capacity)
            hid = jax.nn.gelu(mm(b[at], w_in[e])).astype(BF16)
            res[dest, at] = mm(hid, w_out[e]).astype(BF16)
        return dest

    def give_back(i, k):
        dest = k * 4 + i
        return remote(res.at[dest], ret.at[me], ret_send.at[dest], ret_recv.at[me], k, i)

    def add_rows(source_ref, owner):
        step = 256

        @pl.loop(0, tokens // step)
        def _(r):
            at = pl.ds(pl.multiple_of(r * step, step), step)
            columns = owner * rows + lax.broadcasted_iota(jnp.int32, (step, rows), 1)
            total = acc[at, :]
            for c in range(2):
                pick = jnp.where(columns_ref[at, c:c + 1] == columns, 1.0, 0.0).astype(BF16)
                total = total + gates[at, c:c + 1] * mm(pick, source_ref[...])
            acc[at, :] = total

    with scope("w_yc"):
        for k in range(2):
            block_arrived(c_owner, k)
            block_arrived(yc_owner, k)

    @pl.loop(0, 4)
    def _(t):
        late = t // 2
        beside = lax.rem((t + 1) // 2, 2)
        i = ep + beside * (ep1 - ep)
        k = late * tp + (1 - late) * other
        run_group(i, k)

        @pl.when(t < 3)
        def _():
            give_back(i, k).start()

    add_rows(res.at[me], me)

    for place, k in enumerate((tp, other)):
        with scope(f"w_yx{place}"):
            block_arrived(yx_owner, k)
        forward(6, yx_owner, k, tp, ep1)
        with scope(f"w_far{place}"):
            block_arrived(xc_owner, k)
            block_arrived(yxc_owner, k)

        @pl.loop(0, 2)
        def _(t):
            i = (1 - t) * ep2 + t * ep3
            run_group(i, k)
            give_back(i, k).start()

        if place == 0:
            with scope("w_h1"):
                arrived(h1t_ref, h1_recv)
            cache_part(h1t_ref, 1, other)

    for peer_tp, peer_ep in ((tp, ep1), (other, ep), (other, ep1), (tp, ep2), (tp, ep3), (other, ep2), (other, ep3)):
        owner = peer_tp * 4 + peer_ep
        with scope("w_ret"):
            arrived(ret.at[owner], ret_recv.at[owner])
        add_rows(ret.at[owner], owner)
    out_ref[...] = acc[...].astype(BF16)

    for copy in sends + slot_copies + [send_h1]:
        copy.wait_send()
    for peer_tp, peer_ep in peers:
        give_back(peer_ep, peer_tp).wait_send()


def moe_layer(h2, h1, x0, x0t, expert_ids, ln_ffn, ln_attn, w_router, expert_in, expert_out, w_key, w_value):
    seqs, seq_len, d_model = h2.shape
    tokens = seqs * seq_len
    experts, _, d_ff = expert_in.shape
    groups = 8
    rows = experts * 4 * tokens // (experts * groups)
    inner = w_key.shape[2]
    heads = inner // 64
    any_spec = pl.BlockSpec(memory_space=pl.ANY)
    vmem_spec = pl.BlockSpec(memory_space=pltpu.VMEM)
    cache_shape = jax.ShapeDtypeStruct((2, 2 * seqs, heads, 64, seq_len), BF16)
    dma = pltpu.SemaphoreType.DMA
    return pl.pallas_call(
        moe_body,
        in_specs=[any_spec] * 4 + [vmem_spec] * 4 + [any_spec] * 4,
        out_specs=[vmem_spec, any_spec, any_spec, any_spec],
        out_shape=[jax.ShapeDtypeStruct((tokens, d_model), BF16), cache_shape, cache_shape, jax.ShapeDtypeStruct(h1.shape, BF16)],
        scratch_shapes=[
            pltpu.VMEM((groups,) + h2.shape, BF16),
            pltpu.VMEM((groups, rows, d_model), BF16),
            pltpu.VMEM((groups, rows, d_model), BF16),
            pltpu.VMEM(expert_in.shape, BF16),
            pltpu.VMEM(expert_out.shape, BF16),
            pltpu.VMEM((2, 2, d_model, inner), BF16),
            pltpu.VMEM((tokens, d_model), F32),
            pltpu.VMEM((2, tokens), jnp.int32),
            pltpu.VMEM((groups, 2, tokens), jnp.int32),
            pltpu.VMEM((tokens, 8), jnp.int32),
            pltpu.VMEM((tokens, 2), F32),
            pltpu.VMEM(h1.shape, BF16),
            pltpu.VMEM((seqs, 2, heads, 64, seq_len), BF16),
            dma((6,)), dma, dma((seqs, 2)), dma((7,)), dma((groups,)), dma((7, 2)), dma((groups, 2)),
            dma((groups,)), dma((groups,)), dma, dma,
        ],
        compiler_params=pltpu.CompilerParams(vmem_limit_bytes=67043328, collective_id=2, has_side_effects=True),
        cost_estimate=pl.CostEstimate(flops=40_000_000_000, bytes_accessed=64 << 20, transcendentals=0),
        name="moe",
    )(h2, h1, x0, x0t, jnp.swapaxes(expert_ids, 1, 2), ln_ffn, ln_attn, w_router.T, expert_in, expert_out, w_key, w_value)


def solution(mesh):
    act_spec = P(('dp', 'ep'), 'tp', None)
    col_spec = P(None, None, 'tp')
    row_spec = P(None, 'tp', None)
    expert_spec = P(('tp', 'ep'), None, None)
    cache_spec = P(None, ('dp', 'ep'), 'tp', None, None)
    in_specs = (act_spec, P(), P(), col_spec, col_spec, col_spec, row_spec, row_spec,
                P(None, 'tp'), P(None, 'tp'), P('tp', None), P(), expert_spec, expert_spec, act_spec)

    def device_fn(hidden_in, ln_attn, ln_ffn, w_query, w_key, w_value, w_out, bias_table, w_gate, w_up, w_down, w_router, expert_in, expert_out, expert_ids):
        h1, h2, x0, x0t = dense_layers(hidden_in, ln_attn, ln_ffn, w_query, w_key, w_value, w_out, bias_table, w_gate, w_up, w_down)
        hidden, k_cache, v_cache, _ = moe_layer(
            h2, h1, x0, x0t, expert_ids, ln_ffn, ln_attn, w_router, expert_in, expert_out, w_key, w_value)
        return hidden.reshape(hidden_in.shape), jnp.swapaxes(k_cache, 3, 4), jnp.swapaxes(v_cache, 3, 4)

    return jax.shard_map(device_fn, mesh=mesh, in_specs=in_specs, out_specs=(act_spec, cache_spec, cache_spec), check_vma=False)
```

```python
import contextlib

import jax
import jax.numpy as jnp
from jax import lax
from jax.experimental import pallas as pl
from jax.experimental.pallas import tpu as pltpu
from jax.sharding import PartitionSpec as P

EXACT_BUCKETS = 16
THRESHOLDS = (18, 20, 23, 26, 30, 34, 39, 45, 51, 58, 66, 76, 86, 98, 112)
EPSILON = 1e-6
F32 = jnp.float32
BF16 = jnp.bfloat16
VMEM_LIMIT = 60 * 1024 * 1024
MESH = pl.DeviceIdType.MESH


def scope(name):
    return contextlib.nullcontext()


def rms_rows(rows, ln_scale):
    wide = rows.astype(F32)
    inv_rms = lax.rsqrt(jnp.mean(wide * wide, axis=-1, keepdims=True) + EPSILON)
    return (wide * inv_rms * ln_scale).astype(BF16)


def mm(a, b):
    return lax.dot_general(a, b, (((1,), (0,)), ((), ())), preferred_element_type=F32)


def mm_t(a, b):
    return lax.dot_general(a, b, (((1,), (1,)), ((), ())), preferred_element_type=F32)


def bias_rows(table, seq_len):
    at = lax.broadcasted_iota(jnp.int32, (table.shape[1], 2 * seq_len), 1)
    rel = jnp.where(at == 0, 0, 2 * seq_len - at)
    bucket = jnp.minimum(rel, EXACT_BUCKETS)
    for threshold in THRESHOLDS:
        bucket = bucket + jnp.where(rel >= threshold, 1, 0)
    hot = jnp.where(bucket == lax.broadcasted_iota(jnp.int32, bucket.shape, 0), 1.0, 0.0)
    rows = jnp.dot(table, hot, precision=lax.Precision.HIGHEST, preferred_element_type=F32)
    return jnp.where(rel[:1] < seq_len, rows, -jnp.inf)


def softmax_bf16(scores):
    top = jnp.max(scores, axis=-1, keepdims=True)
    grown = jnp.exp(scores - top)
    return (grown * (1.0 / jnp.sum(grown, axis=-1, keepdims=True))).astype(BF16)


def axis_neighbours(tp, ep):
    core = lax.rem(ep, 2)
    beside = ep + 1 - 2 * core
    return beside, lax.rem(ep + 2, 4), lax.rem(beside + 2, 4)


def remote(src, dst, send, recv, tp, ep):
    return pltpu.make_async_remote_copy(
        src_ref=src, dst_ref=dst, send_sem=send, recv_sem=recv,
        device_id=(lax.axis_index('dp'), tp, ep), device_id_type=MESH)


def layers_body(hid_ref, ln_attn_ref, ln_ffn_ref, wq_hbm, wk_hbm, wv_hbm, wo_hbm, table_ref, wg_hbm, wu_hbm, wd_hbm,
                h1_ref, h2_ref, x0_ref, x0t_ref,
                x, a_ref, acc, w, wo, gu, wd, table_other, u_rows, bias_low, bias_high, qkv, ctx, stage,
                in_sem, own_sem, out_sem, x0_sem, entry_send, entry_recv, misc_send, misc_recv, y_send, y_recv, x_send, x_recv, c_send, c_recv, d_send, d_recv):
    tp, ep = lax.axis_index('tp'), lax.axis_index('ep')
    other = 1 - tp
    ep1, ep2, ep3 = axis_neighbours(tp, ep)
    seqs, seq_len, d_model = x.shape
    half = seq_len // 2
    tokens = seqs * seq_len
    quad = qkv.shape[2]

    def part(count, quarter):
        return pl.ds(pl.multiple_of(quarter * count, count), count)

    my_pos = part(half, tp)
    mine = hid_ref.at[pl.ds(tp * seqs, seqs)]
    theirs = hid_ref.at[pl.ds(other * seqs, seqs)]

    sources, places = [], []
    for layer in range(2):
        for kind, hbm in enumerate((wq_hbm, wk_hbm, wv_hbm)):
            sources.append(hbm.at[layer, part(256, ep), :])
            places.append(lambda q, layer=layer, kind=kind: w.at[layer, 1, kind, part(256, q), :])
        sources.append(wo_hbm.at[layer, part(128, ep), :])
        places.append(lambda q, layer=layer: wo.at[layer, 1, part(128, q), :])
        if layer == 0:
            for kind, hbm in enumerate((wg_hbm, wu_hbm)):
                sources.append(hbm.at[part(256, ep), :])
                places.append(lambda q, kind=kind: gu.at[1, kind, part(256, q), :])
            sources.append(wd_hbm.at[part(64, ep), :])
            places.append(lambda q: wd.at[1, part(64, q), :])

    own_x = pltpu.make_async_copy(mine, x.at[:, my_pos, :], in_sem.at[0])
    own_stage = pltpu.make_async_copy(theirs, stage, in_sem.at[1])
    own_x.start()
    own_loads = []
    for layer in range(2):
        for kind, hbm in enumerate((wq_hbm, wk_hbm, wv_hbm)):
            own_loads.append((hbm.at[layer], w.at[layer, 0, kind]))
        own_loads.append((wo_hbm.at[layer], wo.at[layer, 0]))
        if layer == 0:
            own_loads += [(wg_hbm, gu.at[0, 0]), (wu_hbm, gu.at[0, 1]), (wd_hbm, wd.at[0])]
    own_loads = [pltpu.make_async_copy(s, d, own_sem.at[n]) for n, (s, d) in enumerate(own_loads)]
    for load in own_loads:
        load.start()
    own_stage.start()

    barrier = pltpu.get_barrier_semaphore()
    for peer_tp, peer_ep in ((other, ep), (tp, ep2), (tp, ep1)):
        pl.semaphore_signal(barrier, inc=1, device_id=(lax.axis_index('dp'), peer_tp, peer_ep), device_id_type=MESH)
    pl.semaphore_wait(barrier, 3)

    def arrived(ref, sem):
        remote(ref, ref, misc_send.at[0], sem, tp, ep).wait_recv()

    pieces = range(len(sources))
    entry_copies = [remote(hid_ref.at[other * seqs + s], x.at[s, my_pos, :], entry_send.at[s], entry_recv.at[s], other, ep) for s in range(seqs)]
    send_u = remote(table_ref, table_other, misc_send.at[1], misc_recv.at[1], other, ep)
    send_rest = remote(mine, x0t_ref.at[:, my_pos, :], misc_send.at[2], misc_recv.at[2], other, ep)
    y_copies = [remote(sources[n], places[n](ep), y_send.at[n], y_recv.at[n], other, ep) for n in pieces]
    x_copies = [remote(places[n](ep), places[n](ep), x_send.at[n], x_recv.at[n], tp, ep2) for n in pieces]
    c_copies = [remote(places[n](ep), places[n](ep), c_send.at[n], c_recv.at[n], tp, ep1) for n in pieces]
    d_copies = [remote(places[n](ep2), places[n](ep2), d_send.at[n], d_recv.at[n], tp, ep1) for n in pieces]
    send_u.start()
    for copy in y_copies[:4] + entry_copies + y_copies[4:] + [send_rest]:
        copy.start()

    def pass_on(n):
        arrived(places[n](ep), y_recv.at[n])
        x_copies[n].start()
        c_copies[n].start()

    def pass_across(n):
        arrived(places[n](ep2), x_recv.at[n])
        d_copies[n].start()

    def complete(n):
        arrived(places[n](ep1), c_recv.at[n])
        arrived(places[n](ep3), d_recv.at[n])

    def build_bias(rows_ref, side):
        u_rows[...] = bias_rows(rows_ref[...].reshape(u_rows.shape[0], rows_ref.shape[2]), seq_len)

        @pl.loop(0, 8)
        def _(n):
            layer, pair = n // 4, lax.rem(n, 4)
            for sub in range(2):
                row = u_rows[pl.ds(n * 2 + sub, 1), :]
                wide = pltpu.roll(jnp.broadcast_to(row, (seq_len, 2 * seq_len)), 0, 1, stride=1, stride_axis=0)
                at = slice(sub * half, (sub + 1) * half)
                place = layer * 8 + side * 4 + pair
                bias_low[place, at, :] = wide[:half, :half]
                bias_high[place, at, :] = wide[half:, :seq_len]

    def begin_seq(layer, s):
        rows = part(seq_len, s)
        a_ref[rows, :] = rms_rows(x[s], ln_attn_ref[layer])
        acc[rows, :] = x[s].astype(F32)

    def end_seq(s):
        x[s] = acc[part(seq_len, s), :].astype(BF16)

    def each_seq(step, *args):
        @pl.loop(0, seqs)
        def _(s):
            step(*args, s)

    first = lax.broadcasted_iota(jnp.int32, (1, 128), 1) < 64

    def products(layer, side, block, rows):
        for kind in range(3):
            qkv[kind, rows, :] = mm(a_ref[rows, :], w[layer, side, kind, :, block * quad:(block + 1) * quad]).astype(BF16)

    def attend_seq(layer, side, block, s):
        rows = part(seq_len, s)
        for pair in range(quad // 128):
            lanes = slice(pair * 128, (pair + 1) * 128)
            place = layer * 8 + side * 4 + block * (quad // 128) + pair
            q, k, v = (qkv[kind, rows, lanes] for kind in range(3))
            none = jnp.zeros_like(q[:half])
            outs = []
            for upper in range(2):
                qs = q[half:] if upper else q[:half]
                ks, vs = (k, v) if upper else (k[:half], v[:half])
                both = jnp.concatenate([jnp.where(first, qs, none), jnp.where(first, none, qs)], axis=0)
                bias = bias_high[place] if upper else bias_low[place]
                got = mm(softmax_bf16(mm_t(both, ks) * 0.125 + bias), vs)
                outs.append(jnp.where(first, got[:half], got[half:]))
            ctx[rows, lanes] = jnp.concatenate(outs, axis=0).astype(BF16)

    def project_seq(layer, side, block, s):
        rows = part(seq_len, s)
        acc[rows, :] += mm(ctx[rows, :], wo[layer, side, block * quad:(block + 1) * quad, :])

    def attend(layer, side, block):
        products(layer, side, block, slice(None))
        each_seq(attend_seq, layer, side, block)

    def project(layer, side, block):
        each_seq(project_seq, layer, side, block)

    def dense(s):
        h = x[s]
        b = rms_rows(h, ln_ffn_ref[0])
        total = h.astype(F32)
        for side in range(2):
            hid = (jax.nn.gelu(mm(b, gu[side, 0])) * mm(b, gu[side, 1])).astype(BF16)
            total = total + mm(hid, wd[side])
        x[s] = total.astype(BF16)

    def heads(layer, side, block):
        attend(layer, side, block)
        project(layer, side, block)

    build_bias(table_ref, 0)
    arrived(table_other, misc_recv.at[1])
    build_bias(table_other, 1)
    own_stage.wait()
    own_x0t = pltpu.make_async_copy(stage, x0t_ref.at[:, my_pos, :], out_sem.at[0])
    own_x0t.start()

    with scope("w_l0_y"):
        for n in range(4):
            pass_on(n)
    with scope("w_l0_x"):
        for n in range(4):
            pass_across(n)
    own_x.wait()
    for n in range(4):
        own_loads[n].wait()
        complete(n)

    def x0_copy(s):
        return pltpu.make_async_copy(x.at[s], x0_ref.at[s], x0_sem.at[s])

    @pl.loop(0, seqs)
    def _(s):
        with scope("w_entry"):
            arrived(x.at[s, part(half, other), :], entry_recv.at[s])
        x0_copy(s).start()
        begin_seq(0, s)
        for side in range(2):
            for block in range(2):
                products(0, side, block, part(seq_len, s))
                attend_seq(0, side, block, s)
                project_seq(0, side, block, s)
        x0_copy(s).wait()
        end_seq(s)

        @pl.when(s == seqs - 2)
        def _():
            pass_on(4)

    with scope("w_ffn_y"):
        for n in range(5, 7):
            pass_on(n)
        pass_on(7)
    with scope("w_ffn_x"):
        for n in range(4, 7):
            pass_across(n)
    with scope("w_ffn_all"):
        for n in range(4, 7):
            own_loads[n].wait()
            complete(n)

    @pl.loop(0, seqs // 2)
    def _(s):
        dense(s)

    with scope("w_l1_k"):
        pass_on(8)

    @pl.loop(seqs // 2, seqs)
    def _(s):
        dense(s)

    out_h1 = pltpu.make_async_copy(x, h1_ref, out_sem.at[2])
    out_h1.start()
    each_seq(begin_seq, 1)
    for n in range(7, 11):
        own_loads[n].wait()
    attend(1, 0, 0)
    with scope("w_l1_v"):
        pass_on(9)
    project(1, 0, 0)
    heads(1, 0, 1)
    with scope("w_l1_o"):
        pass_on(10)
    with scope("w_l1_x"):
        for n in range(7, 10):
            pass_across(n)
    with scope("w_l1_all"):
        for n in range(7, 10):
            complete(n)
    attend(1, 1, 0)
    with scope("w_l1_o_all"):
        pass_across(10)
        complete(10)
    project(1, 1, 0)
    heads(1, 1, 1)
    out_h1.wait()
    each_seq(end_seq)
    out_h2 = pltpu.make_async_copy(x, h2_ref, out_sem.at[3])
    out_h2.start()

    with scope("w_rest"):
        arrived(x0t_ref.at[:, part(half, other), :], misc_recv.at[2])
    own_x0t.wait()
    for copy in entry_copies + [send_u, send_rest] + y_copies + x_copies + c_copies + d_copies:
        copy.wait_send()
    out_h2.wait()


def dense_layers(hidden_in, ln_attn, ln_ffn, w_query, w_key, w_value, w_out, bias_table, w_gate, w_up, w_down):
    batch, positions, d_model = hidden_in.shape
    seqs, seq_len = batch // 2, 2 * positions
    inner = w_query.shape[2]
    any_spec = pl.BlockSpec(memory_space=pl.ANY)
    vmem_spec = pl.BlockSpec(memory_space=pltpu.VMEM)
    dma = pltpu.SemaphoreType.DMA
    shape = jax.ShapeDtypeStruct((seqs, seq_len, d_model), BF16)
    return pl.pallas_call(
        layers_body,
        in_specs=[any_spec, vmem_spec, vmem_spec] + [any_spec] * 4 + [vmem_spec] + [any_spec] * 3,
        out_specs=[any_spec] * 4,
        out_shape=[shape] * 4,
        scratch_shapes=[
            pltpu.VMEM(shape.shape, BF16),
            pltpu.VMEM((seqs * seq_len, d_model), BF16),
            pltpu.VMEM((seqs * seq_len, d_model), F32),
            pltpu.VMEM((2, 2, 3, d_model, inner), BF16),
            pltpu.VMEM((2, 2, inner, d_model), BF16),
            pltpu.VMEM((2, 2) + w_gate.shape, BF16),
            pltpu.VMEM((2,) + w_down.shape, BF16),
            pltpu.VMEM(bias_table.shape, F32),
            pltpu.VMEM((bias_table.shape[0] * bias_table.shape[1], 2 * seq_len), F32),
            pltpu.VMEM((16, seq_len, seq_len // 2), F32),
            pltpu.VMEM((16, seq_len, seq_len), F32),
            pltpu.VMEM((3, seqs * seq_len, 256), BF16),
            pltpu.VMEM((seqs * seq_len, 256), BF16),
            pltpu.VMEM((seqs, positions, d_model), BF16),
            dma((2,)), dma((11,)), dma((4,)), dma((seqs,)), dma((seqs,)), dma((seqs,)), dma((3,)), dma((3,)),
        ] + [dma((11,))] * 8,
        compiler_params=pltpu.CompilerParams(vmem_limit_bytes=VMEM_LIMIT, collective_id=1, has_side_effects=True),
        cost_estimate=pl.CostEstimate(flops=32_000_000_000, bytes_accessed=40 << 20, transcendentals=0),
        name="dense_layers",
    )(hidden_in, ln_attn, ln_ffn, w_query, w_key, w_value, w_out, bias_table, w_gate, w_up, w_down)


def moe_body(h2_ref, h1_ref, x0_ref, x0t_ref, ids_ref, ln_ffn_ref, ln_attn_ref, router_ref,
             w_in_hbm, w_out_hbm, wk_hbm, wv_hbm,
             out_ref, k_ref, v_ref, h1t_ref,
             hall, res, ret, w_in, w_out, wkv, acc, slot_row_ref, slots_all, columns_ref, gates, xbuf, kvbuf,
             in_sem, cache_sem, store_sem, slot_send, slot_recv, hs_send, hs_recv, ret_send, ret_recv, h1_send, h1_recv):
    tp, ep = lax.axis_index('tp'), lax.axis_index('ep')
    other = 1 - tp
    ep1, ep2, ep3 = axis_neighbours(tp, ep)
    me = tp * 4 + ep
    seqs, seq_len, d_model = h2_ref.shape
    tokens = acc.shape[0]
    rows = res.shape[1]
    half_pos = seq_len // 2
    experts = w_in.shape[0]
    capacity = rows // experts

    loads = [pltpu.make_async_copy(a, b, in_sem.at[n]) for n, (a, b) in enumerate((
        (x0_ref, xbuf), (wk_hbm, wkv.at[0]), (wv_hbm, wkv.at[1]), (h2_ref, hall.at[me]),
        (w_in_hbm, w_in), (w_out_hbm, w_out)))]
    for load in loads:
        load.start()

    barrier = pltpu.get_barrier_semaphore()
    peers = [(other, ep), (tp, ep2), (tp, ep1), (other, ep1), (other, ep2), (tp, ep3), (other, ep3)]
    for peer_tp, peer_ep in peers:
        pl.semaphore_signal(barrier, inc=1, device_id=(lax.axis_index('dp'), peer_tp, peer_ep), device_id_type=MESH)
    pl.semaphore_wait(barrier, len(peers))

    def half_at(k):
        return pl.ds(pl.multiple_of(k * half_pos, half_pos), half_pos)

    def block(owner, k):
        return hall.at[owner, :, half_at(k), :]

    sends = []
    for n, peer in enumerate(((other, ep), (tp, ep2), (tp, ep1))):
        for k in ((other, tp) if n == 0 else (tp, other)):
            sends.append(remote(h2_ref.at[:, half_at(k), :], block(me, k), hs_send.at[n, k], hs_recv.at[me, k], *peer))
    for copy in sends:
        copy.start()

    def arrived(ref, sem):
        remote(ref, ref, hs_send.at[0], sem, tp, ep).wait_recv()

    def block_arrived(owner, k):
        arrived(block(owner, k), hs_recv.at[owner, k])

    def forward(n, owner, k, *peer):
        copy = remote(block(owner, k), block(owner, k), hs_send.at[n, k], hs_recv.at[owner, k], *peer)
        copy.start()
        sends.append(copy)

    num_experts = router_ref.shape[0]
    ids_row = jnp.concatenate([ids_ref[s] for s in range(ids_ref.shape[0])], axis=1)
    expert = lax.broadcasted_iota(jnp.int32, (num_experts, tokens), 0)
    hot = [jnp.where(ids_row[c:c + 1] == expert, 1.0, 0.0) for c in range(2)]
    earlier = lax.broadcasted_iota(jnp.int32, (tokens, tokens), 0) <= lax.broadcasted_iota(jnp.int32, (tokens, tokens), 1)
    upto = mm(jnp.concatenate(hot, axis=0).astype(BF16), jnp.where(earlier, 1.0, 0.0).astype(BF16))
    base = (0.0, upto[:num_experts, tokens - 1:])
    wide_ids = ids_row.astype(F32)
    slot_rows = []
    for c in range(2):
        place = jnp.sum((upto[c * num_experts:(c + 1) * num_experts] - 1.0 + base[c]) * hot[c], axis=0, keepdims=True)
        slot_rows.append(jnp.where(place < capacity, wide_ids[c:c + 1] * capacity + place, -1.0))
    packed = jnp.concatenate(slot_rows + [wide_ids, jnp.zeros((4, tokens), F32)], axis=0)
    slot_row_ref[...] = packed[:2].astype(jnp.int32)
    slots_all[me] = packed[:2].astype(jnp.int32)
    columns_ref[...] = packed.T.astype(jnp.int32)
    slot_copies = [remote(slot_row_ref, slots_all.at[me], slot_send.at[n], slot_recv.at[me], *peer) for n, peer in enumerate(peers)]
    for copy in slot_copies:
        copy.start()
    send_h1 = remote(h1_ref, h1t_ref, h1_send, h1_recv, other, ep)
    send_h1.start()

    def cache_part(source, layer, owner, load=None):
        if load is None:
            load = pltpu.make_async_copy(source, xbuf, cache_sem)
            load.start()
        load.wait()

        @pl.loop(0, seqs)
        def _(s):
            a = rms_rows(xbuf[s], ln_attn_ref[layer])
            for n, ref in enumerate((k_ref, v_ref)):
                full = mm(a, wkv[n, layer])
                kvbuf[s, n] = full.T.astype(BF16).reshape(kvbuf.shape[2:])
                pltpu.make_async_copy(kvbuf.at[s, n], ref.at[layer, owner * seqs + s], store_sem.at[s, n]).start()

        @pl.loop(0, seqs)
        def _(s):
            for n, ref in enumerate((k_ref, v_ref)):
                pltpu.make_async_copy(kvbuf.at[s, n], ref.at[layer, owner * seqs + s], store_sem.at[s, n]).wait()

    loads[1].wait()
    loads[2].wait()
    cache_part(x0_ref, 0, tp, loads[0])
    cache_part(x0t_ref, 0, other)
    cache_part(h1_ref, 1, tp)

    y_owner, x_owner, c_owner = other * 4 + ep, tp * 4 + ep2, tp * 4 + ep1
    yx_owner, yc_owner, xc_owner, yxc_owner = other * 4 + ep2, other * 4 + ep1, tp * 4 + ep3, other * 4 + ep3
    for place, k in enumerate((tp, other)):
        with scope(f"w_y{place}"):
            block_arrived(y_owner, k)
        forward(3, y_owner, k, tp, ep2)
        forward(4, y_owner, k, tp, ep1)
    loads[3].wait()

    def own_tokens(owner):
        return hall[owner, :, half_at(tp), :].reshape(tokens // 2, d_model)

    for part in range(2):
        at = slice(part * (tokens // 2), (part + 1) * (tokens // 2))
        h_own = own_tokens(part * 4 + ep)
        acc[at] = h_own.astype(F32)
        b = rms_rows(h_own, ln_ffn_ref[1])
        logits = lax.dot_general(b.astype(F32), router_ref[...], (((1,), (1,)), ((), ())),
                                 precision=lax.Precision.HIGHEST, preferred_element_type=F32)
        grown = jnp.exp(logits - jnp.max(logits, axis=-1, keepdims=True))
        probs = grown / jnp.sum(grown, axis=-1, keepdims=True)
        lanes = lax.broadcasted_iota(jnp.int32, probs.shape, 1)
        picked = [jnp.sum(jnp.where(columns_ref[at, 2 + c:3 + c] == lanes, probs, 0.0), axis=-1, keepdims=True) for c in range(2)]
        both = picked[0] + picked[1]
        gates[at, 0:1] = picked[0] / both
        gates[at, 1:2] = picked[1] / both

    with scope("w_x"):
        for k in (tp, other):
            block_arrived(x_owner, k)
            forward(5, x_owner, k, tp, ep1)
    for peer_tp, peer_ep in peers:
        arrived(slots_all.at[peer_tp * 4 + peer_ep], slot_recv.at[peer_tp * 4 + peer_ep])
    loads[4].wait()
    loads[5].wait()

    def run_group(i, k):
        dest = k * 4 + i
        slots = slots_all[dest]
        want = me * rows + lax.broadcasted_iota(jnp.int32, (rows, tokens // 2), 0)
        chosen = None
        for part in range(2):
            h = hall[part * 4 + i, :, half_at(k), :].reshape(tokens // 2, d_model)
            at = slice(part * (tokens // 2), (part + 1) * (tokens // 2))
            pick = jnp.logical_or(slots[0:1, at] == want, slots[1:2, at] == want)
            term = mm(jnp.where(pick, 1.0, 0.0).astype(BF16), h)
            chosen = term if chosen is None else chosen + term
        b = rms_rows(chosen, ln_ffn_ref[1])
        for e in range(experts):
            at = slice(e * capacity, (e + 1) * capacity)
            hid = jax.nn.gelu(mm(b[at], w_in[e])).astype(BF16)
            res[dest, at] = mm(hid, w_out[e]).astype(BF16)
        return dest

    def give_back(i, k):
        dest = k * 4 + i
        return remote(res.at[dest], ret.at[me], ret_send.at[dest], ret_recv.at[me], k, i)

    def add_rows(source_ref, owner):
        step = 256

        @pl.loop(0, tokens // step)
        def _(r):
            at = pl.ds(pl.multiple_of(r * step, step), step)
            columns = owner * rows + lax.broadcasted_iota(jnp.int32, (step, rows), 1)
            total = acc[at, :]
            for c in range(2):
                pick = jnp.where(columns_ref[at, c:c + 1] == columns, 1.0, 0.0).astype(BF16)
                total = total + gates[at, c:c + 1] * mm(pick, source_ref[...])
            acc[at, :] = total

    with scope("w_yc"):
        for k in range(2):
            block_arrived(c_owner, k)
            block_arrived(yc_owner, k)

    @pl.loop(0, 4)
    def _(t):
        late = t // 2
        beside = lax.rem((t + 1) // 2, 2)
        i = ep + beside * (ep1 - ep)
        k = late * tp + (1 - late) * other
        run_group(i, k)

        @pl.when(t < 3)
        def _():
            give_back(i, k).start()

    add_rows(res.at[me], me)

    for place, k in enumerate((tp, other)):
        with scope(f"w_yx{place}"):
            block_arrived(yx_owner, k)
        forward(6, yx_owner, k, tp, ep1)
        with scope(f"w_far{place}"):
            block_arrived(xc_owner, k)
            block_arrived(yxc_owner, k)

        @pl.loop(0, 2)
        def _(t):
            i = (1 - t) * ep2 + t * ep3
            run_group(i, k)
            give_back(i, k).start()

        if place == 0:
            with scope("w_h1"):
                arrived(h1t_ref, h1_recv)
            cache_part(h1t_ref, 1, other)

    @pl.loop(1, 8)
    def _(n):
        across, beside, far = lax.rem(n // 2, 2), lax.rem(n, 2), n // 4
        peer_tp = tp + across * (other - tp)
        peer_ep = lax.rem(ep + beside * (ep1 - ep) + 2 * far, 4)
        owner = peer_tp * 4 + peer_ep
        with scope("w_ret"):
            arrived(ret.at[owner], ret_recv.at[owner])
        add_rows(ret.at[owner], owner)

    out_ref[...] = acc[...].astype(BF16)

    for copy in sends + slot_copies + [send_h1]:
        copy.wait_send()
    for peer_tp, peer_ep in peers:
        give_back(peer_ep, peer_tp).wait_send()


def moe_layer(h2, h1, x0, x0t, expert_ids, ln_ffn, ln_attn, w_router, expert_in, expert_out, w_key, w_value):
    seqs, seq_len, d_model = h2.shape
    tokens = seqs * seq_len
    experts, _, d_ff = expert_in.shape
    groups = 8
    rows = experts * 4 * tokens // (experts * groups)
    inner = w_key.shape[2]
    heads = inner // 64
    any_spec = pl.BlockSpec(memory_space=pl.ANY)
    vmem_spec = pl.BlockSpec(memory_space=pltpu.VMEM)
    cache_shape = jax.ShapeDtypeStruct((2, 2 * seqs, heads, 64, seq_len), BF16)
    dma = pltpu.SemaphoreType.DMA
    return pl.pallas_call(
        moe_body,
        in_specs=[any_spec] * 4 + [vmem_spec] * 4 + [any_spec] * 4,
        out_specs=[vmem_spec, any_spec, any_spec, any_spec],
        out_shape=[jax.ShapeDtypeStruct((tokens, d_model), BF16), cache_shape, cache_shape, jax.ShapeDtypeStruct(h1.shape, BF16)],
        scratch_shapes=[
            pltpu.VMEM((groups,) + h2.shape, BF16),
            pltpu.VMEM((groups, rows, d_model), BF16),
            pltpu.VMEM((groups, rows, d_model), BF16),
            pltpu.VMEM(expert_in.shape, BF16),
            pltpu.VMEM(expert_out.shape, BF16),
            pltpu.VMEM((2, 2, d_model, inner), BF16),
            pltpu.VMEM((tokens, d_model), F32),
            pltpu.VMEM((2, tokens), jnp.int32),
            pltpu.VMEM((groups, 2, tokens), jnp.int32),
            pltpu.VMEM((tokens, 8), jnp.int32),
            pltpu.VMEM((tokens, 2), F32),
            pltpu.VMEM(h1.shape, BF16),
            pltpu.VMEM((seqs, 2, heads, 64, seq_len), BF16),
            dma((6,)), dma, dma((seqs, 2)), dma((7,)), dma((groups,)), dma((7, 2)), dma((groups, 2)),
            dma((groups,)), dma((groups,)), dma, dma,
        ],
        compiler_params=pltpu.CompilerParams(vmem_limit_bytes=67043328, collective_id=2, has_side_effects=True),
        cost_estimate=pl.CostEstimate(flops=40_000_000_000, bytes_accessed=64 << 20, transcendentals=0),
        name="moe",
    )(h2, h1, x0, x0t, jnp.swapaxes(expert_ids, 1, 2), ln_ffn, ln_attn, w_router.T, expert_in, expert_out, w_key, w_value)


def solution(mesh):
    act_spec = P(('dp', 'ep'), 'tp', None)
    col_spec = P(None, None, 'tp')
    row_spec = P(None, 'tp', None)
    expert_spec = P(('tp', 'ep'), None, None)
    cache_spec = P(None, ('dp', 'ep'), 'tp', None, None)
    in_specs = (act_spec, P(), P(), col_spec, col_spec, col_spec, row_spec, row_spec,
                P(None, 'tp'), P(None, 'tp'), P('tp', None), P(), expert_spec, expert_spec, act_spec)

    def device_fn(hidden_in, ln_attn, ln_ffn, w_query, w_key, w_value, w_out, bias_table, w_gate, w_up, w_down, w_router, expert_in, expert_out, expert_ids):
        h1, h2, x0, x0t = dense_layers(hidden_in, ln_attn, ln_ffn, w_query, w_key, w_value, w_out, bias_table, w_gate, w_up, w_down)
        hidden, k_cache, v_cache, _ = moe_layer(
            h2, h1, x0, x0t, expert_ids, ln_ffn, ln_attn, w_router, expert_in, expert_out, w_key, w_value)
        return hidden.reshape(hidden_in.shape), jnp.swapaxes(k_cache, 3, 4), jnp.swapaxes(v_cache, 3, 4)

    return jax.shard_map(device_fn, mesh=mesh, in_specs=in_specs, out_specs=(act_spec, cache_spec, cache_spec), check_vma=False)
```

```python
import contextlib

import jax
import jax.numpy as jnp
from jax import lax
from jax.experimental import pallas as pl
from jax.experimental.pallas import tpu as pltpu
from jax.sharding import PartitionSpec as P

EXACT_BUCKETS = 16
THRESHOLDS = (18, 20, 23, 26, 30, 34, 39, 45, 51, 58, 66, 76, 86, 98, 112)
EPSILON = 1e-6
F32 = jnp.float32
BF16 = jnp.bfloat16
VMEM_LIMIT = 60 * 1024 * 1024
MESH = pl.DeviceIdType.MESH


def scope(name):
    return contextlib.nullcontext()


def rms_rows(rows, ln_scale):
    wide = rows.astype(F32)
    inv_rms = lax.rsqrt(jnp.mean(wide * wide, axis=-1, keepdims=True) + EPSILON)
    return (wide * inv_rms * ln_scale).astype(BF16)


def mm(a, b):
    return lax.dot_general(a, b, (((1,), (0,)), ((), ())), preferred_element_type=F32)


def mm_t(a, b):
    return lax.dot_general(a, b, (((1,), (1,)), ((), ())), preferred_element_type=F32)


def bias_rows(table, seq_len):
    at = lax.broadcasted_iota(jnp.int32, (table.shape[1], 2 * seq_len), 1)
    rel = jnp.where(at == 0, 0, 2 * seq_len - at)
    bucket = jnp.minimum(rel, EXACT_BUCKETS)
    for threshold in THRESHOLDS:
        bucket = bucket + jnp.where(rel >= threshold, 1, 0)
    hot = jnp.where(bucket == lax.broadcasted_iota(jnp.int32, bucket.shape, 0), 1.0, 0.0)
    rows = jnp.dot(table, hot, precision=lax.Precision.HIGHEST, preferred_element_type=F32)
    return jnp.where(rel[:1] < seq_len, rows, -jnp.inf)


def softmax_bf16(scores):
    top = jnp.max(scores, axis=-1, keepdims=True)
    grown = jnp.exp(scores - top)
    return (grown * (1.0 / jnp.sum(grown, axis=-1, keepdims=True))).astype(BF16)


def axis_neighbours(tp, ep):
    core = lax.rem(ep, 2)
    beside = ep + 1 - 2 * core
    return beside, lax.rem(ep + 2, 4), lax.rem(beside + 2, 4)


def remote(src, dst, send, recv, tp, ep):
    return pltpu.make_async_remote_copy(
        src_ref=src, dst_ref=dst, send_sem=send, recv_sem=recv,
        device_id=(lax.axis_index('dp'), tp, ep), device_id_type=MESH)


def layers_body(hid_ref, ln_attn_ref, ln_ffn_ref, wq_hbm, wk_hbm, wv_hbm, wo_hbm, table_ref, wg_hbm, wu_hbm, wd_hbm,
                h1_ref, h2_ref, x0_ref, x0t_ref,
                x, a_ref, acc, w, wo, gu, wd, table_other, u_rows, bias_low, bias_high, qkv, ctx, stage,
                in_sem, own_sem, out_sem, x0_sem, entry_send, entry_recv, misc_send, misc_recv, y_send, y_recv, x_send, x_recv, c_send, c_recv, d_send, d_recv):
    tp, ep = lax.axis_index('tp'), lax.axis_index('ep')
    other = 1 - tp
    ep1, ep2, ep3 = axis_neighbours(tp, ep)
    seqs, seq_len, d_model = x.shape
    half = seq_len // 2
    tokens = seqs * seq_len
    quad = qkv.shape[2]

    def part(count, quarter):
        return pl.ds(pl.multiple_of(quarter * count, count), count)

    my_pos = part(half, tp)
    mine = hid_ref.at[pl.ds(tp * seqs, seqs)]
    theirs = hid_ref.at[pl.ds(other * seqs, seqs)]

    sources, places = [], []
    for layer in range(2):
        for kind, hbm in enumerate((wq_hbm, wk_hbm, wv_hbm)):
            sources.append(hbm.at[layer, part(256, ep), :])
            places.append(lambda q, layer=layer, kind=kind: w.at[layer, 1, kind, part(256, q), :])
        sources.append(wo_hbm.at[layer, part(128, ep), :])
        places.append(lambda q, layer=layer: wo.at[layer, 1, part(128, q), :])
        if layer == 0:
            for kind, hbm in enumerate((wg_hbm, wu_hbm)):
                sources.append(hbm.at[part(256, ep), :])
                places.append(lambda q, kind=kind: gu.at[1, kind, part(256, q), :])
            sources.append(wd_hbm.at[part(64, ep), :])
            places.append(lambda q: wd.at[1, part(64, q), :])

    own_x = pltpu.make_async_copy(mine, x.at[:, my_pos, :], in_sem.at[0])
    own_stage = pltpu.make_async_copy(theirs, stage, in_sem.at[1])
    own_x.start()
    own_loads = []
    for layer in range(2):
        for kind, hbm in enumerate((wq_hbm, wk_hbm, wv_hbm)):
            own_loads.append((hbm.at[layer], w.at[layer, 0, kind]))
        own_loads.append((wo_hbm.at[layer], wo.at[layer, 0]))
        if layer == 0:
            own_loads += [(wg_hbm, gu.at[0, 0]), (wu_hbm, gu.at[0, 1]), (wd_hbm, wd.at[0])]
    own_loads = [pltpu.make_async_copy(s, d, own_sem.at[n]) for n, (s, d) in enumerate(own_loads)]
    for load in own_loads:
        load.start()
    own_stage.start()

    barrier = pltpu.get_barrier_semaphore()
    for peer_tp, peer_ep in ((other, ep), (tp, ep2), (tp, ep1)):
        pl.semaphore_signal(barrier, inc=1, device_id=(lax.axis_index('dp'), peer_tp, peer_ep), device_id_type=MESH)
    pl.semaphore_wait(barrier, 3)

    def arrived(ref, sem):
        remote(ref, ref, misc_send.at[0], sem, tp, ep).wait_recv()

    pieces = range(len(sources))
    entry_copies = [remote(hid_ref.at[other * seqs + s], x.at[s, my_pos, :], entry_send.at[s], entry_recv.at[s], other, ep) for s in range(seqs)]
    send_u = remote(table_ref, table_other, misc_send.at[1], misc_recv.at[1], other, ep)
    send_rest = remote(mine, x0t_ref.at[:, my_pos, :], misc_send.at[2], misc_recv.at[2], other, ep)
    y_copies = [remote(sources[n], places[n](ep), y_send.at[n], y_recv.at[n], other, ep) for n in pieces]
    x_copies = [remote(places[n](ep), places[n](ep), x_send.at[n], x_recv.at[n], tp, ep2) for n in pieces]
    c_copies = [remote(places[n](ep), places[n](ep), c_send.at[n], c_recv.at[n], tp, ep1) for n in pieces]
    d_copies = [remote(places[n](ep2), places[n](ep2), d_send.at[n], d_recv.at[n], tp, ep1) for n in pieces]
    send_u.start()
    for copy in y_copies[:4] + entry_copies + y_copies[4:] + [send_rest]:
        copy.start()

    def pass_on(n):
        arrived(places[n](ep), y_recv.at[n])
        x_copies[n].start()
        c_copies[n].start()

    def pass_across(n):
        arrived(places[n](ep2), x_recv.at[n])
        d_copies[n].start()

    def complete(n):
        arrived(places[n](ep1), c_recv.at[n])
        arrived(places[n](ep3), d_recv.at[n])

    def build_bias(rows_ref, side):
        u_rows[...] = bias_rows(rows_ref[...].reshape(u_rows.shape[0], rows_ref.shape[2]), seq_len)

        @pl.loop(0, 8)
        def _(n):
            layer, pair = n // 4, lax.rem(n, 4)
            for sub in range(2):
                row = u_rows[pl.ds(n * 2 + sub, 1), :]
                wide = pltpu.roll(jnp.broadcast_to(row, (seq_len, 2 * seq_len)), 0, 1, stride=1, stride_axis=0)
                at = slice(sub * half, (sub + 1) * half)
                place = layer * 8 + side * 4 + pair
                bias_low[place, at, :] = wide[:half, :half]
                bias_high[place, at, :] = wide[half:, :seq_len]

    def begin_seq(layer, s):
        rows = part(seq_len, s)
        a_ref[rows, :] = rms_rows(x[s], ln_attn_ref[layer])
        acc[rows, :] = x[s].astype(F32)

    def end_seq(s):
        x[s] = acc[part(seq_len, s), :].astype(BF16)

    def each_seq(step, *args):
        @pl.loop(0, seqs)
        def _(s):
            step(*args, s)

    first = lax.broadcasted_iota(jnp.int32, (1, 128), 1) < 64

    def products(layer, side, block, rows):
        for kind in range(3):
            qkv[kind, rows, :] = mm(a_ref[rows, :], w[layer, side, kind, :, block * quad:(block + 1) * quad]).astype(BF16)

    def attend_seq(layer, side, block, s):
        rows = part(seq_len, s)
        for pair in range(quad // 128):
            lanes = slice(pair * 128, (pair + 1) * 128)
            place = layer * 8 + side * 4 + block * (quad // 128) + pair
            q, k, v = (qkv[kind, rows, lanes] for kind in range(3))
            none = jnp.zeros_like(q[:half])
            outs = []
            for upper in range(2):
                qs = q[half:] if upper else q[:half]
                ks, vs = (k, v) if upper else (k[:half], v[:half])
                both = jnp.concatenate([jnp.where(first, qs, none), jnp.where(first, none, qs)], axis=0)
                bias = bias_high[place] if upper else bias_low[place]
                got = mm(softmax_bf16(mm_t(both, ks) * 0.125 + bias), vs)
                outs.append(jnp.where(first, got[:half], got[half:]))
            ctx[rows, lanes] = jnp.concatenate(outs, axis=0).astype(BF16)

    def project_seq(layer, side, block, s):
        rows = part(seq_len, s)
        acc[rows, :] += mm(ctx[rows, :], wo[layer, side, block * quad:(block + 1) * quad, :])

    def attend(layer, side, block):
        products(layer, side, block, slice(None))
        each_seq(attend_seq, layer, side, block)

    def project(layer, side, block):
        each_seq(project_seq, layer, side, block)

    def dense(s):
        h = x[s]
        b = rms_rows(h, ln_ffn_ref[0])
        total = h.astype(F32)
        for side in range(2):
            hid = (jax.nn.gelu(mm(b, gu[side, 0])) * mm(b, gu[side, 1])).astype(BF16)
            total = total + mm(hid, wd[side])
        x[s] = total.astype(BF16)

    def heads(layer, side, block):
        attend(layer, side, block)
        project(layer, side, block)

    build_bias(table_ref, 0)
    arrived(table_other, misc_recv.at[1])
    build_bias(table_other, 1)
    own_stage.wait()
    own_x0t = pltpu.make_async_copy(stage, x0t_ref.at[:, my_pos, :], out_sem.at[0])
    own_x0t.start()

    with scope("w_l0_y"):
        for n in range(4):
            pass_on(n)
    with scope("w_l0_x"):
        for n in range(4):
            pass_across(n)
    own_x.wait()
    for n in range(4):
        own_loads[n].wait()
        complete(n)

    def x0_copy(s):
        return pltpu.make_async_copy(x.at[s], x0_ref.at[s], x0_sem.at[s])

    @pl.loop(0, seqs)
    def _(s):
        with scope("w_entry"):
            arrived(x.at[s, part(half, other), :], entry_recv.at[s])
        x0_copy(s).start()
        begin_seq(0, s)
        for side in range(2):
            for block in range(2):
                products(0, side, block, part(seq_len, s))
                attend_seq(0, side, block, s)
                project_seq(0, side, block, s)
            if side == 0:
                @pl.when(s == seqs - 1)
                def _():
                    pass_on(5)
                    pass_on(6)
        x0_copy(s).wait()
        end_seq(s)

        @pl.when(s == seqs - 2)
        def _():
            pass_on(4)

    with scope("w_ffn_y"):
        pass_on(7)
    with scope("w_ffn_x"):
        for n in range(4, 7):
            pass_across(n)
    with scope("w_ffn_all"):
        for n in range(4, 7):
            own_loads[n].wait()
            complete(n)

    @pl.loop(0, seqs // 2)
    def _(s):
        dense(s)

    with scope("w_l1_k"):
        pass_on(8)

    @pl.loop(seqs // 2, seqs)
    def _(s):
        dense(s)

    out_h1 = pltpu.make_async_copy(x, h1_ref, out_sem.at[2])
    out_h1.start()
    each_seq(begin_seq, 1)
    for n in range(7, 11):
        own_loads[n].wait()
    attend(1, 0, 0)
    with scope("w_l1_v"):
        pass_on(9)
    project(1, 0, 0)
    heads(1, 0, 1)
    with scope("w_l1_o"):
        pass_on(10)
    with scope("w_l1_x"):
        for n in range(7, 10):
            pass_across(n)
    with scope("w_l1_all"):
        for n in range(7, 10):
            complete(n)
    attend(1, 1, 0)
    with scope("w_l1_o_all"):
        pass_across(10)
        complete(10)
    project(1, 1, 0)
    heads(1, 1, 1)
    out_h1.wait()
    each_seq(end_seq)
    out_h2 = pltpu.make_async_copy(x, h2_ref, out_sem.at[3])
    out_h2.start()

    with scope("w_rest"):
        arrived(x0t_ref.at[:, part(half, other), :], misc_recv.at[2])
    own_x0t.wait()
    for copy in entry_copies + [send_u, send_rest] + y_copies + x_copies + c_copies + d_copies:
        copy.wait_send()
    out_h2.wait()


def dense_layers(hidden_in, ln_attn, ln_ffn, w_query, w_key, w_value, w_out, bias_table, w_gate, w_up, w_down):
    batch, positions, d_model = hidden_in.shape
    seqs, seq_len = batch // 2, 2 * positions
    inner = w_query.shape[2]
    any_spec = pl.BlockSpec(memory_space=pl.ANY)
    vmem_spec = pl.BlockSpec(memory_space=pltpu.VMEM)
    dma = pltpu.SemaphoreType.DMA
    shape = jax.ShapeDtypeStruct((seqs, seq_len, d_model), BF16)
    return pl.pallas_call(
        layers_body,
        in_specs=[any_spec, vmem_spec, vmem_spec] + [any_spec] * 4 + [vmem_spec] + [any_spec] * 3,
        out_specs=[any_spec] * 4,
        out_shape=[shape] * 4,
        scratch_shapes=[
            pltpu.VMEM(shape.shape, BF16),
            pltpu.VMEM((seqs * seq_len, d_model), BF16),
            pltpu.VMEM((seqs * seq_len, d_model), F32),
            pltpu.VMEM((2, 2, 3, d_model, inner), BF16),
            pltpu.VMEM((2, 2, inner, d_model), BF16),
            pltpu.VMEM((2, 2) + w_gate.shape, BF16),
            pltpu.VMEM((2,) + w_down.shape, BF16),
            pltpu.VMEM(bias_table.shape, F32),
            pltpu.VMEM((bias_table.shape[0] * bias_table.shape[1], 2 * seq_len), F32),
            pltpu.VMEM((16, seq_len, seq_len // 2), F32),
            pltpu.VMEM((16, seq_len, seq_len), F32),
            pltpu.VMEM((3, seqs * seq_len, 256), BF16),
            pltpu.VMEM((seqs * seq_len, 256), BF16),
            pltpu.VMEM((seqs, positions, d_model), BF16),
            dma((2,)), dma((11,)), dma((4,)), dma((seqs,)), dma((seqs,)), dma((seqs,)), dma((3,)), dma((3,)),
        ] + [dma((11,))] * 8,
        compiler_params=pltpu.CompilerParams(vmem_limit_bytes=VMEM_LIMIT, collective_id=1, has_side_effects=True),
        cost_estimate=pl.CostEstimate(flops=32_000_000_000, bytes_accessed=40 << 20, transcendentals=0),
        name="dense_layers",
    )(hidden_in, ln_attn, ln_ffn, w_query, w_key, w_value, w_out, bias_table, w_gate, w_up, w_down)


def moe_body(h2_ref, h1_ref, x0_ref, x0t_ref, ids_ref, ln_ffn_ref, ln_attn_ref, router_ref,
             w_in_hbm, w_out_hbm, wk_hbm, wv_hbm,
             out_ref, k_ref, v_ref, h1t_ref,
             hall, res, ret, w_in, w_out, wkv, acc, slot_row_ref, slots_all, columns_ref, gates, xbuf, kvbuf,
             in_sem, cache_sem, store_sem, slot_send, slot_recv, hs_send, hs_recv, ret_send, ret_recv, h1_send, h1_recv):
    tp, ep = lax.axis_index('tp'), lax.axis_index('ep')
    other = 1 - tp
    ep1, ep2, ep3 = axis_neighbours(tp, ep)
    me = tp * 4 + ep
    seqs, seq_len, d_model = h2_ref.shape
    tokens = acc.shape[0]
    rows = res.shape[1]
    half_pos = seq_len // 2
    experts = w_in.shape[0]
    capacity = rows // experts

    loads = [pltpu.make_async_copy(a, b, in_sem.at[n]) for n, (a, b) in enumerate((
        (x0_ref, xbuf), (wk_hbm, wkv.at[0]), (wv_hbm, wkv.at[1]), (h2_ref, hall.at[me]),
        (w_in_hbm, w_in), (w_out_hbm, w_out)))]
    for load in loads:
        load.start()

    barrier = pltpu.get_barrier_semaphore()
    peers = [(other, ep), (tp, ep2), (tp, ep1), (other, ep1), (other, ep2), (tp, ep3), (other, ep3)]
    for peer_tp, peer_ep in peers:
        pl.semaphore_signal(barrier, inc=1, device_id=(lax.axis_index('dp'), peer_tp, peer_ep), device_id_type=MESH)
    pl.semaphore_wait(barrier, len(peers))

    def half_at(k):
        return pl.ds(pl.multiple_of(k * half_pos, half_pos), half_pos)

    def block(owner, k):
        return hall.at[owner, :, half_at(k), :]

    sends = []
    for n, peer in enumerate(((other, ep), (tp, ep2), (tp, ep1))):
        for k in ((other, tp) if n == 0 else (tp, other)):
            sends.append(remote(h2_ref.at[:, half_at(k), :], block(me, k), hs_send.at[n, k], hs_recv.at[me, k], *peer))
    for copy in sends:
        copy.start()

    def arrived(ref, sem):
        remote(ref, ref, hs_send.at[0], sem, tp, ep).wait_recv()

    def block_arrived(owner, k):
        arrived(block(owner, k), hs_recv.at[owner, k])

    def forward(n, owner, k, *peer):
        copy = remote(block(owner, k), block(owner, k), hs_send.at[n, k], hs_recv.at[owner, k], *peer)
        copy.start()
        sends.append(copy)

    num_experts = router_ref.shape[0]
    ids_row = jnp.concatenate([ids_ref[s] for s in range(ids_ref.shape[0])], axis=1)
    expert = lax.broadcasted_iota(jnp.int32, (num_experts, tokens), 0)
    hot = [jnp.where(ids_row[c:c + 1] == expert, 1.0, 0.0) for c in range(2)]
    earlier = lax.broadcasted_iota(jnp.int32, (tokens, tokens), 0) <= lax.broadcasted_iota(jnp.int32, (tokens, tokens), 1)
    upto = mm(jnp.concatenate(hot, axis=0).astype(BF16), jnp.where(earlier, 1.0, 0.0).astype(BF16))
    base = (0.0, upto[:num_experts, tokens - 1:])
    wide_ids = ids_row.astype(F32)
    slot_rows = []
    for c in range(2):
        place = jnp.sum((upto[c * num_experts:(c + 1) * num_experts] - 1.0 + base[c]) * hot[c], axis=0, keepdims=True)
        slot_rows.append(jnp.where(place < capacity, wide_ids[c:c + 1] * capacity + place, -1.0))
    packed = jnp.concatenate(slot_rows + [wide_ids, jnp.zeros((4, tokens), F32)], axis=0)
    slot_row_ref[...] = packed[:2].astype(jnp.int32)
    slots_all[me] = packed[:2].astype(jnp.int32)
    columns_ref[...] = packed.T.astype(jnp.int32)
    slot_copies = [remote(slot_row_ref, slots_all.at[me], slot_send.at[n], slot_recv.at[me], *peer) for n, peer in enumerate(peers)]
    for copy in slot_copies:
        copy.start()
    send_h1 = remote(h1_ref, h1t_ref, h1_send, h1_recv, other, ep)
    send_h1.start()

    def cache_part(source, layer, owner, load=None):
        if load is None:
            load = pltpu.make_async_copy(source, xbuf, cache_sem)
            load.start()
        load.wait()

        @pl.loop(0, seqs)
        def _(s):
            a = rms_rows(xbuf[s], ln_attn_ref[layer])
            for n, ref in enumerate((k_ref, v_ref)):
                full = mm(a, wkv[n, layer])
                kvbuf[s, n] = full.T.astype(BF16).reshape(kvbuf.shape[2:])
                pltpu.make_async_copy(kvbuf.at[s, n], ref.at[layer, owner * seqs + s], store_sem.at[s, n]).start()

        @pl.loop(0, seqs)
        def _(s):
            for n, ref in enumerate((k_ref, v_ref)):
                pltpu.make_async_copy(kvbuf.at[s, n], ref.at[layer, owner * seqs + s], store_sem.at[s, n]).wait()

    loads[1].wait()
    loads[2].wait()
    cache_part(x0_ref, 0, tp, loads[0])
    cache_part(x0t_ref, 0, other)
    cache_part(h1_ref, 1, tp)

    y_owner, x_owner, c_owner = other * 4 + ep, tp * 4 + ep2, tp * 4 + ep1
    yx_owner, yc_owner, xc_owner, yxc_owner = other * 4 + ep2, other * 4 + ep1, tp * 4 + ep3, other * 4 + ep3
    for place, k in enumerate((tp, other)):
        with scope(f"w_y{place}"):
            block_arrived(y_owner, k)
        forward(3, y_owner, k, tp, ep2)
        forward(4, y_owner, k, tp, ep1)
    loads[3].wait()

    def own_tokens(owner):
        return hall[owner, :, half_at(tp), :].reshape(tokens // 2, d_model)

    for part in range(2):
        at = slice(part * (tokens // 2), (part + 1) * (tokens // 2))
        h_own = own_tokens(part * 4 + ep)
        acc[at] = h_own.astype(F32)
        b = rms_rows(h_own, ln_ffn_ref[1])
        logits = lax.dot_general(b.astype(F32), router_ref[...], (((1,), (1,)), ((), ())),
                                 precision=lax.Precision.HIGHEST, preferred_element_type=F32)
        grown = jnp.exp(logits - jnp.max(logits, axis=-1, keepdims=True))
        probs = grown / jnp.sum(grown, axis=-1, keepdims=True)
        lanes = lax.broadcasted_iota(jnp.int32, probs.shape, 1)
        picked = [jnp.sum(jnp.where(columns_ref[at, 2 + c:3 + c] == lanes, probs, 0.0), axis=-1, keepdims=True) for c in range(2)]
        both = picked[0] + picked[1]
        gates[at, 0:1] = picked[0] / both
        gates[at, 1:2] = picked[1] / both

    with scope("w_x"):
        for k in (tp, other):
            block_arrived(x_owner, k)
            forward(5, x_owner, k, tp, ep1)
    for peer_tp, peer_ep in peers:
        arrived(slots_all.at[peer_tp * 4 + peer_ep], slot_recv.at[peer_tp * 4 + peer_ep])
    loads[4].wait()
    loads[5].wait()

    def run_group(i, k):
        dest = k * 4 + i
        slots = slots_all[dest]
        want = me * rows + lax.broadcasted_iota(jnp.int32, (rows, tokens // 2), 0)
        chosen = None
        for part in range(2):
            h = hall[part * 4 + i, :, half_at(k), :].reshape(tokens // 2, d_model)
            at = slice(part * (tokens // 2), (part + 1) * (tokens // 2))
            pick = jnp.logical_or(slots[0:1, at] == want, slots[1:2, at] == want)
            term = mm(jnp.where(pick, 1.0, 0.0).astype(BF16), h)
            chosen = term if chosen is None else chosen + term
        b = rms_rows(chosen, ln_ffn_ref[1])
        for e in range(experts):
            at = slice(e * capacity, (e + 1) * capacity)
            hid = jax.nn.gelu(mm(b[at], w_in[e])).astype(BF16)
            res[dest, at] = mm(hid, w_out[e]).astype(BF16)
        return dest

    some = rows // 2

    def give_back(i, k):
        dest = k * 4 + i
        return [remote(res.at[dest, pl.ds(p * some, some), :], ret.at[me, pl.ds(p * some, some), :],
                       ret_send.at[dest, p], ret_recv.at[me, p], k, i) for p in range(2)]

    def add_rows(source_ref, base, rows):
        step = 256

        @pl.loop(0, tokens // step)
        def _(r):
            at = pl.ds(pl.multiple_of(r * step, step), step)
            columns = base + lax.broadcasted_iota(jnp.int32, (step, rows), 1)
            total = acc[at, :]
            for c in range(2):
                pick = jnp.where(columns_ref[at, c:c + 1] == columns, 1.0, 0.0).astype(BF16)
                total = total + gates[at, c:c + 1] * mm(pick, source_ref[...])
            acc[at, :] = total

    with scope("w_yc"):
        for k in range(2):
            block_arrived(c_owner, k)
            block_arrived(yc_owner, k)

    @pl.loop(0, 4)
    def _(t):
        late = t // 2
        beside = lax.rem((t + 1) // 2, 2)
        i = ep + beside * (ep1 - ep)
        k = late * tp + (1 - late) * other
        run_group(i, k)

        @pl.when(t < 3)
        def _():
            for copy in give_back(i, k):
                copy.start()

    add_rows(res.at[me], me * rows, rows)

    for place, k in enumerate((tp, other)):
        with scope(f"w_yx{place}"):
            block_arrived(yx_owner, k)
        forward(6, yx_owner, k, tp, ep1)
        with scope(f"w_far{place}"):
            block_arrived(xc_owner, k)
            block_arrived(yxc_owner, k)

        @pl.loop(0, 2)
        def _(t):
            i = (1 - t) * ep2 + t * ep3
            run_group(i, k)
            for copy in give_back(i, k):
                copy.start()

        if place == 0:
            with scope("w_h1"):
                arrived(h1t_ref, h1_recv)
            cache_part(h1t_ref, 1, other)

    @pl.loop(1, 8)
    def _(n):
        across, beside, far = lax.rem(n // 2, 2), lax.rem(n, 2), n // 4
        peer_tp = tp + across * (other - tp)
        peer_ep = lax.rem(ep + beside * (ep1 - ep) + 2 * far, 4)
        owner = peer_tp * 4 + peer_ep
        for p in range(2):
            arrived(ret.at[owner, pl.ds(p * some, some), :], ret_recv.at[owner, p])
            add_rows(ret.at[owner, pl.ds(p * some, some), :], owner * rows + p * some, some)

    out_ref[...] = acc[...].astype(BF16)

    for copy in sends + slot_copies + [send_h1]:
        copy.wait_send()
    for peer_tp, peer_ep in peers:
        for copy in give_back(peer_ep, peer_tp):
            copy.wait_send()


def moe_layer(h2, h1, x0, x0t, expert_ids, ln_ffn, ln_attn, w_router, expert_in, expert_out, w_key, w_value):
    seqs, seq_len, d_model = h2.shape
    tokens = seqs * seq_len
    experts, _, d_ff = expert_in.shape
    groups = 8
    rows = experts * 4 * tokens // (experts * groups)
    inner = w_key.shape[2]
    heads = inner // 64
    any_spec = pl.BlockSpec(memory_space=pl.ANY)
    vmem_spec = pl.BlockSpec(memory_space=pltpu.VMEM)
    cache_shape = jax.ShapeDtypeStruct((2, 2 * seqs, heads, 64, seq_len), BF16)
    dma = pltpu.SemaphoreType.DMA
    return pl.pallas_call(
        moe_body,
        in_specs=[any_spec] * 4 + [vmem_spec] * 4 + [any_spec] * 4,
        out_specs=[vmem_spec, any_spec, any_spec, any_spec],
        out_shape=[jax.ShapeDtypeStruct((tokens, d_model), BF16), cache_shape, cache_shape, jax.ShapeDtypeStruct(h1.shape, BF16)],
        scratch_shapes=[
            pltpu.VMEM((groups,) + h2.shape, BF16),
            pltpu.VMEM((groups, rows, d_model), BF16),
            pltpu.VMEM((groups, rows, d_model), BF16),
            pltpu.VMEM(expert_in.shape, BF16),
            pltpu.VMEM(expert_out.shape, BF16),
            pltpu.VMEM((2, 2, d_model, inner), BF16),
            pltpu.VMEM((tokens, d_model), F32),
            pltpu.VMEM((2, tokens), jnp.int32),
            pltpu.VMEM((groups, 2, tokens), jnp.int32),
            pltpu.VMEM((tokens, 8), jnp.int32),
            pltpu.VMEM((tokens, 2), F32),
            pltpu.VMEM(h1.shape, BF16),
            pltpu.VMEM((seqs, 2, heads, 64, seq_len), BF16),
            dma((6,)), dma, dma((seqs, 2)), dma((7,)), dma((groups,)), dma((7, 2)), dma((groups, 2)),
            dma((groups, 2)), dma((groups, 2)), dma, dma,
        ],
        compiler_params=pltpu.CompilerParams(vmem_limit_bytes=67043328, collective_id=2, has_side_effects=True),
        cost_estimate=pl.CostEstimate(flops=40_000_000_000, bytes_accessed=64 << 20, transcendentals=0),
        name="moe",
    )(h2, h1, x0, x0t, jnp.swapaxes(expert_ids, 1, 2), ln_ffn, ln_attn, w_router.T, expert_in, expert_out, w_key, w_value)


def solution(mesh):
    act_spec = P(('dp', 'ep'), 'tp', None)
    col_spec = P(None, None, 'tp')
    row_spec = P(None, 'tp', None)
    expert_spec = P(('tp', 'ep'), None, None)
    cache_spec = P(None, ('dp', 'ep'), 'tp', None, None)
    in_specs = (act_spec, P(), P(), col_spec, col_spec, col_spec, row_spec, row_spec,
                P(None, 'tp'), P(None, 'tp'), P('tp', None), P(), expert_spec, expert_spec, act_spec)

    def device_fn(hidden_in, ln_attn, ln_ffn, w_query, w_key, w_value, w_out, bias_table, w_gate, w_up, w_down, w_router, expert_in, expert_out, expert_ids):
        h1, h2, x0, x0t = dense_layers(hidden_in, ln_attn, ln_ffn, w_query, w_key, w_value, w_out, bias_table, w_gate, w_up, w_down)
        hidden, k_cache, v_cache, _ = moe_layer(
            h2, h1, x0, x0t, expert_ids, ln_ffn, ln_attn, w_router, expert_in, expert_out, w_key, w_value)
        return hidden.reshape(hidden_in.shape), jnp.swapaxes(k_cache, 3, 4), jnp.swapaxes(v_cache, 3, 4)

    return jax.shard_map(device_fn, mesh=mesh, in_specs=in_specs, out_specs=(act_spec, cache_spec, cache_spec), check_vma=False)
```

```python
import contextlib

import jax
import jax.numpy as jnp
from jax import lax
from jax.experimental import pallas as pl
from jax.experimental.pallas import tpu as pltpu
from jax.sharding import PartitionSpec as P

EXACT_BUCKETS = 16
THRESHOLDS = (18, 20, 23, 26, 30, 34, 39, 45, 51, 58, 66, 76, 86, 98, 112)
EPSILON = 1e-6
F32 = jnp.float32
BF16 = jnp.bfloat16
VMEM_LIMIT = 60 * 1024 * 1024
MESH = pl.DeviceIdType.MESH


def scope(name):
    return contextlib.nullcontext()


def rms_rows(rows, ln_scale):
    wide = rows.astype(F32)
    inv_rms = lax.rsqrt(jnp.mean(wide * wide, axis=-1, keepdims=True) + EPSILON)
    return (wide * inv_rms * ln_scale).astype(BF16)


def mm(a, b):
    return lax.dot_general(a, b, (((1,), (0,)), ((), ())), preferred_element_type=F32)


def mm_t(a, b):
    return lax.dot_general(a, b, (((1,), (1,)), ((), ())), preferred_element_type=F32)


def bias_rows(table, seq_len):
    at = lax.broadcasted_iota(jnp.int32, (table.shape[1], 2 * seq_len), 1)
    rel = jnp.where(at == 0, 0, 2 * seq_len - at)
    bucket = jnp.minimum(rel, EXACT_BUCKETS)
    for threshold in THRESHOLDS:
        bucket = bucket + jnp.where(rel >= threshold, 1, 0)
    hot = jnp.where(bucket == lax.broadcasted_iota(jnp.int32, bucket.shape, 0), 1.0, 0.0)
    rows = jnp.dot(table, hot, precision=lax.Precision.HIGHEST, preferred_element_type=F32)
    return jnp.where(rel[:1] < seq_len, rows, -jnp.inf)


def softmax_bf16(scores):
    top = jnp.max(scores, axis=-1, keepdims=True)
    grown = jnp.exp(scores - top)
    return (grown * (1.0 / jnp.sum(grown, axis=-1, keepdims=True))).astype(BF16)


def axis_neighbours(tp, ep):
    core = lax.rem(ep, 2)
    beside = ep + 1 - 2 * core
    return beside, lax.rem(ep + 2, 4), lax.rem(beside + 2, 4)


def remote(src, dst, send, recv, tp, ep):
    return pltpu.make_async_remote_copy(
        src_ref=src, dst_ref=dst, send_sem=send, recv_sem=recv,
        device_id=(lax.axis_index('dp'), tp, ep), device_id_type=MESH)


def layers_body(hid_ref, ln_attn_ref, ln_ffn_ref, wq_hbm, wk_hbm, wv_hbm, wo_hbm, table_ref, wg_hbm, wu_hbm, wd_hbm,
                h1_ref, h2_ref, x0_ref, x0t_ref,
                x, a_ref, acc, w, wo, gu, wd, table_other, u_rows, bias_low, bias_high, qkv, ctx, stage,
                in_sem, own_sem, out_sem, x0_sem, entry_send, entry_recv, misc_send, misc_recv, y_send, y_recv, x_send, x_recv, c_send, c_recv, d_send, d_recv):
    tp, ep = lax.axis_index('tp'), lax.axis_index('ep')
    other = 1 - tp
    ep1, ep2, ep3 = axis_neighbours(tp, ep)
    seqs, seq_len, d_model = x.shape
    half = seq_len // 2
    tokens = seqs * seq_len
    quad = qkv.shape[2]

    def part(count, quarter):
        return pl.ds(pl.multiple_of(quarter * count, count), count)

    my_pos = part(half, tp)
    mine = hid_ref.at[pl.ds(tp * seqs, seqs)]
    theirs = hid_ref.at[pl.ds(other * seqs, seqs)]

    sources, places = [], []
    for layer in range(2):
        for kind, hbm in enumerate((wq_hbm, wk_hbm, wv_hbm)):
            sources.append(hbm.at[layer, part(256, ep), :])
            places.append(lambda q, layer=layer, kind=kind: w.at[layer, 1, kind, part(256, q), :])
        sources.append(wo_hbm.at[layer, part(128, ep), :])
        places.append(lambda q, layer=layer: wo.at[layer, 1, part(128, q), :])
        if layer == 0:
            for kind, hbm in enumerate((wg_hbm, wu_hbm)):
                sources.append(hbm.at[part(256, ep), :])
                places.append(lambda q, kind=kind: gu.at[1, kind, part(256, q), :])
            sources.append(wd_hbm.at[part(64, ep), :])
            places.append(lambda q: wd.at[1, part(64, q), :])

    own_x = pltpu.make_async_copy(mine, x.at[:, my_pos, :], in_sem.at[0])
    own_stage = pltpu.make_async_copy(theirs, stage, in_sem.at[1])
    own_x.start()
    own_loads = []
    for layer in range(2):
        for kind, hbm in enumerate((wq_hbm, wk_hbm, wv_hbm)):
            own_loads.append((hbm.at[layer], w.at[layer, 0, kind]))
        own_loads.append((wo_hbm.at[layer], wo.at[layer, 0]))
        if layer == 0:
            own_loads += [(wg_hbm, gu.at[0, 0]), (wu_hbm, gu.at[0, 1]), (wd_hbm, wd.at[0])]
    own_loads = [pltpu.make_async_copy(s, d, own_sem.at[n]) for n, (s, d) in enumerate(own_loads)]
    for load in own_loads:
        load.start()
    own_stage.start()

    barrier = pltpu.get_barrier_semaphore()
    for peer_tp, peer_ep in ((other, ep), (tp, ep2), (tp, ep1)):
        pl.semaphore_signal(barrier, inc=1, device_id=(lax.axis_index('dp'), peer_tp, peer_ep), device_id_type=MESH)
    pl.semaphore_wait(barrier, 3)

    def arrived(ref, sem):
        remote(ref, ref, misc_send.at[0], sem, tp, ep).wait_recv()

    pieces = range(len(sources))
    entry_copies = [remote(hid_ref.at[other * seqs + s], x.at[s, my_pos, :], entry_send.at[s], entry_recv.at[s], other, ep) for s in range(seqs)]
    send_u = remote(table_ref, table_other, misc_send.at[1], misc_recv.at[1], other, ep)
    send_rest = remote(mine, x0t_ref.at[:, my_pos, :], misc_send.at[2], misc_recv.at[2], other, ep)
    y_copies = [remote(sources[n], places[n](ep), y_send.at[n], y_recv.at[n], other, ep) for n in pieces]
    x_copies = [remote(places[n](ep), places[n](ep), x_send.at[n], x_recv.at[n], tp, ep2) for n in pieces]
    c_copies = [remote(places[n](ep), places[n](ep), c_send.at[n], c_recv.at[n], tp, ep1) for n in pieces]
    d_copies = [remote(places[n](ep2), places[n](ep2), d_send.at[n], d_recv.at[n], tp, ep1) for n in pieces]
    send_u.start()
    for copy in y_copies[:4] + entry_copies + y_copies[4:] + [send_rest]:
        copy.start()

    def pass_on(n):
        arrived(places[n](ep), y_recv.at[n])
        x_copies[n].start()
        c_copies[n].start()

    def pass_across(n):
        arrived(places[n](ep2), x_recv.at[n])
        d_copies[n].start()

    def complete(n):
        arrived(places[n](ep1), c_recv.at[n])
        arrived(places[n](ep3), d_recv.at[n])

    def build_bias(rows_ref, side):
        u_rows[...] = bias_rows(rows_ref[...].reshape(u_rows.shape[0], rows_ref.shape[2]), seq_len)

        @pl.loop(0, 8)
        def _(n):
            layer, pair = n // 4, lax.rem(n, 4)
            for sub in range(2):
                row = u_rows[pl.ds(n * 2 + sub, 1), :]
                wide = pltpu.roll(jnp.broadcast_to(row, (seq_len, 2 * seq_len)), 0, 1, stride=1, stride_axis=0)
                at = slice(sub * half, (sub + 1) * half)
                place = layer * 8 + side * 4 + pair
                bias_low[place, at, :] = wide[:half, :half]
                bias_high[place, at, :] = wide[half:, :seq_len]

    def begin_seq(layer, s):
        rows = part(seq_len, s)
        a_ref[rows, :] = rms_rows(x[s], ln_attn_ref[layer])
        acc[rows, :] = x[s].astype(F32)

    def end_seq(s):
        x[s] = acc[part(seq_len, s), :].astype(BF16)

    def each_seq(step, *args):
        @pl.loop(0, seqs)
        def _(s):
            step(*args, s)

    first = lax.broadcasted_iota(jnp.int32, (1, 128), 1) < 64

    def products(layer, side, block, rows):
        for kind in range(3):
            qkv[kind, rows, :] = mm(a_ref[rows, :], w[layer, side, kind, :, block * quad:(block + 1) * quad]).astype(BF16)

    def attend_seq(layer, side, block, s):
        rows = part(seq_len, s)
        for pair in range(quad // 128):
            lanes = slice(pair * 128, (pair + 1) * 128)
            place = layer * 8 + side * 4 + block * (quad // 128) + pair
            q, k, v = (qkv[kind, rows, lanes] for kind in range(3))
            none = jnp.zeros_like(q[:half])
            outs = []
            for upper in range(2):
                qs = q[half:] if upper else q[:half]
                ks, vs = (k, v) if upper else (k[:half], v[:half])
                both = jnp.concatenate([jnp.where(first, qs, none), jnp.where(first, none, qs)], axis=0)
                bias = bias_high[place] if upper else bias_low[place]
                got = mm(softmax_bf16(mm_t(both, ks) * 0.125 + bias), vs)
                outs.append(jnp.where(first, got[:half], got[half:]))
            ctx[rows, lanes] = jnp.concatenate(outs, axis=0).astype(BF16)

    def project_seq(layer, side, block, s):
        rows = part(seq_len, s)
        acc[rows, :] += mm(ctx[rows, :], wo[layer, side, block * quad:(block + 1) * quad, :])

    def attend(layer, side, block):
        products(layer, side, block, slice(None))
        each_seq(attend_seq, layer, side, block)

    def project(layer, side, block):
        each_seq(project_seq, layer, side, block)

    def dense(s):
        h = x[s]
        b = rms_rows(h, ln_ffn_ref[0])
        total = h.astype(F32)
        for side in range(2):
            hid = (jax.nn.gelu(mm(b, gu[side, 0])) * mm(b, gu[side, 1])).astype(BF16)
            total = total + mm(hid, wd[side])
        x[s] = total.astype(BF16)

    def heads(layer, side, block):
        attend(layer, side, block)
        project(layer, side, block)

    build_bias(table_ref, 0)
    arrived(table_other, misc_recv.at[1])
    build_bias(table_other, 1)
    own_stage.wait()
    own_x0t = pltpu.make_async_copy(stage, x0t_ref.at[:, my_pos, :], out_sem.at[0])
    own_x0t.start()

    with scope("w_l0_y"):
        for n in range(4):
            pass_on(n)
    with scope("w_l0_x"):
        for n in range(4):
            pass_across(n)
    own_x.wait()
    for n in range(4):
        own_loads[n].wait()
        complete(n)

    def x0_copy(s):
        return pltpu.make_async_copy(x.at[s], x0_ref.at[s], x0_sem.at[s])

    @pl.loop(0, seqs)
    def _(s):
        with scope("w_entry"):
            arrived(x.at[s, part(half, other), :], entry_recv.at[s])
        x0_copy(s).start()
        begin_seq(0, s)
        for side in range(2):
            for block in range(2):
                products(0, side, block, part(seq_len, s))
                attend_seq(0, side, block, s)
                project_seq(0, side, block, s)
            if side == 0:
                @pl.when(s == seqs - 1)
                def _():
                    pass_on(5)
                    pass_on(6)
        x0_copy(s).wait()
        end_seq(s)

        @pl.when(s == seqs - 2)
        def _():
            pass_on(4)

    with scope("w_ffn_y"):
        pass_on(7)
    with scope("w_ffn_x"):
        for n in range(4, 7):
            pass_across(n)
    with scope("w_ffn_all"):
        for n in range(4, 7):
            own_loads[n].wait()
            complete(n)

    @pl.loop(0, seqs // 2)
    def _(s):
        dense(s)

    with scope("w_l1_k"):
        pass_on(8)

    @pl.loop(seqs // 2, seqs)
    def _(s):
        dense(s)

    out_h1 = pltpu.make_async_copy(x, h1_ref, out_sem.at[2])
    out_h1.start()
    each_seq(begin_seq, 1)
    for n in range(7, 11):
        own_loads[n].wait()
    attend(1, 0, 0)
    with scope("w_l1_v"):
        pass_on(9)
    project(1, 0, 0)
    heads(1, 0, 1)
    with scope("w_l1_o"):
        pass_on(10)
    with scope("w_l1_x"):
        for n in range(7, 10):
            pass_across(n)
    with scope("w_l1_all"):
        for n in range(7, 10):
            complete(n)
    attend(1, 1, 0)
    with scope("w_l1_o_all"):
        pass_across(10)
        complete(10)
    project(1, 1, 0)
    heads(1, 1, 1)
    out_h1.wait()
    each_seq(end_seq)
    out_h2 = pltpu.make_async_copy(x, h2_ref, out_sem.at[3])
    out_h2.start()

    with scope("w_rest"):
        arrived(x0t_ref.at[:, part(half, other), :], misc_recv.at[2])
    own_x0t.wait()
    for copy in entry_copies + [send_u, send_rest] + y_copies + x_copies + c_copies + d_copies:
        copy.wait_send()
    out_h2.wait()


def dense_layers(hidden_in, ln_attn, ln_ffn, w_query, w_key, w_value, w_out, bias_table, w_gate, w_up, w_down):
    batch, positions, d_model = hidden_in.shape
    seqs, seq_len = batch // 2, 2 * positions
    inner = w_query.shape[2]
    any_spec = pl.BlockSpec(memory_space=pl.ANY)
    vmem_spec = pl.BlockSpec(memory_space=pltpu.VMEM)
    dma = pltpu.SemaphoreType.DMA
    shape = jax.ShapeDtypeStruct((seqs, seq_len, d_model), BF16)
    return pl.pallas_call(
        layers_body,
        in_specs=[any_spec, vmem_spec, vmem_spec] + [any_spec] * 4 + [vmem_spec] + [any_spec] * 3,
        out_specs=[any_spec] * 4,
        out_shape=[shape] * 4,
        scratch_shapes=[
            pltpu.VMEM(shape.shape, BF16),
            pltpu.VMEM((seqs * seq_len, d_model), BF16),
            pltpu.VMEM((seqs * seq_len, d_model), F32),
            pltpu.VMEM((2, 2, 3, d_model, inner), BF16),
            pltpu.VMEM((2, 2, inner, d_model), BF16),
            pltpu.VMEM((2, 2) + w_gate.shape, BF16),
            pltpu.VMEM((2,) + w_down.shape, BF16),
            pltpu.VMEM(bias_table.shape, F32),
            pltpu.VMEM((bias_table.shape[0] * bias_table.shape[1], 2 * seq_len), F32),
            pltpu.VMEM((16, seq_len, seq_len // 2), F32),
            pltpu.VMEM((16, seq_len, seq_len), F32),
            pltpu.VMEM((3, seqs * seq_len, 256), BF16),
            pltpu.VMEM((seqs * seq_len, 256), BF16),
            pltpu.VMEM((seqs, positions, d_model), BF16),
            dma((2,)), dma((11,)), dma((4,)), dma((seqs,)), dma((seqs,)), dma((seqs,)), dma((3,)), dma((3,)),
        ] + [dma((11,))] * 8,
        compiler_params=pltpu.CompilerParams(vmem_limit_bytes=VMEM_LIMIT, collective_id=1, has_side_effects=True),
        cost_estimate=pl.CostEstimate(flops=32_000_000_000, bytes_accessed=40 << 20, transcendentals=0),
        name="dense_layers",
    )(hidden_in, ln_attn, ln_ffn, w_query, w_key, w_value, w_out, bias_table, w_gate, w_up, w_down)


def moe_body(h2_ref, h1_ref, x0_ref, x0t_ref, ids_ref, ln_ffn_ref, ln_attn_ref, router_ref,
             w_in_hbm, w_out_hbm, wk_hbm, wv_hbm,
             out_ref, k_ref, v_ref, h1t_ref,
             hall, res, ret, w_in, w_out, wkv, acc, slot_row_ref, slots_all, columns_ref, gates, xbuf, kvbuf,
             in_sem, cache_sem, store_sem, slot_send, slot_recv, hs_send, hs_recv, ret_send, ret_recv, h1_send, h1_recv):
    tp, ep = lax.axis_index('tp'), lax.axis_index('ep')
    other = 1 - tp
    ep1, ep2, ep3 = axis_neighbours(tp, ep)
    me = tp * 4 + ep
    seqs, seq_len, d_model = h2_ref.shape
    tokens = acc.shape[0]
    rows = res.shape[1]
    half_pos = seq_len // 2
    experts = w_in.shape[0]
    capacity = rows // experts

    loads = [pltpu.make_async_copy(a, b, in_sem.at[n]) for n, (a, b) in enumerate((
        (x0_ref, xbuf), (wk_hbm, wkv.at[0]), (wv_hbm, wkv.at[1]), (h2_ref, hall.at[me]),
        (w_in_hbm, w_in), (w_out_hbm, w_out)))]
    for load in loads:
        load.start()

    barrier = pltpu.get_barrier_semaphore()
    peers = [(other, ep), (tp, ep2), (tp, ep1), (other, ep1), (other, ep2), (tp, ep3), (other, ep3)]
    for peer_tp, peer_ep in peers:
        pl.semaphore_signal(barrier, inc=1, device_id=(lax.axis_index('dp'), peer_tp, peer_ep), device_id_type=MESH)
    pl.semaphore_wait(barrier, len(peers))

    def half_at(k):
        return pl.ds(pl.multiple_of(k * half_pos, half_pos), half_pos)

    def block(owner, k):
        return hall.at[owner, :, half_at(k), :]

    sends = []
    for n, peer in enumerate(((other, ep), (tp, ep2), (tp, ep1))):
        for k in ((other, tp) if n == 0 else (tp, other)):
            sends.append(remote(h2_ref.at[:, half_at(k), :], block(me, k), hs_send.at[n, k], hs_recv.at[me, k], *peer))
    for copy in sends:
        copy.start()

    def arrived(ref, sem):
        remote(ref, ref, hs_send.at[0], sem, tp, ep).wait_recv()

    def block_arrived(owner, k):
        arrived(block(owner, k), hs_recv.at[owner, k])

    def forward(n, owner, k, *peer):
        copy = remote(block(owner, k), block(owner, k), hs_send.at[n, k], hs_recv.at[owner, k], *peer)
        copy.start()
        sends.append(copy)

    num_experts = router_ref.shape[0]
    ids_row = jnp.concatenate([ids_ref[s] for s in range(ids_ref.shape[0])], axis=1)
    expert = lax.broadcasted_iota(jnp.int32, (num_experts, tokens), 0)
    hot = [jnp.where(ids_row[c:c + 1] == expert, 1.0, 0.0) for c in range(2)]
    earlier = lax.broadcasted_iota(jnp.int32, (tokens, tokens), 0) <= lax.broadcasted_iota(jnp.int32, (tokens, tokens), 1)
    upto = mm(jnp.concatenate(hot, axis=0).astype(BF16), jnp.where(earlier, 1.0, 0.0).astype(BF16))
    base = (0.0, upto[:num_experts, tokens - 1:])
    wide_ids = ids_row.astype(F32)
    slot_rows = []
    for c in range(2):
        place = jnp.sum((upto[c * num_experts:(c + 1) * num_experts] - 1.0 + base[c]) * hot[c], axis=0, keepdims=True)
        slot_rows.append(jnp.where(place < capacity, wide_ids[c:c + 1] * capacity + place, -1.0))
    packed = jnp.concatenate(slot_rows + [wide_ids, jnp.zeros((4, tokens), F32)], axis=0)
    slot_row_ref[...] = packed[:2].astype(jnp.int32)
    slots_all[me] = packed[:2].astype(jnp.int32)
    columns_ref[...] = packed.T.astype(jnp.int32)
    slot_copies = [remote(slot_row_ref, slots_all.at[me], slot_send.at[n], slot_recv.at[me], *peer) for n, peer in enumerate(peers)]
    for copy in slot_copies:
        copy.start()
    send_h1 = remote(h1_ref, h1t_ref, h1_send, h1_recv, other, ep)
    send_h1.start()

    def cache_part(source, layer, owner, load=None):
        if load is None:
            load = pltpu.make_async_copy(source, xbuf, cache_sem)
            load.start()
        load.wait()

        @pl.loop(0, seqs)
        def _(s):
            a = rms_rows(xbuf[s], ln_attn_ref[layer])
            for n, ref in enumerate((k_ref, v_ref)):
                full = mm(a, wkv[n, layer])
                kvbuf[s, n] = full.T.astype(BF16).reshape(kvbuf.shape[2:])
                pltpu.make_async_copy(kvbuf.at[s, n], ref.at[layer, owner * seqs + s], store_sem.at[s, n]).start()

        @pl.loop(0, seqs)
        def _(s):
            for n, ref in enumerate((k_ref, v_ref)):
                pltpu.make_async_copy(kvbuf.at[s, n], ref.at[layer, owner * seqs + s], store_sem.at[s, n]).wait()

    loads[1].wait()
    loads[2].wait()
    cache_part(x0_ref, 0, tp, loads[0])
    cache_part(x0t_ref, 0, other)
    cache_part(h1_ref, 1, tp)

    y_owner, x_owner, c_owner = other * 4 + ep, tp * 4 + ep2, tp * 4 + ep1
    yx_owner, yc_owner, xc_owner, yxc_owner = other * 4 + ep2, other * 4 + ep1, tp * 4 + ep3, other * 4 + ep3
    for place, k in enumerate((tp, other)):
        with scope(f"w_y{place}"):
            block_arrived(y_owner, k)
        forward(3, y_owner, k, tp, ep2)
        forward(4, y_owner, k, tp, ep1)
    loads[3].wait()

    def own_tokens(owner):
        return hall[owner, :, half_at(tp), :].reshape(tokens // 2, d_model)

    for part in range(2):
        at = slice(part * (tokens // 2), (part + 1) * (tokens // 2))
        h_own = own_tokens(part * 4 + ep)
        acc[at] = h_own.astype(F32)
        b = rms_rows(h_own, ln_ffn_ref[1])
        logits = lax.dot_general(b.astype(F32), router_ref[...], (((1,), (1,)), ((), ())),
                                 precision=lax.Precision.HIGHEST, preferred_element_type=F32)
        grown = jnp.exp(logits - jnp.max(logits, axis=-1, keepdims=True))
        probs = grown / jnp.sum(grown, axis=-1, keepdims=True)
        lanes = lax.broadcasted_iota(jnp.int32, probs.shape, 1)
        picked = [jnp.sum(jnp.where(columns_ref[at, 2 + c:3 + c] == lanes, probs, 0.0), axis=-1, keepdims=True) for c in range(2)]
        both = picked[0] + picked[1]
        gates[at, 0:1] = picked[0] / both
        gates[at, 1:2] = picked[1] / both

    with scope("w_x"):
        for k in (tp, other):
            block_arrived(x_owner, k)
            forward(5, x_owner, k, tp, ep1)
    for peer_tp, peer_ep in peers:
        arrived(slots_all.at[peer_tp * 4 + peer_ep], slot_recv.at[peer_tp * 4 + peer_ep])
    loads[4].wait()
    loads[5].wait()

    def run_group(i, k):
        dest = k * 4 + i
        slots = slots_all[dest]
        want = me * rows + lax.broadcasted_iota(jnp.int32, (rows, tokens // 2), 0)
        chosen = None
        for part in range(2):
            h = hall[part * 4 + i, :, half_at(k), :].reshape(tokens // 2, d_model)
            at = slice(part * (tokens // 2), (part + 1) * (tokens // 2))
            pick = jnp.logical_or(slots[0:1, at] == want, slots[1:2, at] == want)
            term = mm(jnp.where(pick, 1.0, 0.0).astype(BF16), h)
            chosen = term if chosen is None else chosen + term
        b = rms_rows(chosen, ln_ffn_ref[1])
        for e in range(experts):
            at = slice(e * capacity, (e + 1) * capacity)
            hid = jax.nn.gelu(mm(b[at], w_in[e])).astype(BF16)
            res[dest, at] = mm(hid, w_out[e]).astype(BF16)
        return dest

    some = rows // 2

    def give_back(i, k):
        dest = k * 4 + i
        return [remote(res.at[dest, pl.ds(p * some, some), :], ret.at[me, pl.ds(p * some, some), :],
                       ret_send.at[dest, p], ret_recv.at[me, p], k, i) for p in range(2)]

    def out_copy(r):
        return pltpu.make_async_copy(xbuf.at[r], out_ref.at[pl.ds(r * seq_len, seq_len), :], in_sem.at[r])

    def add_rows(source_ref, base, rows, last=None):
        step = seq_len

        @pl.loop(0, tokens // step)
        def _(r):
            at = pl.ds(pl.multiple_of(r * step, step), step)
            columns = base + lax.broadcasted_iota(jnp.int32, (step, rows), 1)
            total = acc[at, :]
            for c in range(2):
                pick = jnp.where(columns_ref[at, c:c + 1] == columns, 1.0, 0.0).astype(BF16)
                total = total + gates[at, c:c + 1] * mm(pick, source_ref[...])
            acc[at, :] = total
            if last is not None:
                @pl.when(last)
                def _():
                    xbuf[r] = total.astype(BF16)
                    out_copy(r).start()

    with scope("w_yc"):
        for k in range(2):
            block_arrived(c_owner, k)
            block_arrived(yc_owner, k)

    @pl.loop(0, 4)
    def _(t):
        late = t // 2
        beside = lax.rem((t + 1) // 2, 2)
        i = ep + beside * (ep1 - ep)
        k = late * tp + (1 - late) * other
        run_group(i, k)

        @pl.when(t < 3)
        def _():
            for copy in give_back(i, k):
                copy.start()

    add_rows(res.at[me], me * rows, rows)

    for place, k in enumerate((tp, other)):
        with scope(f"w_yx{place}"):
            block_arrived(yx_owner, k)
        forward(6, yx_owner, k, tp, ep1)
        with scope(f"w_far{place}"):
            block_arrived(xc_owner, k)
            block_arrived(yxc_owner, k)

        @pl.loop(0, 2)
        def _(t):
            i = (1 - t) * ep2 + t * ep3
            run_group(i, k)
            for copy in give_back(i, k):
                copy.start()

        if place == 0:
            with scope("w_h1"):
                arrived(h1t_ref, h1_recv)
            cache_part(h1t_ref, 1, other)

    @pl.loop(1, 8)
    def _(n):
        across, beside, far = lax.rem(n // 2, 2), lax.rem(n, 2), n // 4
        peer_tp = tp + across * (other - tp)
        peer_ep = lax.rem(ep + beside * (ep1 - ep) + 2 * far, 4)
        owner = peer_tp * 4 + peer_ep
        for p in range(2):
            arrived(ret.at[owner, pl.ds(p * some, some), :], ret_recv.at[owner, p])
            add_rows(ret.at[owner, pl.ds(p * some, some), :], owner * rows + p * some, some, n == 7 if p == 1 else None)

    for r in range(seqs):
        out_copy(r).wait()

    for copy in sends + slot_copies + [send_h1]:
        copy.wait_send()
    for peer_tp, peer_ep in peers:
        for copy in give_back(peer_ep, peer_tp):
            copy.wait_send()


def moe_layer(h2, h1, x0, x0t, expert_ids, ln_ffn, ln_attn, w_router, expert_in, expert_out, w_key, w_value):
    seqs, seq_len, d_model = h2.shape
    tokens = seqs * seq_len
    experts, _, d_ff = expert_in.shape
    groups = 8
    rows = experts * 4 * tokens // (experts * groups)
    inner = w_key.shape[2]
    heads = inner // 64
    any_spec = pl.BlockSpec(memory_space=pl.ANY)
    vmem_spec = pl.BlockSpec(memory_space=pltpu.VMEM)
    cache_shape = jax.ShapeDtypeStruct((2, 2 * seqs, heads, 64, seq_len), BF16)
    dma = pltpu.SemaphoreType.DMA
    return pl.pallas_call(
        moe_body,
        in_specs=[any_spec] * 4 + [vmem_spec] * 4 + [any_spec] * 4,
        out_specs=[any_spec] * 4,
        out_shape=[jax.ShapeDtypeStruct((tokens, d_model), BF16), cache_shape, cache_shape, jax.ShapeDtypeStruct(h1.shape, BF16)],
        scratch_shapes=[
            pltpu.VMEM((groups,) + h2.shape, BF16),
            pltpu.VMEM((groups, rows, d_model), BF16),
            pltpu.VMEM((groups, rows, d_model), BF16),
            pltpu.VMEM(expert_in.shape, BF16),
            pltpu.VMEM(expert_out.shape, BF16),
            pltpu.VMEM((2, 2, d_model, inner), BF16),
            pltpu.VMEM((tokens, d_model), F32),
            pltpu.VMEM((2, tokens), jnp.int32),
            pltpu.VMEM((groups, 2, tokens), jnp.int32),
            pltpu.VMEM((tokens, 8), jnp.int32),
            pltpu.VMEM((tokens, 2), F32),
            pltpu.VMEM(h1.shape, BF16),
            pltpu.VMEM((seqs, 2, heads, 64, seq_len), BF16),
            dma((6,)), dma, dma((seqs, 2)), dma((7,)), dma((groups,)), dma((7, 2)), dma((groups, 2)),
            dma((groups, 2)), dma((groups, 2)), dma, dma,
        ],
        compiler_params=pltpu.CompilerParams(vmem_limit_bytes=67043328, collective_id=2, has_side_effects=True),
        cost_estimate=pl.CostEstimate(flops=40_000_000_000, bytes_accessed=64 << 20, transcendentals=0),
        name="moe",
    )(h2, h1, x0, x0t, jnp.swapaxes(expert_ids, 1, 2), ln_ffn, ln_attn, w_router.T, expert_in, expert_out, w_key, w_value)


def solution(mesh):
    act_spec = P(('dp', 'ep'), 'tp', None)
    col_spec = P(None, None, 'tp')
    row_spec = P(None, 'tp', None)
    expert_spec = P(('tp', 'ep'), None, None)
    cache_spec = P(None, ('dp', 'ep'), 'tp', None, None)
    in_specs = (act_spec, P(), P(), col_spec, col_spec, col_spec, row_spec, row_spec,
                P(None, 'tp'), P(None, 'tp'), P('tp', None), P(), expert_spec, expert_spec, act_spec)

    def device_fn(hidden_in, ln_attn, ln_ffn, w_query, w_key, w_value, w_out, bias_table, w_gate, w_up, w_down, w_router, expert_in, expert_out, expert_ids):
        h1, h2, x0, x0t = dense_layers(hidden_in, ln_attn, ln_ffn, w_query, w_key, w_value, w_out, bias_table, w_gate, w_up, w_down)
        hidden, k_cache, v_cache, _ = moe_layer(
            h2, h1, x0, x0t, expert_ids, ln_ffn, ln_attn, w_router, expert_in, expert_out, w_key, w_value)
        return hidden.reshape(hidden_in.shape), jnp.swapaxes(k_cache, 3, 4), jnp.swapaxes(v_cache, 3, 4)

    return jax.shard_map(device_fn, mesh=mesh, in_specs=in_specs, out_specs=(act_spec, cache_spec, cache_spec), check_vma=False)
```
